32 devices in a mesh: batch: 4 (over z), rows: 8 (over y, x, core).
Axes of the slice: x: 2, y: 2, z: 4, core: 2. Of those that a mesh axis runs over, the one named last changes fastest.
Arguments:
- level_two: bfloat16 [8, 64, 256, 256], P('batch', 'rows'), parts along dimension 0, may hold values from -130 to 130
- level_three: bfloat16 [8, 32, 128, 512], P('batch', 'rows'), parts along dimension 0, may hold values from -130 to 130
- level_four: bfloat16 [8, 16, 64, 1024], P('batch', 'rows'), parts along dimension 0, may hold values from -130 to 130
- level_five: bfloat16 [8, 8, 32, 2048], P('batch', 'rows'), parts along dimension 0, may hold values from -130 to 130
- lateral_two: bfloat16 [256, 256], replicated, may hold values from -0.375 to 0.375
- lateral_three: bfloat16 [512, 256], replicated, may hold values from -0.25 to 0.25
- lateral_four: bfloat16 [1024, 256], replicated, may hold values from -0.1875 to 0.1875
- lateral_five: bfloat16 [2048, 256], replicated, may hold values from -0.125 to 0.125
- lateral_bias: float32 [4, 256], replicated, may hold values from -4 to 4
- smooth_weight: bfloat16 [4, 3, 768, 256], replicated, may hold values from -0.125 to 0.125
- norm_gain: float32 [4, 256], replicated, may hold values from 0.5 to 1.5
- norm_shift: float32 [4, 256], replicated, may hold values from -2 to 2
Outputs:
- pyramid_two: bfloat16 [8, 64, 256, 256], P('batch', 'rows'), parts along dimension 0
- pyramid_three: bfloat16 [8, 32, 128, 256], P('batch', 'rows'), parts along dimension 0
- pyramid_four: bfloat16 [8, 16, 64, 256], P('batch', 'rows'), parts along dimension 0
- pyramid_five: bfloat16 [8, 8, 32, 256], P('batch', 'rows'), parts along dimension 0
The draws below stay inside these ranges and needn't reach their ends.
There are 4 independent parts, one for each index of `batch`. The reference program is written for one: setup_inputs(seed, part) draws one part's arguments, and reference() takes and returns one part's arrays. A program takes and returns all parts, laid end to end along the dimension named above; an argument that names none is the same for every part. Nothing has to cross between parts.
All inputs are finite; a program needn't handle non-finite values.
Results may differ from the reference program's by a relative error of at most 0.0054.
Values may be sent and summed in bfloat16 or wider, within the bound.
A program may use at most 128 MiB of HBM per device.

```python
import math
import jax
import jax.numpy as jnp
from jax import lax

CHANNELS = 256
DEPTH_TWO = 256
DEPTH_THREE = 512
DEPTH_FOUR = 1024
DEPTH_FIVE = 2048
GROUPS = 32
LEVELS = 4
IMAGES = 2
COLUMNS = 256
HEIGHT = 64


def feature_draw(key, rows_all, cols_all, depth_all, salt_code):
    base_key = jax.random.fold_in(key, salt_code)
    subkeys = jax.random.split(base_key, 3)
    relative = (jnp.arange(rows_all, dtype=jnp.float32) + 0.5) / rows_all
    jitter = jnp.exp(jax.random.uniform(subkeys[0], (IMAGES, rows_all), jnp.float32, 0.0, math.log(3.3)))
    row_scale = jnp.exp(math.log(3.0) * relative)[None, :] * jitter
    chan_scale = jnp.exp(jax.random.uniform(subkeys[1], (depth_all,), jnp.float32, -0.5 * math.log(10.0), 0.5 * math.log(10.0)))
    shape_all = (IMAGES, rows_all, cols_all, depth_all)
    values = jnp.clip(jax.random.normal(subkeys[2], shape_all, jnp.float32), -4.0, 4.0)
    return (values * row_scale[:, :, None, None] * chan_scale).astype(jnp.bfloat16)


def draw_level_two(key, part):
    return feature_draw(key, HEIGHT, COLUMNS, DEPTH_TWO, 11)


def draw_level_three(key, part):
    return feature_draw(key, HEIGHT // 2, COLUMNS // 2, DEPTH_THREE, 12)


def draw_level_four(key, part):
    return feature_draw(key, HEIGHT // 4, COLUMNS // 4, DEPTH_FOUR, 13)


def draw_level_five(key, part):
    return feature_draw(key, HEIGHT // 8, COLUMNS // 8, DEPTH_FIVE, 14)


def bell_draw(rng, shape, width, bound, kind=jnp.bfloat16):
    values = jax.random.normal(rng, shape, jnp.float32) * width
    return jnp.minimum(jnp.maximum(values, -bound), bound).astype(kind)


def setup_inputs(seed: int = 0, part: int = 0) -> dict:
    key_of = jax.random.split(jax.random.key(seed), 13)
    own_keys = jax.random.split(jax.random.fold_in(key_of[12], part), 13)
    return {
        "level_two": draw_level_two(jax.random.fold_in(jax.random.fold_in(key_of[12], part), 71), part),
        "level_three": draw_level_three(jax.random.fold_in(jax.random.fold_in(key_of[12], part), 71), part),
        "level_four": draw_level_four(jax.random.fold_in(jax.random.fold_in(key_of[12], part), 71), part),
        "level_five": draw_level_five(jax.random.fold_in(jax.random.fold_in(key_of[12], part), 71), part),
        "lateral_two": bell_draw(key_of[4], (DEPTH_TWO, CHANNELS), DEPTH_TWO ** -0.5, 0.375),
        "lateral_three": bell_draw(key_of[5], (DEPTH_THREE, CHANNELS), DEPTH_THREE ** -0.5, 0.25),
        "lateral_four": bell_draw(key_of[6], (DEPTH_FOUR, CHANNELS), DEPTH_FOUR ** -0.5, 0.1875),
        "lateral_five": bell_draw(key_of[7], (DEPTH_FIVE, CHANNELS), DEPTH_FIVE ** -0.5, 0.125),
        "lateral_bias": bell_draw(key_of[8], (LEVELS, CHANNELS), 1.0, 4.0, jnp.float32),
        "smooth_weight": bell_draw(key_of[9], (LEVELS, 3, 3 * CHANNELS, CHANNELS), (9 * CHANNELS) ** -0.5, 0.125),
        "norm_gain": jnp.clip(1.0 + 0.1 * jax.random.normal(key_of[10], (LEVELS, CHANNELS), jnp.float32), 0.5, 1.5),
        "norm_shift": bell_draw(key_of[11], (LEVELS, CHANNELS), 0.5, 2.0, jnp.float32),
    }


epsilon = 1e-05

def refine(widened, axis_pos):
    length = widened.shape[axis_pos] - 2
    before = lax.slice_in_dim(widened, 0, length, axis=axis_pos)
    middle = lax.slice_in_dim(widened, 1, length + 1, axis=axis_pos)
    beyond = lax.slice_in_dim(widened, 2, length + 2, axis=axis_pos)
    even_rows = 0.25 * before + 0.75 * middle
    odd_rows = 0.75 * middle + 0.25 * beyond
    stacked = jnp.stack([even_rows, odd_rows], axis_pos + 1)
    new_shape = list(widened.shape)
    new_shape[axis_pos] = 2 * length
    return stacked.reshape(new_shape)

def edge_columns(values):
    return jnp.concatenate([values[:, :, :1], values, values[:, :, -1:]], 2)

def lateral(feature, weight, bias_row):
    flattened = feature.reshape(-1, feature.shape[-1])
    result = jnp.dot(flattened, weight, preferred_element_type=jnp.float32) + bias_row
    return result.reshape(feature.shape[:-1] + (weight.shape[1],))

def conv_three(widened, weight):
    padded = jnp.pad(widened, ((0, 0), (0, 0), (1, 1), (0, 0)))
    strip_rows = widened.shape[1] - 2
    width_cells = widened.shape[2]
    channels = widened.shape[3]
    result = jnp.zeros((widened.shape[0] * strip_rows * width_cells, weight.shape[2]), jnp.float32)
    for tap_row in range(3):
        band_rows = padded[:, tap_row:tap_row + strip_rows]
        stacked = jnp.concatenate([band_rows[:, :, 0:width_cells], band_rows[:, :, 1:width_cells + 1], band_rows[:, :, 2:width_cells + 2]], 3)
        result = result + jnp.dot(stacked.reshape(-1, 3 * channels), weight[tap_row], preferred_element_type=jnp.float32)
    return result.reshape(widened.shape[0], strip_rows, width_cells, weight.shape[2])

def group_sums(conv_out):
    dims_all = conv_out.shape
    grouped = conv_out.reshape(dims_all[0], -1, GROUPS, dims_all[3] // GROUPS)
    return (lax.optimization_barrier(jnp.sum(grouped, axis=(1, 3))), lax.optimization_barrier(jnp.sum(grouped * grouped, axis=(1, 3))))

def normalize(conv_out, totals, squares, entries, gain_row, shift_row):
    mean_val = totals / entries
    variance = squares / entries - mean_val * mean_val
    scale_inv = lax.rsqrt(variance + epsilon)
    dims_all = conv_out.shape
    grouped = conv_out.reshape(dims_all[0], dims_all[1], dims_all[2], GROUPS, dims_all[3] // GROUPS)
    centred = (grouped - mean_val[:, None, None, :, None]) * scale_inv[:, None, None, :, None]
    return (centred.reshape(dims_all) * gain_row + shift_row).astype(jnp.bfloat16)

def reference(level_two, level_three, level_four, level_five, lateral_two, lateral_three, lateral_four, lateral_five, lateral_bias, smooth_weight, norm_gain, norm_shift):
    features = (level_two, level_three, level_four, level_five)
    weights = (lateral_two, lateral_three, lateral_four, lateral_five)
    laterals = [lateral(features[level_idx], weights[level_idx], lateral_bias[level_idx]) for level_idx in range(4)]
    merged_maps = [None, None, None, None]
    merged_maps[3] = laterals[3].astype(jnp.bfloat16)
    for level_idx in (2, 1, 0):
        coarse = merged_maps[level_idx + 1].astype(jnp.float32)
        widened = jnp.concatenate([coarse[:, :1], coarse, coarse[:, -1:]], 1)
        upsampled = refine(edge_columns(refine(widened, 1)), 2)
        merged_maps[level_idx] = (laterals[level_idx] + upsampled).astype(jnp.bfloat16)
    outputs = []
    for level_idx in range(4):
        widened = jnp.pad(merged_maps[level_idx], ((0, 0), (1, 1), (0, 0), (0, 0)))
        conv_out = conv_three(widened, smooth_weight[level_idx])
        totals, squares = group_sums(conv_out)
        entries = float(conv_out.shape[1] * conv_out.shape[2] * (conv_out.shape[3] // GROUPS))
        outputs.append(normalize(conv_out, totals, squares, entries, norm_gain[level_idx], norm_shift[level_idx]))
    return (outputs[0], outputs[1], outputs[2], outputs[3])
```

```python
import functools

import jax
import jax.numpy as jnp
from jax import lax
from jax.experimental import pallas as pl
from jax.experimental.pallas import tpu as pltpu
from jax.sharding import PartitionSpec as P

GROUPS = 32
EPSILON = 1e-05
F32 = jnp.float32
BF16 = jnp.bfloat16
MESH = pl.DeviceIdType.MESH
KERNEL_BYTES = 52 * 1024 * 1024
LANES = 128


def bilinear(cols):
    half = cols // 2
    fine = lax.broadcasted_iota(jnp.int32, (cols, cols), 0)
    coarse = lax.broadcasted_iota(jnp.int32, (cols, cols), 1)
    second = coarse >= half
    coarse = jnp.where(second, coarse - half, coarse)
    near = fine // 2
    odd = fine % 2 == 1
    far = jnp.where(odd, jnp.minimum(near + 1, half - 1), jnp.maximum(near - 1, 0))
    value = jnp.where(coarse == near, 0.75, 0.0) + jnp.where(coarse == far, 0.25, 0.0)
    odd_rows = value * jnp.where(second, 0.25, 0.75)
    even_rows = value * jnp.where(second, 0.75, 0.25)
    return odd_rows.astype(BF16), even_rows.astype(BF16)


def mm(a, b):
    return jnp.dot(a, b, preferred_element_type=F32)


def group_totals(value, size):
    parts = []
    for start in range(0, value.shape[1], LANES):
        part = value[:, start : start + LANES]
        lane = lax.broadcasted_iota(jnp.int32, part.shape, 1)
        step = 1
        while step < size:
            upper = (lane // step) % 2 == 1
            other = jnp.where(
                upper, pltpu.roll(part, step, 1), pltpu.roll(part, LANES - step, 1)
            )
            part = part + other
            step *= 2
        parts.append(part)
    return jnp.concatenate(parts, 1)


def kernel(n, geom, *refs):
    images, chans = geom["images"], geom["chans"]
    rows, cols = geom["rows"], geom["cols"]
    it = iter(refs)
    take = lambda count: [next(it) for _ in range(count)]
    feat_hbm, lat_hbm = take(4), take(4)
    bias_hbm, smooth_hbm, gain_hbm, shift_hbm = take(4)
    (conv_two,) = take(1)
    done = [None] + take(3)
    (affine,) = take(1)
    feat, lat_w = take(4), take(4)
    bias, smooth, gain, shift = take(4)
    big, sends, recvs, lats = take(4), [None] + take(3), take(4), take(3)
    conv = [conv_two] + take(3)
    ups, edge, hang = take(3), [None] + take(3), take(1)[0]
    stat_two, stat_rest, got_two, got_rest = take(4)
    in_sem, w_sem, s_sem, p_sem = take(4)
    halo_send, halo_recv, two_send, two_recv, rest_send, rest_recv = take(6)

    me = lax.axis_index("rows")
    first, last = me == 0, me == n - 1
    size = chans // GROUPS

    feat_copy = [pltpu.make_async_copy(feat_hbm[k], feat[k], in_sem.at[k]) for k in range(4)]
    lat_copy = [pltpu.make_async_copy(lat_hbm[k], lat_w[k], w_sem.at[k]) for k in range(4)]
    smooth_copy = [
        pltpu.make_async_copy(smooth_hbm.at[k], smooth.at[k], s_sem.at[k]) for k in range(4)
    ]
    small_copy = [
        pltpu.make_async_copy(src, dst, p_sem.at[j])
        for j, (src, dst) in enumerate(((bias_hbm, bias), (gain_hbm, gain), (shift_hbm, shift)))
    ]
    feat_copy[3].start()
    lat_copy[3].start()
    small_copy[0].start()
    barrier = pltpu.get_barrier_semaphore()
    for d in range(1, n):
        pl.semaphore_signal(
            barrier, inc=1, device_id={"rows": lax.rem(me + d, n)}, device_id_type=MESH
        )
    for k in (2, 1, 0):
        lat_copy[k].start()
        feat_copy[k].start()
    for k in (3, 2, 0, 1):
        smooth_copy[k].start()
    small_copy[1].start()
    small_copy[2].start()

    for k in range(3):
        odd, even = bilinear(cols[k])
        ups[k][0 : cols[k]] = odd
        ups[k][cols[k] :] = even

    def halo_source(k, way):
        if k == 0:
            return feat[0].at[:, way * (rows[0] - 1)]
        return sends[k].at[way * (sends[k].shape[0] - 1)]

    def halo_copy(k, way):
        return pltpu.make_async_remote_copy(
            src_ref=halo_source(k, way),
            dst_ref=recvs[k].at[1 - way],
            send_sem=halo_send.at[k, way],
            recv_sem=halo_recv.at[k, 1 - way],
            device_id={"rows": lax.rem(me + (1 if way else n - 1), n)},
            device_id_type=MESH,
        )

    def halo_start(k):
        @pl.when(jnp.logical_not(first))
        def _():
            halo_copy(k, 0).start()

        @pl.when(jnp.logical_not(last))
        def _():
            halo_copy(k, 1).start()

    def halo_wait(k):
        @pl.when(jnp.logical_not(last))
        def _():
            halo_copy(k, 0).wait_recv()

        @pl.when(jnp.logical_not(first))
        def _():
            halo_copy(k, 1).wait_recv()

    def sent_wait(k):
        @pl.when(jnp.logical_not(first))
        def _():
            halo_copy(k, 0).wait_send()

        @pl.when(jnp.logical_not(last))
        def _():
            halo_copy(k, 1).wait_send()

    small_copy[0].wait()
    feat_copy[3].wait()
    lat_copy[3].wait()
    five = mm(feat[3][...].reshape(-1, feat[3].shape[-1]), lat_w[3][...]) + bias[3:4, :]
    five = five.reshape(images, rows[3], cols[3], chans)
    for y in range(rows[3]):
        sends[3][y] = five[:, y].astype(BF16)
    pl.semaphore_wait(barrier, n - 1)
    halo_start(3)

    lat_copy[2].wait()
    feat_copy[2].wait()
    four = mm(feat[2][...].reshape(-1, feat[2].shape[-1]), lat_w[2][...]) + bias[2:3, :]
    four = four.reshape(images, rows[2], cols[2], chans)
    for y in range(rows[2]):
        lats[2][y] = four[:, y]
    for way, y in ((0, 0), (1, rows[2] - 1)):
        sends[2][way] = four[:, y].astype(BF16)
    halo_start(2)

    lat_copy[1].wait()
    feat_copy[1].wait()
    for y in [0, rows[1] - 1] + list(range(1, rows[1] - 1)):
        for i in range(images):
            value = mm(feat[1][i, y], lat_w[1][...]) + bias[1:2, :]
            lats[1][y, i] = value
            if y in (0, rows[1] - 1):
                sends[1][0 if y == 0 else 1, i] = value.astype(BF16)
        if y == rows[1] - 1:
            halo_start(1)

    lat_copy[0].wait()
    feat_copy[0].wait()
    halo_start(0)
    for y in range(0, rows[0], 2):
        for i in range(images):
            flat = feat[0][i, y : y + 2].reshape(2 * cols[0], -1)
            value = mm(flat, lat_w[0][...]) + bias[0:1, :]
            lats[0][y, i] = value[: cols[0]]
            lats[0][y + 1, i] = value[cols[0] :]

    def put(k, r, i, value):
        width = cols[k]
        spot = lax.broadcasted_iota(jnp.int32, (8, chans), 0)
        before = pltpu.roll(value, 1, 0)
        beyond = pltpu.roll(value, width - 1, 0)
        before = jnp.concatenate([jnp.where(spot == 0, 0.0, before[:8]), before[8:]], 0)
        beyond = jnp.concatenate(
            [beyond[: width - 8], jnp.where(spot == 7, 0.0, beyond[width - 8 :])], 0
        )
        big[k][r, i, :, 0:chans] = before.astype(BF16)
        big[k][r, i, :, chans : 2 * chans] = value.astype(BF16)
        big[k][r, i, :, 2 * chans :] = beyond.astype(BF16)

    def center(k, r, i):
        return big[k][r, i, :, chans : 2 * chans]

    def borders(k, i, above, below):
        if k:
            edge[k][0, i] = jnp.where(first, center(k, 1, i), above.astype(BF16))
            edge[k][1, i] = jnp.where(last, center(k, rows[k], i), below.astype(BF16))
        put(k, 0, i, jnp.where(first, 0.0, above))
        put(k, rows[k] + 1, i, jnp.where(last, 0.0, below))

    def pair(k, p, i):
        upper = edge[k][0, i] if p == 0 else center(k, p, i)
        lower = edge[k][1, i] if p == rows[k] else center(k, p + 1, i)
        return jnp.concatenate([upper, lower], 0)

    def conv_rows(k, y, count):
        bands = [
            big[k][y + a : y + a + count].reshape(count * images * cols[k], 3 * chans)
            for a in range(3)
        ]
        total = mm(jnp.concatenate(bands, 1), smooth[k])
        total = total.reshape(count, images, cols[k], chans)
        sums = []
        for i in range(images):
            part = total[:, i].reshape(-1, 8, chans)
            conv[k][i, y : y + count] = total[:, i]
            sums.append((jnp.sum(part, 0), jnp.sum(part * part, 0)))
        return sums

    def joined(parts):
        total = parts[0]
        for part in parts[1:]:
            total = [(t[0] + u[0], t[1] + u[1]) for t, u in zip(total, part)]
        return total

    def write_sums(dst, start, sums):
        for i in range(images):
            for j in range(2):
                slot = start + 2 * i + j
                dst[slot : slot + 1, :] = jnp.sum(sums[i][j], 0, keepdims=True)

    def spread(mine, got, send_sem, recv_sem):
        return [
            pltpu.make_async_remote_copy(
                src_ref=mine,
                dst_ref=got.at[d],
                send_sem=send_sem.at[d],
                recv_sem=recv_sem.at[d],
                device_id={"rows": lax.rem(me + d, n)},
                device_id_type=MESH,
            )
            for d in range(1, n)
        ]

    stat_rest[...] = jnp.zeros_like(stat_rest)
    stat_two[...] = jnp.zeros_like(stat_two)

    for i in range(images):
        for y in range(rows[3]):
            put(3, y + 1, i, five[i, y])
    halo_wait(3)
    for i in range(images):
        borders(3, i, recvs[3][0, i].astype(F32), recvs[3][1, i].astype(F32))

    outer = {}
    for i in range(images):
        for p in range(rows[3] + 1):
            both = mm(ups[2][...], pair(3, p, i))
            for y, value in ((2 * p - 1, both[: cols[2]]), (2 * p, both[cols[2] :])):
                if 0 <= y < rows[2]:
                    put(2, y + 1, i, lats[2][y, i] + value)
                else:
                    outer[y, i] = value
    smooth_copy[3].wait()
    sums_five = conv_rows(3, 0, rows[3])
    halo_wait(2)
    for i in range(images):
        borders(
            2,
            i,
            recvs[2][0, i].astype(F32) + outer[-1, i],
            recvs[2][1, i].astype(F32) + outer[rows[2], i],
        )

    for p in [*range(1, rows[2]), 0, rows[2]]:
        for i in range(images):
            both = mm(ups[1][...], pair(2, p, i))
            for y, value in ((2 * p - 1, both[: cols[1]]), (2 * p, both[cols[1] :])):
                if 0 <= y < rows[1]:
                    put(1, y + 1, i, lats[1][y, i] + value)
                else:
                    hang[0 if y < 0 else 1, i] = value

    def merge_two(p):
        for i in range(images):
            both = mm(ups[0][...], pair(1, p, i))
            put(0, 2 * p, i, lats[0][2 * p - 1, i] + both[: cols[0]])
            put(0, 2 * p + 1, i, lats[0][2 * p, i] + both[cols[0] :])

    middle = list(range(1, rows[1]))
    merge_two(middle[0])
    smooth_copy[2].wait()
    sums_four = conv_rows(2, 0, rows[2])
    for p in middle[1:2]:
        merge_two(p)
    smooth_copy[0].wait()
    smooth_copy[1].wait()
    sums_two, sums_three = [], []
    sums_three.append(conv_rows(1, 1, rows[1] - 2))
    merged = 2
    for y in range(2, rows[0] - 2):
        while merged < len(middle) and middle[merged - 1] < (y + 2) // 2:
            merge_two(middle[merged])
            merged += 1
        sums_two.append(conv_rows(0, y, 1))

    halo_wait(1)
    for i in range(images):
        borders(
            1,
            i,
            recvs[1][0, i].astype(F32) + hang[0, i],
            recvs[1][1, i].astype(F32) + hang[1, i],
        )
    for i in range(images):
        put(0, 1, i, lats[0][0, i] + mm(ups[0][cols[0] :], pair(1, 0, i)))
        put(0, rows[0], i, lats[0][rows[0] - 1, i] + mm(ups[0][: cols[0]], pair(1, rows[1], i)))
    for y in (0, rows[1] - 1):
        sums_three.append(conv_rows(1, y, 1))
    for start, sums in ((0, sums_three), (1, [sums_four]), (2, [sums_five])):
        write_sums(stat_rest, start * images * 2, joined(sums))
    rest_copies = spread(stat_rest, got_rest, rest_send, rest_recv)
    for copy in rest_copies:
        copy.start()
    for y in (1, rows[0] - 2):
        sums_two.append(conv_rows(0, y, 1))

    halo_wait(0)
    for i in range(images):
        above = mm(
            jnp.concatenate([recvs[0][0, i], ups[0][: cols[0]]], 1),
            jnp.concatenate([lat_w[0][...], pair(1, 0, i)], 0),
        )
        below = mm(
            jnp.concatenate([recvs[0][1, i], ups[0][cols[0] :]], 1),
            jnp.concatenate([lat_w[0][...], pair(1, rows[1], i)], 0),
        )
        borders(0, i, above + bias[0:1, :], below + bias[0:1, :])
    for y in (0, rows[0] - 1):
        sums_two.append(conv_rows(0, y, 1))
    write_sums(stat_two, 0, joined(sums_two))
    two_copies = spread(stat_two, got_two, two_send, two_recv)
    for copy in two_copies:
        copy.start()

    def gathered(mine, got):
        total = mine[...]
        for d in range(1, n):
            total = total + got[d]
        return group_totals(total, size)

    def scales(k, total, square):
        entries = float(rows[k] * n * cols[k] * size)
        mean = total / entries
        variance = square / entries - mean * mean
        scale = lax.rsqrt(variance + EPSILON) * gain[k : k + 1, :]
        return scale, shift[k : k + 1, :] - mean * scale

    small_copy[1].wait()
    small_copy[2].wait()
    for copy in rest_copies:
        copy.wait_recv()
    rest = gathered(stat_rest, got_rest)
    for k in (1, 2, 3):
        for i in range(images):
            slot = ((k - 1) * images + i) * 2
            scale, offset = scales(k, rest[slot : slot + 1], rest[slot + 1 : slot + 2])
            done[k][i] = (conv[k][i] * scale + offset).astype(BF16)

    for copy in two_copies:
        copy.wait_recv()
    two = gathered(stat_two, got_two)
    for i in range(images):
        scale, offset = scales(0, two[2 * i : 2 * i + 1], two[2 * i + 1 : 2 * i + 2])
        affine[2 * i : 2 * i + 1, :] = scale
        affine[2 * i + 1 : 2 * i + 2, :] = offset
    for k in range(4):
        sent_wait(k)
    for copy in two_copies + rest_copies:
        copy.wait_send()


def finish_kernel(geom, *refs):
    images, rows = geom["images"], geom["rows"]
    conv_two, affine = refs[0:2]
    done = [None, *refs[2:5]]
    out_hbm, staged, rest_sem, two_sem = refs[5:9], refs[9], refs[10], refs[11]
    copies = []
    for k in (1, 2, 3):
        copies.append(pltpu.make_async_copy(done[k], out_hbm[k], rest_sem.at[k]))
        copies[-1].start()
    for i in range(images):
        scale = affine[2 * i : 2 * i + 1, :]
        offset = affine[2 * i + 1 : 2 * i + 2, :]
        for y in range(rows[0]):
            staged[i, y] = (conv_two[i, y] * scale + offset).astype(BF16)
            copies.append(
                pltpu.make_async_copy(staged.at[i, y], out_hbm[0].at[i, y], two_sem.at[i, y])
            )
            copies[-1].start()
    for copy in copies:
        copy.wait()


def per_device(n, *args):
    feats, lat_ws = args[0:4], args[4:8]
    bias, smooth, gain, shift = args[8:12]
    smooth = smooth.reshape(smooth.shape[0], -1, smooth.shape[3])
    images, chans = feats[0].shape[0], lat_ws[0].shape[1]
    rows = [f.shape[1] for f in feats]
    cols = [f.shape[2] for f in feats]
    geom = {"images": images, "chans": chans, "rows": rows, "cols": cols}
    any_spec = pl.BlockSpec(memory_space=pltpu.HBM)
    vmem_spec = pl.BlockSpec(memory_space=pltpu.VMEM)
    outs = [jax.ShapeDtypeStruct((images, r, c, chans), BF16) for r, c in zip(rows, cols)]
    dma = pltpu.SemaphoreType.DMA
    rest_rows = -(-(3 * images * 2) // 8) * 8
    two_rows = -(-(images * 2) // 8) * 8
    strip = lambda k, count, width, kind: pltpu.VMEM((count, images, cols[k], width), kind)
    scratch = (
        [pltpu.VMEM(f.shape, BF16) for f in feats]
        + [pltpu.VMEM(w.shape, BF16) for w in lat_ws]
        + [pltpu.VMEM(bias.shape, F32), pltpu.VMEM(smooth.shape, BF16)]
        + [pltpu.VMEM(gain.shape, F32), pltpu.VMEM(shift.shape, F32)]
        + [strip(k, rows[k] + 2, 3 * chans, BF16) for k in range(4)]
        + [strip(k, min(rows[k], 2), chans, BF16) for k in range(1, 4)]
        + [strip(k, 2, chans, BF16) for k in range(4)]
        + [strip(k, rows[k], chans, F32) for k in range(3)]
        + [pltpu.VMEM(o.shape, F32) for o in outs[1:]]
        + [pltpu.VMEM((2 * c, c), BF16) for c in cols[:3]]
        + [strip(k, 2, chans, BF16) for k in range(1, 4)]
        + [strip(1, 2, chans, F32)]
        + [
            pltpu.VMEM((two_rows, chans), F32),
            pltpu.VMEM((rest_rows, chans), F32),
            pltpu.VMEM((n, two_rows, chans), F32),
            pltpu.VMEM((n, rest_rows, chans), F32),
        ]
        + [dma((4,)), dma((4,)), dma((4,)), dma((3,))]
        + [dma((4, 2)), dma((4, 2)), dma((n,)), dma((n,)), dma((n,)), dma((n,))]
    )
    held = pl.pallas_call(
        functools.partial(kernel, n, geom),
        out_shape=[pltpu.VMEM(outs[0].shape, F32)]
        + [pltpu.VMEM(o.shape, BF16) for o in outs[1:]]
        + [pltpu.VMEM((two_rows, chans), F32)],
        in_specs=[any_spec] * 12,
        out_specs=[vmem_spec] * 5,
        scratch_shapes=scratch,
        compiler_params=pltpu.CompilerParams(
            collective_id=0, has_side_effects=True, vmem_limit_bytes=KERNEL_BYTES
        ),
    )(*args[:9], smooth, gain, shift)
    held = [pltpu.with_memory_space_constraint(h, pltpu.VMEM) for h in held]
    return pl.pallas_call(
        functools.partial(finish_kernel, geom),
        out_shape=outs,
        in_specs=[vmem_spec] * 5,
        out_specs=[any_spec] * 4,
        scratch_shapes=[pltpu.VMEM(outs[0].shape, BF16), dma((4,)), dma((images, rows[0]))],
        compiler_params=pltpu.CompilerParams(vmem_limit_bytes=16 * 1024 * 1024),
    )(held[0], held[4], *held[1:4])


def solution(mesh):
    strips = P("batch", "rows", None, None)
    run = functools.partial(per_device, mesh.shape["rows"])
    return jax.shard_map(
        lambda *args: tuple(run(*args)),
        mesh=mesh,
        in_specs=(strips,) * 4 + (P(),) * 8,
        out_specs=(strips,) * 4,
        check_vma=False,
    )
```

```python
import functools

import jax
import jax.numpy as jnp
from jax import lax
from jax.experimental import pallas as pl
from jax.experimental.pallas import tpu as pltpu
from jax.sharding import PartitionSpec as P

GROUPS = 32
EPSILON = 1e-05
F32 = jnp.float32
BF16 = jnp.bfloat16
MESH = pl.DeviceIdType.MESH
KERNEL_BYTES = 52 * 1024 * 1024
LANES = 128


def bilinear(cols):
    half = cols // 2
    fine = lax.broadcasted_iota(jnp.int32, (cols, cols), 0)
    coarse = lax.broadcasted_iota(jnp.int32, (cols, cols), 1)
    second = coarse >= half
    coarse = jnp.where(second, coarse - half, coarse)
    near = fine // 2
    odd = fine % 2 == 1
    far = jnp.where(odd, jnp.minimum(near + 1, half - 1), jnp.maximum(near - 1, 0))
    value = jnp.where(coarse == near, 0.75, 0.0) + jnp.where(coarse == far, 0.25, 0.0)
    odd_rows = value * jnp.where(second, 0.25, 0.75)
    even_rows = value * jnp.where(second, 0.75, 0.25)
    return odd_rows.astype(BF16), even_rows.astype(BF16)


def mm(a, b):
    return jnp.dot(a, b, preferred_element_type=F32)


def mm_halves(a, b, step):
    cut = -(-(a.shape[1] // step) // 2) * step
    return mm(a[:, :cut], b[:cut]) + mm(a[:, cut:], b[cut:])


def group_totals(value, size):
    parts = []
    for start in range(0, value.shape[1], LANES):
        part = value[:, start : start + LANES]
        lane = lax.broadcasted_iota(jnp.int32, part.shape, 1)
        step = 1
        while step < size:
            upper = (lane // step) % 2 == 1
            other = jnp.where(
                upper, pltpu.roll(part, step, 1), pltpu.roll(part, LANES - step, 1)
            )
            part = part + other
            step *= 2
        parts.append(part)
    return jnp.concatenate(parts, 1)


def kernel(n, geom, *refs):
    images, chans = geom["images"], geom["chans"]
    rows, cols = geom["rows"], geom["cols"]
    it = iter(refs)
    take = lambda count: [next(it) for _ in range(count)]
    feat_hbm, lat_hbm = take(4), take(4)
    bias_hbm, smooth_hbm, gain_hbm, shift_hbm = take(4)
    (conv_two,) = take(1)
    done = [None] + take(3)
    (affine,) = take(1)
    feat, lat_w = take(4), take(4)
    bias, smooth, gain, shift = take(4)
    big, sends, recvs, lats = take(4), [None] + take(3), take(4), take(3)
    conv = [conv_two] + take(3)
    ups, edge, hang = take(3), [None] + take(3), take(1)[0]
    stat_two, stat_rest, got_two, got_rest = take(4)
    in_sem, w_sem, s_sem, p_sem = take(4)
    halo_send, halo_recv, two_send, two_recv, rest_send, rest_recv = take(6)

    me = lax.axis_index("rows")
    first, last = me == 0, me == n - 1
    size = chans // GROUPS

    feat_copy = [pltpu.make_async_copy(feat_hbm[k], feat[k], in_sem.at[k]) for k in range(4)]
    lat_copy = [pltpu.make_async_copy(lat_hbm[k], lat_w[k], w_sem.at[k]) for k in range(4)]
    smooth_copy = pltpu.make_async_copy(smooth_hbm, smooth, s_sem.at[0])
    small_copy = [
        pltpu.make_async_copy(src, dst, p_sem.at[j])
        for j, (src, dst) in enumerate(((bias_hbm, bias), (gain_hbm, gain), (shift_hbm, shift)))
    ]
    feat_copy[3].start()
    lat_copy[3].start()
    small_copy[0].start()
    barrier = pltpu.get_barrier_semaphore()
    for d in range(1, n):
        pl.semaphore_signal(
            barrier, inc=1, device_id={"rows": lax.rem(me + d, n)}, device_id_type=MESH
        )
    for k in (2, 1, 0):
        lat_copy[k].start()
        feat_copy[k].start()
    smooth_copy.start()
    small_copy[1].start()
    small_copy[2].start()

    for k in range(3):
        odd, even = bilinear(cols[k])
        ups[k][0 : cols[k]] = odd
        ups[k][cols[k] :] = even

    def halo_source(k, way):
        if k == 0:
            return feat[0].at[:, way * (rows[0] - 1)]
        return sends[k].at[way * (sends[k].shape[0] - 1)]

    def halo_copy(k, way):
        return pltpu.make_async_remote_copy(
            src_ref=halo_source(k, way),
            dst_ref=recvs[k].at[1 - way],
            send_sem=halo_send.at[k, way],
            recv_sem=halo_recv.at[k, 1 - way],
            device_id={"rows": lax.rem(me + (1 if way else n - 1), n)},
            device_id_type=MESH,
        )

    def halo_start(k):
        @pl.when(jnp.logical_not(first))
        def _():
            halo_copy(k, 0).start()

        @pl.when(jnp.logical_not(last))
        def _():
            halo_copy(k, 1).start()

    def halo_wait(k):
        @pl.when(jnp.logical_not(last))
        def _():
            halo_copy(k, 0).wait_recv()

        @pl.when(jnp.logical_not(first))
        def _():
            halo_copy(k, 1).wait_recv()

    def sent_wait(k):
        @pl.when(jnp.logical_not(first))
        def _():
            halo_copy(k, 0).wait_send()

        @pl.when(jnp.logical_not(last))
        def _():
            halo_copy(k, 1).wait_send()

    small_copy[0].wait()
    feat_copy[3].wait()
    lat_copy[3].wait()
    flat = feat[3][...].reshape(-1, feat[3].shape[-1])
    five = mm_halves(flat, lat_w[3], chans) + bias[3:4, :]
    five = five.reshape(images, rows[3], cols[3], chans)
    for y in range(rows[3]):
        sends[3][y] = five[:, y].astype(BF16)
    pl.semaphore_wait(barrier, n - 1)
    halo_start(3)

    lat_copy[2].wait()
    feat_copy[2].wait()
    for i in range(images):
        flat = feat[2][i].reshape(rows[2] * cols[2], -1)
        value = (mm(flat, lat_w[2][...]) + bias[2:3, :]).reshape(rows[2], cols[2], chans)
        for y in range(rows[2]):
            lats[2][y, i] = value[y]
        sends[2][0, i] = value[0].astype(BF16)
        sends[2][1, i] = value[rows[2] - 1].astype(BF16)
    halo_start(2)

    lat_copy[1].wait()
    feat_copy[1].wait()
    def lateral_three(some):
        for i in range(images):
            flat = jnp.concatenate([feat[1][i, y] for y in some], 0)
            value = (mm(flat, lat_w[1][...]) + bias[1:2, :]).reshape(len(some), cols[1], chans)
            for j, y in enumerate(some):
                lats[1][y, i] = value[j]
                if y in (0, rows[1] - 1):
                    sends[1][0 if y == 0 else 1, i] = value[j].astype(BF16)

    lateral_three([0, rows[1] - 1])
    halo_start(1)
    lateral_three(list(range(1, rows[1] - 1)))

    lat_copy[0].wait()
    feat_copy[0].wait()
    halo_start(0)
    for y in range(0, rows[0], 2):
        for i in range(images):
            flat = feat[0][i, y : y + 2].reshape(2 * cols[0], -1)
            value = mm(flat, lat_w[0][...]) + bias[0:1, :]
            lats[0][y, i] = value[: cols[0]]
            lats[0][y + 1, i] = value[cols[0] :]

    def put(k, r, i, value):
        width = cols[k]
        spot = lax.broadcasted_iota(jnp.int32, (8, chans), 0)
        before = pltpu.roll(value, 1, 0)
        beyond = pltpu.roll(value, width - 1, 0)
        before = jnp.concatenate([jnp.where(spot == 0, 0.0, before[:8]), before[8:]], 0)
        beyond = jnp.concatenate(
            [beyond[: width - 8], jnp.where(spot == 7, 0.0, beyond[width - 8 :])], 0
        )
        big[k][r, i, :, 0:chans] = before.astype(BF16)
        big[k][r, i, :, chans : 2 * chans] = value.astype(BF16)
        big[k][r, i, :, 2 * chans :] = beyond.astype(BF16)

    def center(k, r, i):
        return big[k][r, i, :, chans : 2 * chans]

    def borders(k, i, above, below):
        if k:
            edge[k][0, i] = jnp.where(first, center(k, 1, i), above.astype(BF16))
            edge[k][1, i] = jnp.where(last, center(k, rows[k], i), below.astype(BF16))
        put(k, 0, i, jnp.where(first, 0.0, above))
        put(k, rows[k] + 1, i, jnp.where(last, 0.0, below))

    def pair(k, p, i):
        upper = edge[k][0, i] if p == 0 else center(k, p, i)
        lower = edge[k][1, i] if p == rows[k] else center(k, p + 1, i)
        return jnp.concatenate([upper, lower], 0)

    def conv_rows(k, some, split=False):
        sums = []
        if split:
            stacked = [
                jnp.concatenate(
                    [big[k][y + a, i] for y in some for i in range(images)], 0
                )
                for a in range(3)
            ]
            total = mm_halves(jnp.concatenate(stacked, 1), smooth.at[k], chans)
            total = total.reshape(len(some), images, cols[k], chans)
            values = [total[:, i] for i in range(images)]
        else:
            values = []
            for i in range(images):
                stacked = [
                    jnp.concatenate([big[k][y + a, i] for y in some], 0) for a in range(3)
                ]
                total = mm(jnp.concatenate(stacked, 1), smooth[k])
                values.append(total.reshape(len(some), cols[k], chans))
        for i in range(images):
            for j, y in enumerate(some):
                conv[k][i, y] = values[i][j]
            part = values[i].reshape(-1, 8, chans)
            sums.append((jnp.sum(part, 0), jnp.sum(part * part, 0)))
        return sums

    def joined(parts):
        total = parts[0]
        for part in parts[1:]:
            total = [(t[0] + u[0], t[1] + u[1]) for t, u in zip(total, part)]
        return total

    def write_sums(dst, start, sums):
        for i in range(images):
            for j in range(2):
                slot = start + 2 * i + j
                dst[slot : slot + 1, :] = jnp.sum(sums[i][j], 0, keepdims=True)

    def spread(mine, got, send_sem, recv_sem):
        return [
            pltpu.make_async_remote_copy(
                src_ref=mine,
                dst_ref=got.at[d - 1],
                send_sem=send_sem.at[0],
                recv_sem=recv_sem.at[0],
                device_id={"rows": lax.rem(me + d, n)},
                device_id_type=MESH,
            )
            for d in range(1, n)
        ]

    def all_of(got, sem):
        pltpu.make_async_copy(got, got, sem.at[0]).wait()

    stat_rest[...] = jnp.zeros_like(stat_rest)
    stat_two[...] = jnp.zeros_like(stat_two)

    smooth_copy.wait()

    for i in range(images):
        for y in range(rows[3]):
            put(3, y + 1, i, five[i, y])
    halo_wait(3)
    for i in range(images):
        borders(3, i, recvs[3][0, i].astype(F32), recvs[3][1, i].astype(F32))

    outer = {}
    for p in range(rows[3] + 1):
        for i in range(images):
            both = mm(ups[2][...], pair(3, p, i))
            for y, value in ((2 * p - 1, both[: cols[2]]), (2 * p, both[cols[2] :])):
                if 0 <= y < rows[2]:
                    put(2, y + 1, i, lats[2][y, i] + value)
                else:
                    outer[y, i] = value
    halo_wait(2)
    for i in range(images):
        borders(
            2,
            i,
            recvs[2][0, i].astype(F32) + outer[-1, i],
            recvs[2][1, i].astype(F32) + outer[rows[2], i],
        )

    def merge_three(p):
        for i in range(images):
            both = mm(ups[1][...], pair(2, p, i))
            for y, value in ((2 * p - 1, both[: cols[1]]), (2 * p, both[cols[1] :])):
                if 0 <= y < rows[1]:
                    put(1, y + 1, i, lats[1][y, i] + value)
                else:
                    hang[0 if y < 0 else 1, i] = value

    def merge_two(p):
        for i in range(images):
            both = mm(ups[0][...], pair(1, p, i))
            put(0, 2 * p, i, lats[0][2 * p - 1, i] + both[: cols[0]])
            put(0, 2 * p + 1, i, lats[0][2 * p, i] + both[cols[0] :])

    for p in range(1, rows[2]):
        merge_three(p)
    sums_five = conv_rows(3, list(range(rows[3])), True)
    merge_three(0)
    merge_three(rows[2])
    merge_two(1)
    sums_four = conv_rows(2, list(range(rows[2])))
    sums_three = [conv_rows(1, list(range(1, rows[1] - 1)))]
    merged, sums_two = 1, []

    def conv_two_row(y):
        nonlocal merged
        while merged < min((y + 2) // 2, rows[1] - 1):
            merged += 1
            merge_two(merged)
        sums_two.append(conv_rows(0, [y]))

    inner = list(range(2, rows[0] - 2))
    for y in inner[: len(inner) // 2]:
        conv_two_row(y)

    halo_wait(1)
    for i in range(images):
        borders(
            1,
            i,
            recvs[1][0, i].astype(F32) + hang[0, i],
            recvs[1][1, i].astype(F32) + hang[1, i],
        )
    for i in range(images):
        put(0, 1, i, lats[0][0, i] + mm(ups[0][cols[0] :], pair(1, 0, i)))
    for i in range(images):
        put(0, rows[0], i, lats[0][rows[0] - 1, i] + mm(ups[0][: cols[0]], pair(1, rows[1], i)))
    for y in inner[len(inner) // 2 :]:
        conv_two_row(y)
    sums_three.append(conv_rows(1, [0, rows[1] - 1]))
    for start, sums in ((0, sums_three), (1, [sums_four]), (2, [sums_five])):
        write_sums(stat_rest, start * images * 2, joined(sums))
    conv_two_row(1)
    conv_two_row(rows[0] - 2)

    rest_copies = spread(stat_rest, got_rest, rest_send, rest_recv)
    for copy in rest_copies:
        copy.start()
    halo_wait(0)
    sides = []
    for way, half, p in ((0, ups[0][: cols[0]], 0), (1, ups[0][cols[0] :], rows[1])):
        for i in range(images):
            sides.append(
                mm(
                    jnp.concatenate([recvs[0][way, i], half], 1),
                    jnp.concatenate([lat_w[0][...], pair(1, p, i)], 0),
                )
                + bias[0:1, :]
            )
    for i in range(images):
        borders(0, i, sides[i], sides[images + i])
    conv_two_row(0)
    conv_two_row(rows[0] - 1)
    write_sums(stat_two, 0, joined(sums_two))
    two_copies = spread(stat_two, got_two, two_send, two_recv)
    for copy in two_copies:
        copy.start()

    def gathered(mine, got):
        total = mine[...]
        for d in range(n - 1):
            total = total + got[d]
        return group_totals(total, size)

    def scales(k, total, square):
        share = 1.0 / float(rows[k] * n * cols[k] * size)
        mean = total * share
        variance = square * share - mean * mean
        scale = lax.rsqrt(variance + EPSILON) * gain[k : k + 1, :]
        return scale, shift[k : k + 1, :] - mean * scale

    small_copy[1].wait()
    small_copy[2].wait()
    all_of(got_rest, rest_recv)
    rest = gathered(stat_rest, got_rest)
    for k in (1, 2, 3):
        for i in range(images):
            slot = ((k - 1) * images + i) * 2
            scale, offset = scales(k, rest[slot : slot + 1], rest[slot + 1 : slot + 2])
            done[k][i] = (conv[k][i] * scale + offset).astype(BF16)

    all_of(got_two, two_recv)
    two = gathered(stat_two, got_two)
    for i in range(images):
        scale, offset = scales(0, two[2 * i : 2 * i + 1], two[2 * i + 1 : 2 * i + 2])
        affine[2 * i : 2 * i + 1, :] = scale
        affine[2 * i + 1 : 2 * i + 2, :] = offset
    for k in range(4):
        sent_wait(k)
    all_of(got_rest, rest_send)
    all_of(got_two, two_send)


def finish_kernel(geom, *refs):
    images, rows = geom["images"], geom["rows"]
    conv_two, affine = refs[0:2]
    done = [None, *refs[2:5]]
    out_hbm, staged, rest_sem, two_sem = refs[5:9], refs[9], refs[10], refs[11]
    copies = []
    for k in (1, 2, 3):
        copies.append(pltpu.make_async_copy(done[k], out_hbm[k], rest_sem.at[k]))
        copies[-1].start()
    for i in range(images):
        scale = affine[2 * i : 2 * i + 1, :]
        offset = affine[2 * i + 1 : 2 * i + 2, :]
        for y in range(rows[0]):
            staged[i, y] = (conv_two[i, y] * scale + offset).astype(BF16)
            pltpu.make_async_copy(
                staged.at[i, y], out_hbm[0].at[i, y], two_sem.at[0]
            ).start()
    for copy in copies:
        copy.wait()
    pltpu.make_async_copy(staged, out_hbm[0], two_sem.at[0]).wait()


def per_device(n, *args):
    feats, lat_ws = args[0:4], args[4:8]
    bias, smooth, gain, shift = args[8:12]
    smooth = smooth.reshape(smooth.shape[0], -1, smooth.shape[3])
    images, chans = feats[0].shape[0], lat_ws[0].shape[1]
    rows = [f.shape[1] for f in feats]
    cols = [f.shape[2] for f in feats]
    geom = {"images": images, "chans": chans, "rows": rows, "cols": cols}
    any_spec = pl.BlockSpec(memory_space=pltpu.HBM)
    vmem_spec = pl.BlockSpec(memory_space=pltpu.VMEM)
    outs = [jax.ShapeDtypeStruct((images, r, c, chans), BF16) for r, c in zip(rows, cols)]
    dma = pltpu.SemaphoreType.DMA
    rest_rows = -(-(3 * images * 2) // 8) * 8
    two_rows = -(-(images * 2) // 8) * 8
    strip = lambda k, count, width, kind: pltpu.VMEM((count, images, cols[k], width), kind)
    scratch = (
        [pltpu.VMEM(f.shape, BF16) for f in feats]
        + [pltpu.VMEM(w.shape, BF16) for w in lat_ws]
        + [pltpu.VMEM(bias.shape, F32), pltpu.VMEM(smooth.shape, BF16)]
        + [pltpu.VMEM(gain.shape, F32), pltpu.VMEM(shift.shape, F32)]
        + [strip(k, rows[k] + 2, 3 * chans, BF16) for k in range(4)]
        + [strip(k, min(rows[k], 2), chans, BF16) for k in range(1, 4)]
        + [strip(k, 2, chans, BF16) for k in range(4)]
        + [strip(k, rows[k], chans, F32) for k in range(3)]
        + [pltpu.VMEM(o.shape, F32) for o in outs[1:]]
        + [pltpu.VMEM((2 * c, c), BF16) for c in cols[:3]]
        + [strip(k, 2, chans, BF16) for k in range(1, 4)]
        + [strip(1, 2, chans, F32)]
        + [
            pltpu.VMEM((two_rows, chans), F32),
            pltpu.VMEM((rest_rows, chans), F32),
            pltpu.VMEM((n - 1, two_rows, chans), F32),
            pltpu.VMEM((n - 1, rest_rows, chans), F32),
        ]
        + [dma((4,)), dma((4,)), dma((1,)), dma((3,))]
        + [dma((4, 2)), dma((4, 2)), dma((1,)), dma((1,)), dma((1,)), dma((1,))]
    )
    held = pl.pallas_call(
        functools.partial(kernel, n, geom),
        out_shape=[pltpu.VMEM(outs[0].shape, F32)]
        + [pltpu.VMEM(o.shape, BF16) for o in outs[1:]]
        + [pltpu.VMEM((two_rows, chans), F32)],
        in_specs=[any_spec] * 12,
        out_specs=[vmem_spec] * 5,
        scratch_shapes=scratch,
        compiler_params=pltpu.CompilerParams(
            collective_id=0, has_side_effects=True, vmem_limit_bytes=KERNEL_BYTES
        ),
    )(*args[:9], smooth, gain, shift)
    held = [pltpu.with_memory_space_constraint(h, pltpu.VMEM) for h in held]
    return pl.pallas_call(
        functools.partial(finish_kernel, geom),
        out_shape=outs,
        in_specs=[vmem_spec] * 5,
        out_specs=[any_spec] * 4,
        scratch_shapes=[pltpu.VMEM(outs[0].shape, BF16), dma((4,)), dma((1,))],
        compiler_params=pltpu.CompilerParams(vmem_limit_bytes=16 * 1024 * 1024),
    )(held[0], held[4], *held[1:4])


def solution(mesh):
    strips = P("batch", "rows", None, None)
    run = functools.partial(per_device, mesh.shape["rows"])
    return jax.shard_map(
        lambda *args: tuple(run(*args)),
        mesh=mesh,
        in_specs=(strips,) * 4 + (P(),) * 8,
        out_specs=(strips,) * 4,
        check_vma=False,
    )
```

```python
import functools
import math

import jax
import jax.numpy as jnp
from jax import lax
from jax.experimental import pallas as pl
from jax.experimental.pallas import tpu as pltpu
from jax.sharding import PartitionSpec as P

GROUPS = 32
EPSILON = 1e-05
F32 = jnp.float32
BF16 = jnp.bfloat16
MESH = pl.DeviceIdType.MESH
KERNEL_BYTES = 52 * 1024 * 1024
LANES = 128


def halves_first(index, width, split):
    if not split:
        return index
    return 2 * (index % (width // 2)) + index // (width // 2)


def bilinear(cols, fine_split, coarse_split):
    half = cols // 2
    fine = halves_first(lax.broadcasted_iota(jnp.int32, (cols, cols), 0), cols, fine_split)
    place = lax.broadcasted_iota(jnp.int32, (cols, cols), 1)
    second = place >= half
    coarse = halves_first(jnp.where(second, place - half, place), half, coarse_split)
    near = fine // 2
    odd = fine % 2 == 1
    far = jnp.where(odd, jnp.minimum(near + 1, half - 1), jnp.maximum(near - 1, 0))
    value = jnp.where(coarse == near, 0.75, 0.0) + jnp.where(coarse == far, 0.25, 0.0)
    odd_rows = value * jnp.where(second, 0.25, 0.75)
    even_rows = value * jnp.where(second, 0.75, 0.25)
    return odd_rows.astype(BF16), even_rows.astype(BF16)


def mm(a, b):
    return jnp.dot(a, b, preferred_element_type=F32)


def mm_halves(start, a, b, step):
    cut = -(-(a.shape[1] // step) // 2) * step
    return (start + mm(a[:, :cut], b[:cut])) + mm(a[:, cut:], b[cut:])


def group_totals(value, size):
    parts = []
    for start in range(0, value.shape[1], LANES):
        part = value[:, start : start + LANES]
        spot = lax.broadcasted_iota(jnp.int32, part.shape, 1) % size
        terms = [part]
        for step in range(1, size):
            terms.append(
                jnp.where(
                    spot >= step,
                    pltpu.roll(part, step, 1),
                    pltpu.roll(part, LANES + step - size, 1),
                )
            )
        while len(terms) > 1:
            terms = [sum(terms[j : j + 2]) for j in range(0, len(terms), 2)]
        parts.append(terms[0])
    return jnp.concatenate(parts, 1)


def own_slots(shape, size):
    row = lax.broadcasted_iota(jnp.int32, shape, 0)
    return lax.broadcasted_iota(jnp.int32, shape, 1) % size == row


def packed(stats, size):
    value = jnp.concatenate(stats, 0)
    value = jnp.where(own_slots(value.shape, size), group_totals(value, size), 0.0)
    return jnp.sum(value, 0, keepdims=True)


def unpacked(row, size):
    value = jnp.broadcast_to(row, (size, row.shape[1]))
    return group_totals(jnp.where(own_slots(value.shape, size), value, 0.0), size)


def kernel(n, geom, *refs):
    images, chans = geom["images"], geom["chans"]
    rows, cols = geom["rows"], geom["cols"]
    it = iter(refs)
    take = lambda count: [next(it) for _ in range(count)]
    feat_hbm, lat_hbm = take(4), take(4)
    consts_hbm, smooth_hbm = take(3), take(1)[0]
    (conv_two,) = take(1)
    done = [None] + take(3)
    (affine,) = take(1)
    feat, lat_w = take(4), take(4)
    consts, smooth, mixed = take(3)
    vee, big = take(2), [None, None] + take(2)
    sends, recvs, lats = [None] + take(3), take(4), take(3)
    conv = [conv_two] + take(3)
    ups, edge, hang = take(3), [None] + take(3), take(2)
    mid, hop = take(2)
    box_two, box_rest = take(2)
    in_sem, w_sem, s_sem, p_sem = take(4)
    halo_send, halo_recv, hop_send, hop_recv = take(4)
    two_send, two_recv, rest_send, rest_recv = take(4)
    bias, gain, shift = (consts.at[j] for j in range(3))

    me = lax.axis_index("rows")
    first, last = me == 0, me == n - 1
    size, blocks = chans // GROUPS, chans // LANES
    half = [c // 2 for c in cols]
    top = [r + 1 for r in rows]

    feat_copy = [pltpu.make_async_copy(feat_hbm[k], feat[k], in_sem.at[k]) for k in range(4)]
    lat_copy = [pltpu.make_async_copy(lat_hbm[k], lat_w[k], w_sem.at[k]) for k in range(4)]
    smooth_copy = [
        pltpu.make_async_copy(
            smooth_hbm.at[2 * j : 2 * j + 2], smooth.at[2 * j : 2 * j + 2], s_sem.at[j]
        )
        for j in range(2)
    ]
    feat_copy[3].start()
    lat_copy[3].start()
    for j in range(3):
        pltpu.make_async_copy(consts_hbm[j], consts.at[j], p_sem.at[0]).start()
    barrier = pltpu.get_barrier_semaphore()
    for d in range(1, n):
        pl.semaphore_signal(
            barrier, inc=1, device_id={"rows": lax.rem(me + d, n)}, device_id_type=MESH
        )
    for k in (2, 1, 0):
        lat_copy[k].start()
        feat_copy[k].start()
    for copy in smooth_copy:
        copy.start()

    for k in range(3):
        odd, even = bilinear(cols[k], k < 2, k == 0)
        ups[k][0 : cols[k]] = odd
        ups[k][cols[k] :] = even

    def remote(src, dst, send_sem, recv_sem, shift_by):
        return pltpu.make_async_remote_copy(
            src_ref=src,
            dst_ref=dst,
            send_sem=send_sem,
            recv_sem=recv_sem,
            device_id={"rows": lax.rem(me + (n + shift_by), n)},
            device_id_type=MESH,
        )

    def halo_source(k, way):
        if k == 0:
            return feat[0].at[:, way * (rows[0] - 1)]
        return sends[k].at[way * (sends[k].shape[0] - 1)]

    def halo_copy(k, way):
        return remote(
            halo_source(k, way),
            recvs[k].at[1 - way],
            halo_send.at[k, way],
            halo_recv.at[k, 1 - way],
            1 if way else -1,
        )

    def on_ends(act):
        @pl.when(jnp.logical_not(first))
        def _():
            act(0)

        @pl.when(jnp.logical_not(last))
        def _():
            act(1)

    def halo_start(k):
        on_ends(lambda way: halo_copy(k, way).start())

    def halo_wait(k):
        on_ends(lambda way: halo_copy(k, 1 - way).wait_recv())

    span = 2 * max(1, math.isqrt(n // 2))
    early = images // 2
    pieces = ((0, early), (early, images)) if early else ((0, images), (0, images))
    place = lax.rem(me, span)
    crosses = (
        jnp.logical_and(place == 0, jnp.logical_not(first)),
        jnp.logical_and(place == span - 1, jnp.logical_not(last)),
    )
    carries = (
        jnp.logical_and(place == 0, me + span < n),
        jnp.logical_and(place == span - 1, me >= span),
    )
    relays = span < n
    hops = range(2) if early else range(1, 2)

    def fine_start():
        def begin(way):
            if not relays:
                halo_copy(0, way).start()
                return

            @pl.when(jnp.logical_not(crosses[way]))
            def _():
                halo_copy(0, way).start()

            @pl.when(crosses[way])
            def _():
                for j in hops:
                    here = slice(*pieces[j])
                    remote(
                        feat[0].at[here, way * (rows[0] - 1)],
                        hop.at[here],
                        halo_send.at[0, way],
                        hop_recv.at[j],
                        span if way else -span,
                    ).start()

        on_ends(begin)

    def carry(act):
        if relays:
            for way in range(2):
                pl.when(carries[way])(functools.partial(act, way))

    def carry_start(j):
        def act(way):
            here = hop.at[slice(*pieces[j])]
            pltpu.make_async_copy(here, here, hop_recv.at[j]).wait()
            remote(
                here,
                recvs[0].at[1 - way, slice(*pieces[j])],
                hop_send.at[0],
                halo_recv.at[0, 1 - way],
                1 - span if way else span - 1,
            ).start()

        if j in hops:
            carry(act)

    pltpu.make_async_copy(consts, consts, p_sem.at[0]).wait()
    feat_copy[3].wait()
    lat_copy[3].wait()
    flat = feat[3][...].reshape(-1, feat[3].shape[-1])
    five = mm_halves(bias[3:4, :], flat, lat_w[3], chans)
    five = five.reshape(images, rows[3], cols[3], chans)
    for y in range(rows[3]):
        sends[3][y] = five[:, y].astype(BF16)
    pl.semaphore_wait(barrier, n - 1)
    halo_start(3)

    lat_copy[2].wait()
    feat_copy[2].wait()
    for i in range(images):
        flat = feat[2][i].reshape(rows[2] * cols[2], -1)
        value = (bias[2:3, :] + mm(flat, lat_w[2][...])).reshape(rows[2], cols[2], chans)
        for y in range(rows[2]):
            lats[2][y, i] = value[y]
        sends[2][0, i] = value[0].astype(BF16)
        sends[2][1, i] = value[rows[2] - 1].astype(BF16)
    halo_start(2)

    def columns(k, r, i):
        return [
            jnp.concatenate(
                [lats[k][r, i, b, pl.ds(odd, half[k], stride=2), :] for b in range(blocks)], 1
            )
            for odd in range(2)
        ]

    def keep(k, r, i, value):
        for b in range(blocks):
            lats[k][r, i, b] = value[:, b * LANES : (b + 1) * LANES]

    lat_copy[1].wait()
    feat_copy[1].wait()

    def lateral_three(some):
        for i in range(images):
            flat = jnp.concatenate([feat[1][i, y] for y in some], 0)
            value = (bias[1:2, :] + mm(flat, lat_w[1][...])).reshape(len(some), cols[1], chans)
            for j, y in enumerate(some):
                keep(1, y, i, value[j])
        for y in some:
            if y in (0, rows[1] - 1):
                for i in range(images):
                    even, odd = columns(1, y, i)
                    sends[1][0 if y == 0 else 1, i, : half[1]] = even.astype(BF16)
                    sends[1][0 if y == 0 else 1, i, half[1] :] = odd.astype(BF16)

    lateral_three([0, rows[1] - 1])
    halo_start(1)
    lateral_three(list(range(1, rows[1] - 1)))

    def lateral_two(y):
        for i in range(images):
            flat = feat[0][i, y : y + 2].reshape(2 * cols[0], -1)
            value = bias[0:1, :] + mm(flat, lat_w[0][...])
            keep(0, y + 1, i, value[: cols[0]])
            keep(0, y + 2, i, value[cols[0] :])

    lat_copy[0].wait()
    feat_copy[0].wait()
    fine_start()
    steps = list(range(0, rows[0], 2))
    for y in steps[: len(steps) // 2]:
        lateral_two(y)

    def tap(k, a, b, start=0, count=chans):
        return smooth[k, pl.ds((3 * a + b) * chans + start, count)]

    smooth_copy[0].wait()
    piece = 16

    def mix(k, a, start):
        taps = [tap(k, a, b, start, piece).astype(F32) for b in range(3)]
        outer_taps, inner_tap = (taps[0] + taps[2]) * 0.5, taps[1] * 0.5
        mixed[k, 0, pl.ds(a * chans + start, piece)] = (outer_taps + inner_tap).astype(BF16)
        mixed[k, 1, pl.ds(a * chans + start, piece)] = (outer_taps - inner_tap).astype(BF16)

    for k in range(2):
        for a in range(3):
            for start in range(0, chans, piece):
                mix(k, a, start)
    for y in steps[len(steps) // 2 :]:
        lateral_two(y)
    smooth_copy[1].wait()

    def moved(value, by):
        length = value.shape[0]
        spot = lax.broadcasted_iota(jnp.int32, (8, value.shape[1]), 0)
        if by > 0:
            value = pltpu.roll(value, 1, 0)
            return jnp.concatenate([jnp.where(spot == 0, 0.0, value[:8]), value[8:]], 0)
        value = pltpu.roll(value, length - 1, 0)
        cut = length - 8
        return jnp.concatenate([value[:cut], jnp.where(spot == 7, 0.0, value[cut:])], 0)

    def put(k, r, i, value):
        big[k][r, i, :, 0:chans] = moved(value, 1).astype(BF16)
        big[k][r, i, :, chans : 2 * chans] = value.astype(BF16)
        big[k][r, i, :, 2 * chans :] = moved(value, -1).astype(BF16)

    def put_pairs(k, r, i, even, odd):
        vee[k][r, 0, i] = (moved(odd, 1) - odd).astype(BF16)
        vee[k][r, 1, i] = (even + odd).astype(BF16)
        vee[k][r, 2, i] = (odd - even).astype(BF16)
        vee[k][r, 3, i] = (even - moved(even, -1)).astype(BF16)

    def center(k, r, i):
        return big[k][r, i, :, chans : 2 * chans]

    def borders(k, i, above, below):
        edge[k][0, i] = jnp.where(first, center(k, 1, i), above.astype(BF16))
        edge[k][1, i] = jnp.where(last, center(k, rows[k], i), below.astype(BF16))
        put(k, 0, i, jnp.where(first, 0.0, above))
        put(k, top[k], i, jnp.where(last, 0.0, below))

    def pair(k, p, i):
        own = (lambda y: mid[y, i]) if k == 1 else (lambda y: center(k, y + 1, i))
        upper = edge[k][0, i] if p == 0 else own(p - 1)
        lower = edge[k][1, i] if p == rows[k] else own(p)
        return jnp.concatenate([upper, lower], 0)

    def folded(value):
        part = value.reshape(-1, 8, chans)
        return jnp.sum(part, 0), jnp.sum(part * part, 0)

    def conv_rows(k, apart):
        groups = [[i] for i in range(images)] if apart else [list(range(images))]
        sums = []
        for group in groups:
            bands = [
                jnp.concatenate([big[k][y + a, i] for i in group for y in range(rows[k])], 0)
                for a in range(3)
            ]
            total = mm(jnp.concatenate(bands, 1), smooth[k])
            total = total.reshape(len(group), rows[k], cols[k], chans)
            for j, i in enumerate(group):
                conv[k][i] = total[j]
                sums.append(folded(total[j]))
        return sums

    def conv_pairs(k, some, taps=(0, 1, 2), add=False, keep_sums=True):
        at = [slice(a * chans, (a + 1) * chans) for a in taps]
        weights = [
            jnp.concatenate([tap(k, a, 0) for a in taps], 0),
            jnp.concatenate([mixed[k, 0, here] for here in at], 0),
            jnp.concatenate([mixed[k, 1, here] for here in at], 0),
            jnp.concatenate([tap(k, a, 2) for a in taps], 0),
        ]
        parts = []
        for t in range(4):
            bands = [
                jnp.concatenate([vee[k][y + a, t, i] for y in some for i in range(images)], 0)
                for a in taps
            ]
            parts.append(mm(jnp.concatenate(bands, 1), weights[t]))
        even = (parts[1] + parts[2]) + parts[0]
        odd = (parts[1] - parts[2]) - parts[3]
        sums = [None] * images
        for j, (y, i) in enumerate((y, i) for y in some for i in range(images)):
            here = slice(j * half[k], (j + 1) * half[k])
            values = []
            for odd_ones, value in ((0, even[here]), (1, odd[here])):
                spots = [
                    conv[k].at[i, y, b, pl.ds(odd_ones, half[k], stride=2), :]
                    for b in range(blocks)
                ]
                if add:
                    value = value + jnp.concatenate([spot[...] for spot in spots], 1)
                for b, spot in enumerate(spots):
                    spot[...] = value[:, b * LANES : (b + 1) * LANES]
                values.append(value)
            if keep_sums:
                new = joined([[folded(value)] for value in values])[0]
                sums[i] = new if sums[i] is None else joined([[sums[i]], [new]])[0]
        return sums

    def joined(parts):
        total = parts[0]
        for part in parts[1:]:
            total = [(t[0] + u[0], t[1] + u[1]) for t, u in zip(total, part)]
        return total

    def stat_rows(sums):
        return [jnp.sum(part, 0, keepdims=True) for pair in sums for part in pair]

    def post(box, rows_of, send_sem, recv_sem):
        for j in range(box.shape[1]):
            some = rows_of[j * size : (j + 1) * size]
            some = some + [jnp.zeros_like(some[0])] * (size - len(some))
            box[0, j] = packed(some, size)
        for d in range(1, n):
            remote(box.at[0], box.at[d], send_sem.at[0], recv_sem.at[0], d).start()

    def all_of(box, sem):
        pltpu.make_async_copy(box.at[1:n], box.at[1:n], sem.at[0]).wait()

    def gathered(box):
        stats = []
        for j in range(box.shape[1]):
            total = box[0, j]
            for d in range(1, n):
                total = total + box[d, j]
            stats.append(unpacked(total, size))
        return jnp.concatenate(stats, 0)

    for i in range(images):
        for y in range(rows[3]):
            put(3, y + 1, i, five[i, y])
    halo_wait(3)
    for i in range(images):
        borders(3, i, recvs[3][0, i].astype(F32), recvs[3][1, i].astype(F32))

    outer = {}
    for p in range(rows[3] + 1):
        for i in range(images):
            both = mm(ups[2][...], pair(3, p, i))
            for y, value in ((2 * p - 1, both[: cols[2]]), (2 * p, both[cols[2] :])):
                if 0 <= y < rows[2]:
                    put(2, y + 1, i, lats[2][y, i] + value)
                else:
                    outer[y, i] = value
    carry_start(0)
    halo_wait(2)
    for i in range(images):
        borders(
            2,
            i,
            recvs[2][0, i].astype(F32) + outer[-1, i],
            recvs[2][1, i].astype(F32) + outer[rows[2], i],
        )

    def merge(k, p):
        for i in range(images):
            both = mm(ups[k][...], pair(k + 1, p, i))
            for y, value in ((2 * p - 1, both[: cols[k]]), (2 * p, both[cols[k] :])):
                if not 0 <= y < rows[k]:
                    hang[k][0 if y < 0 else 1, i] = value
                    continue
                even, odd = columns(k, y + 1 if k == 0 else y, i)
                even = even + value[: half[k]]
                odd = odd + value[half[k] :]
                if k:
                    mid[y, i, : half[k]] = even.astype(BF16)
                    mid[y, i, half[k] :] = odd.astype(BF16)
                put_pairs(k, y + 1, i, even, odd)

    def outside(k, way, i, even, odd):
        none = last if way else first
        put_pairs(
            k, way * top[k], i, jnp.where(none, 0.0, even), jnp.where(none, 0.0, odd)
        )

    for p in range(1, rows[2]):
        merge(1, p)
    sums_five = conv_rows(3, False)
    merge(1, 0)
    merge(1, rows[2])
    merge(0, 1)
    sums_four = conv_rows(2, True)
    sums_three = [conv_pairs(1, list(range(1, rows[1] - 1)))]
    merged, sums_two = 1, []

    def conv_two_row(y):
        nonlocal merged
        while merged < min((y + 2) // 2, rows[1] - 1):
            merged += 1
            merge(0, merged)
        sums_two.append(conv_pairs(0, [y]))

    inner = list(range(2, rows[0] - 2))
    for y in inner[: len(inner) // 2]:
        conv_two_row(y)

    carry_start(1)
    halo_wait(1)
    for way in range(2):
        for i in range(images):
            value = recvs[1][way, i].astype(F32) + hang[1][way, i]
            none = last if way else first
            own = mid[way * (rows[1] - 1), i]
            edge[1][way, i] = jnp.where(none, own, value.astype(BF16))
            outside(1, way, i, value[: half[1]], value[half[1] :])
    merge(0, 0)
    merge(0, rows[1])
    for y in inner[len(inner) // 2 :]:
        conv_two_row(y)
    sums_three.append(conv_pairs(1, [0, rows[1] - 1]))
    conv_two_row(1)
    conv_two_row(rows[0] - 2)
    conv_pairs(0, [0], (1, 2), keep_sums=False)
    conv_pairs(0, [rows[0] - 1], (0, 1), keep_sums=False)
    rest_rows = stat_rows(joined(sums_three)) + stat_rows(sums_four) + stat_rows(sums_five)
    post(box_rest, rest_rows, rest_send, rest_recv)

    halo_wait(0)
    for way in range(2):
        value = bias[0:1, :] + mm(recvs[0][way].reshape(images * cols[0], -1), lat_w[0][...])
        for i in range(images):
            keep(0, way * top[0], i, value[i * cols[0] : (i + 1) * cols[0]])
    for way in range(2):
        for i in range(images):
            even, odd = columns(0, way * top[0], i)
            even = even + hang[0][way, i, : half[0]]
            odd = odd + hang[0][way, i, half[0] :]
            outside(0, way, i, even, odd)
    sums_two.append(conv_pairs(0, [0], (0,), add=True))
    sums_two.append(conv_pairs(0, [rows[0] - 1], (2,), add=True))
    post(box_two, stat_rows(joined(sums_two)), two_send, two_recv)

    def scales(k, total, square):
        share = 1.0 / float(rows[k] * n * cols[k] * size)
        mean = total * share
        variance = square * share - mean * mean
        scale = lax.rsqrt(variance + EPSILON) * gain[k : k + 1, :]
        return scale, shift[k : k + 1, :] - mean * scale

    all_of(box_rest, rest_recv)
    rest = gathered(box_rest)
    for k in (1, 2, 3):
        for i in range(images):
            slot = ((k - 1) * images + i) * 2
            scale, offset = scales(k, rest[slot : slot + 1], rest[slot + 1 : slot + 2])
            if k == 1:
                for y in range(rows[k]):
                    value = jnp.concatenate([conv[k][i, y, b] for b in range(blocks)], 1)
                    done[k][i, y] = (value * scale + offset).astype(BF16)
            else:
                done[k][i] = (conv[k][i] * scale + offset).astype(BF16)
    on_ends(lambda way: [halo_copy(k, way).wait_send() for k in range(4)])
    carry(lambda way: pltpu.make_async_copy(hop, hop, hop_send.at[0]).wait())
    all_of(box_rest, rest_send)

    all_of(box_two, two_recv)
    two = gathered(box_two)
    for i in range(images):
        scale, offset = scales(0, two[2 * i : 2 * i + 1], two[2 * i + 1 : 2 * i + 2])
        affine[2 * i : 2 * i + 1, :] = scale
        affine[2 * i + 1 : 2 * i + 2, :] = offset
    all_of(box_two, two_send)


def finish_kernel(geom, *refs):
    images, rows = geom["images"], geom["rows"]
    conv_two, affine = refs[0:2]
    done = [None, *refs[2:5]]
    out_hbm, staged, rest_sem, two_sem = refs[5:9], refs[9], refs[10], refs[11]
    copies = []
    for k in (1, 2, 3):
        copies.append(pltpu.make_async_copy(done[k], out_hbm[k], rest_sem.at[k]))
        copies[-1].start()
    for i in range(images):
        scale = affine[2 * i : 2 * i + 1, :]
        offset = affine[2 * i + 1 : 2 * i + 2, :]
        for y in range(rows[0]):
            value = jnp.concatenate(
                [conv_two[i, y, b] for b in range(conv_two.shape[2])], 1
            )
            staged[i, y] = (value * scale + offset).astype(BF16)
            pltpu.make_async_copy(
                staged.at[i, y], out_hbm[0].at[i, y], two_sem.at[0]
            ).start()
    for copy in copies:
        copy.wait()
    pltpu.make_async_copy(staged, out_hbm[0], two_sem.at[0]).wait()


def per_device(n, *args):
    feats, lat_ws = args[0:4], args[4:8]
    bias, smooth, gain, shift = args[8:12]
    smooth = smooth.reshape(smooth.shape[0], -1, smooth.shape[3])
    images, chans = feats[0].shape[0], lat_ws[0].shape[1]
    rows = [f.shape[1] for f in feats]
    cols = [f.shape[2] for f in feats]
    geom = {"images": images, "chans": chans, "rows": rows, "cols": cols}
    any_spec = pl.BlockSpec(memory_space=pltpu.HBM)
    vmem_spec = pl.BlockSpec(memory_space=pltpu.VMEM)
    outs = [jax.ShapeDtypeStruct((images, r, c, chans), BF16) for r, c in zip(rows, cols)]
    dma = pltpu.SemaphoreType.DMA
    blocks = chans // LANES
    two_rows = -(-(images * 2) // 8) * 8
    strip = lambda k, count, width, kind: pltpu.VMEM((count, images, cols[k], width), kind)
    scratch = (
        [pltpu.VMEM(f.shape, BF16) for f in feats]
        + [pltpu.VMEM(w.shape, BF16) for w in lat_ws]
        + [pltpu.VMEM((3, *bias.shape), F32), pltpu.VMEM(smooth.shape, BF16)]
        + [pltpu.VMEM((2, 2, 3 * chans, chans), BF16)]
        + [pltpu.VMEM((rows[k] + 2, 4, images, cols[k] // 2, chans), BF16) for k in range(2)]
        + [strip(k, rows[k] + 2, 3 * chans, BF16) for k in (2, 3)]
        + [strip(k, min(rows[k], 2), chans, BF16) for k in range(1, 4)]
        + [strip(k, 2, chans, BF16) for k in range(4)]
        + [pltpu.VMEM((rows[0] + 2, images, blocks, cols[0], LANES), F32)]
        + [pltpu.VMEM((rows[1], images, blocks, cols[1], LANES), F32)]
        + [strip(2, rows[2], chans, F32)]
        + [pltpu.VMEM((images, rows[1], blocks, cols[1], LANES), F32)]
        + [pltpu.VMEM(o.shape, F32) for o in outs[2:]]
        + [pltpu.VMEM((2 * c, c), BF16) for c in cols[:3]]
        + [strip(k, 2, chans, BF16) for k in range(1, 4)]
        + [strip(k, 2, chans, F32) for k in range(2)]
        + [strip(1, rows[1], chans, BF16)]
        + [pltpu.VMEM((images, cols[0], chans), BF16)]
        + [
            pltpu.VMEM((n, -(-levels * images * 2 // (chans // GROUPS)), 1, chans), F32)
            for levels in (1, 3)
        ]
        + [dma((4,)), dma((4,)), dma((2,)), dma((1,))]
        + [dma((4, 2)), dma((4, 2)), dma((1,)), dma((2,))]
        + [dma((1,)) for _ in range(4)]
    )
    held = pl.pallas_call(
        functools.partial(kernel, n, geom),
        out_shape=[pltpu.VMEM((images, rows[0], blocks, cols[0], LANES), F32)]
        + [pltpu.VMEM(o.shape, BF16) for o in outs[1:]]
        + [pltpu.VMEM((two_rows, chans), F32)],
        in_specs=[any_spec] * 12,
        out_specs=[vmem_spec] * 5,
        scratch_shapes=scratch,
        compiler_params=pltpu.CompilerParams(
            collective_id=0, has_side_effects=True, vmem_limit_bytes=KERNEL_BYTES
        ),
    )(*args[:8], bias, gain, shift, smooth)
    held = [pltpu.with_memory_space_constraint(h, pltpu.VMEM) for h in held]
    return pl.pallas_call(
        functools.partial(finish_kernel, geom),
        out_shape=outs,
        in_specs=[vmem_spec] * 5,
        out_specs=[any_spec] * 4,
        scratch_shapes=[pltpu.VMEM(outs[0].shape, BF16), dma((4,)), dma((1,))],
        compiler_params=pltpu.CompilerParams(vmem_limit_bytes=16 * 1024 * 1024),
    )(held[0], held[4], *held[1:4])


def solution(mesh):
    strips = P("batch", "rows", None, None)
    run = functools.partial(per_device, mesh.shape["rows"])
    return jax.shard_map(
        lambda *args: tuple(run(*args)),
        mesh=mesh,
        in_specs=(strips,) * 4 + (P(),) * 8,
        out_specs=(strips,) * 4,
        check_vma=False,
    )
```

```python
import functools
import math

import jax
import jax.numpy as jnp
from jax import lax
from jax.experimental import pallas as pl
from jax.experimental.pallas import tpu as pltpu
from jax.sharding import PartitionSpec as P

GROUPS = 32
EPSILON = 1e-05
F32 = jnp.float32
BF16 = jnp.bfloat16
MESH = pl.DeviceIdType.MESH
KERNEL_BYTES = 52 * 1024 * 1024
LANES = 128


def halves_first(index, width, split):
    if not split:
        return index
    return 2 * (index % (width // 2)) + index // (width // 2)


def bilinear(cols, fine_split, coarse_split):
    half = cols // 2
    fine = halves_first(lax.broadcasted_iota(jnp.int32, (cols, cols), 0), cols, fine_split)
    place = lax.broadcasted_iota(jnp.int32, (cols, cols), 1)
    second = place >= half
    coarse = halves_first(jnp.where(second, place - half, place), half, coarse_split)
    near = fine // 2
    odd = fine % 2 == 1
    far = jnp.where(odd, jnp.minimum(near + 1, half - 1), jnp.maximum(near - 1, 0))
    value = jnp.where(coarse == near, 0.75, 0.0) + jnp.where(coarse == far, 0.25, 0.0)
    odd_rows = value * jnp.where(second, 0.25, 0.75)
    even_rows = value * jnp.where(second, 0.75, 0.25)
    return odd_rows.astype(BF16), even_rows.astype(BF16)


def mm(a, b):
    return jnp.dot(a, b, preferred_element_type=F32)


def group_totals(value, size):
    parts = []
    for start in range(0, value.shape[1], LANES):
        part = value[:, start : start + LANES]
        spot = lax.broadcasted_iota(jnp.int32, part.shape, 1) % size
        terms = [part]
        for step in range(1, size):
            terms.append(
                jnp.where(
                    spot >= step,
                    pltpu.roll(part, step, 1),
                    pltpu.roll(part, LANES + step - size, 1),
                )
            )
        while len(terms) > 1:
            terms = [sum(terms[j : j + 2]) for j in range(0, len(terms), 2)]
        parts.append(terms[0])
    return jnp.concatenate(parts, 1)


def own_slots(shape, size):
    row = lax.broadcasted_iota(jnp.int32, shape, 0)
    return lax.broadcasted_iota(jnp.int32, shape, 1) % size == row


def packed(stats, size):
    value = jnp.concatenate(stats, 0)
    value = jnp.where(own_slots(value.shape, size), group_totals(value, size), 0.0)
    return jnp.sum(value, 0, keepdims=True)


def unpacked(row, size):
    value = jnp.broadcast_to(row, (size, row.shape[1]))
    return group_totals(jnp.where(own_slots(value.shape, size), value, 0.0), size)


def kernel(n, geom, *refs):
    images, chans = geom["images"], geom["chans"]
    rows, cols = geom["rows"], geom["cols"]
    it = iter(refs)
    take = lambda count: [next(it) for _ in range(count)]
    feat_hbm, lat_hbm = take(4), take(4)
    consts_hbm, smooth_hbm = take(3), take(1)[0]
    (conv_two,) = take(1)
    done = [None] + take(3)
    (affine,) = take(1)
    feat, lat_w = take(4), take(4)
    consts, smooth, mixed = take(3)
    vee, big = take(2), [None, None] + take(2)
    sends, recvs, lats = [None] + take(3), take(4), take(3)
    conv = [conv_two] + take(3)
    ups, edge, hang = take(3), [None] + take(3), take(2)
    mid, hop = take(2)
    box_two, box_rest = take(2)
    in_sem, w_sem, s_sem, p_sem = take(4)
    halo_send, halo_recv, hop_send, hop_recv = take(4)
    two_send, two_recv, rest_send, rest_recv = take(4)
    bias, gain, shift = (consts.at[j] for j in range(3))

    me = lax.axis_index("rows")
    first, last = me == 0, me == n - 1
    size, blocks = chans // GROUPS, chans // LANES
    half = [c // 2 for c in cols]
    top = [r + 1 for r in rows]

    feat_copy = [pltpu.make_async_copy(feat_hbm[k], feat[k], in_sem.at[k]) for k in range(4)]
    lat_copy = [pltpu.make_async_copy(lat_hbm[k], lat_w[k], w_sem.at[k]) for k in range(4)]
    smooth_copy = [
        pltpu.make_async_copy(
            smooth_hbm.at[2 * j : 2 * j + 2], smooth.at[2 * j : 2 * j + 2], s_sem.at[j]
        )
        for j in range(2)
    ]
    feat_copy[3].start()
    lat_copy[3].start()
    for j in range(3):
        pltpu.make_async_copy(consts_hbm[j], consts.at[j], p_sem.at[0]).start()
    barrier = pltpu.get_barrier_semaphore()
    for d in range(1, n):
        pl.semaphore_signal(
            barrier, inc=1, device_id={"rows": lax.rem(me + d, n)}, device_id_type=MESH
        )
    for k in (2, 1, 0):
        lat_copy[k].start()
        feat_copy[k].start()
    for copy in smooth_copy:
        copy.start()

    @pl.when(first)
    def _():
        recvs[0][0] = jnp.zeros_like(recvs[0][0])

    @pl.when(last)
    def _():
        recvs[0][1] = jnp.zeros_like(recvs[0][1])

    for k in range(3):
        odd, even = bilinear(cols[k], k < 2, k == 0)
        ups[k][0 : cols[k]] = odd
        ups[k][cols[k] :] = even

    def remote(src, dst, send_sem, recv_sem, shift_by):
        return pltpu.make_async_remote_copy(
            src_ref=src,
            dst_ref=dst,
            send_sem=send_sem,
            recv_sem=recv_sem,
            device_id={"rows": lax.rem(me + (n + shift_by), n)},
            device_id_type=MESH,
        )

    def halo_source(k, way):
        if k == 0:
            return feat[0].at[:, way * (rows[0] - 1)]
        return sends[k].at[way * (sends[k].shape[0] - 1)]

    def halo_copy(k, way):
        return remote(
            halo_source(k, way),
            recvs[k].at[1 - way],
            halo_send.at[k, way],
            halo_recv.at[k, 1 - way],
            1 if way else -1,
        )

    def on_ends(act):
        @pl.when(jnp.logical_not(first))
        def _():
            act(0)

        @pl.when(jnp.logical_not(last))
        def _():
            act(1)

    def halo_start(k):
        on_ends(lambda way: halo_copy(k, way).start())

    def halo_wait(k):
        on_ends(lambda way: halo_copy(k, 1 - way).wait_recv())

    span = 2 * max(1, math.isqrt(n // 2))
    early = images // 2
    pieces = ((0, early), (early, images)) if early else ((0, images), (0, images))
    place = lax.rem(me, span)
    crosses = (
        jnp.logical_and(place == 0, jnp.logical_not(first)),
        jnp.logical_and(place == span - 1, jnp.logical_not(last)),
    )
    carries = (
        jnp.logical_and(place == 0, me + span < n),
        jnp.logical_and(place == span - 1, me >= span),
    )
    relays = span < n
    hops = range(2) if early else range(1, 2)

    def fine_start():
        def begin(way):
            if not relays:
                halo_copy(0, way).start()
                return

            @pl.when(jnp.logical_not(crosses[way]))
            def _():
                halo_copy(0, way).start()

            @pl.when(crosses[way])
            def _():
                for j in hops:
                    here = slice(*pieces[j])
                    remote(
                        feat[0].at[here, way * (rows[0] - 1)],
                        hop.at[here],
                        halo_send.at[0, way],
                        hop_recv.at[j],
                        span if way else -span,
                    ).start()

        on_ends(begin)

    def carry(act):
        if relays:
            for way in range(2):
                pl.when(carries[way])(functools.partial(act, way))

    def carry_start(j):
        def act(way):
            here = hop.at[slice(*pieces[j])]
            pltpu.make_async_copy(here, here, hop_recv.at[j]).wait()
            remote(
                here,
                recvs[0].at[1 - way, slice(*pieces[j])],
                hop_send.at[0],
                halo_recv.at[0, 1 - way],
                1 - span if way else span - 1,
            ).start()

        if j in hops:
            carry(act)

    pltpu.make_async_copy(consts, consts, p_sem.at[0]).wait()
    feat_copy[3].wait()
    lat_copy[3].wait()
    five = []
    for i in range(images):
        flat = feat[3][i].reshape(rows[3] * cols[3], -1)
        five.append((bias[3:4, :] + mm(flat, lat_w[3][...])).reshape(rows[3], cols[3], chans))
    for y in range(rows[3]):
        for i in range(images):
            sends[3][y, i] = five[i][y].astype(BF16)
    pl.semaphore_wait(barrier, n - 1)
    halo_start(3)

    lat_copy[2].wait()
    feat_copy[2].wait()
    for i in range(images):
        flat = feat[2][i].reshape(rows[2] * cols[2], -1)
        value = (bias[2:3, :] + mm(flat, lat_w[2][...])).reshape(rows[2], cols[2], chans)
        for y in range(rows[2]):
            lats[2][y, i] = value[y]
        sends[2][0, i] = value[0].astype(BF16)
        sends[2][1, i] = value[rows[2] - 1].astype(BF16)
    halo_start(2)

    def columns(k, r, i):
        return [
            jnp.concatenate(
                [lats[k][r, i, b, pl.ds(odd, half[k], stride=2), :] for b in range(blocks)], 1
            )
            for odd in range(2)
        ]

    def keep(k, r, i, value):
        for b in range(blocks):
            lats[k][r, i, b] = value[:, b * LANES : (b + 1) * LANES]

    lat_copy[1].wait()
    feat_copy[1].wait()

    def lateral_three(some):
        for i in range(images):
            flat = jnp.concatenate([feat[1][i, y] for y in some], 0)
            value = (bias[1:2, :] + mm(flat, lat_w[1][...])).reshape(len(some), cols[1], chans)
            for j, y in enumerate(some):
                keep(1, y, i, value[j])
        for y in some:
            if y in (0, rows[1] - 1):
                for i in range(images):
                    even, odd = columns(1, y, i)
                    sends[1][0 if y == 0 else 1, i, : half[1]] = even.astype(BF16)
                    sends[1][0 if y == 0 else 1, i, half[1] :] = odd.astype(BF16)

    lateral_three([0, rows[1] - 1])
    halo_start(1)
    lateral_three(list(range(1, rows[1] - 1)))

    def lateral_two(y):
        for i in range(images):
            flat = feat[0][i, y : y + 2].reshape(2 * cols[0], -1)
            value = bias[0:1, :] + mm(flat, lat_w[0][...])
            keep(0, y + 1, i, value[: cols[0]])
            keep(0, y + 2, i, value[cols[0] :])

    lat_copy[0].wait()
    feat_copy[0].wait()
    fine_start()
    steps = list(range(0, rows[0], 2))
    for y in steps[: len(steps) // 2]:
        lateral_two(y)

    def tap(k, a, b, start=0, count=chans):
        return smooth[k, pl.ds((3 * a + b) * chans + start, count)]

    smooth_copy[0].wait()
    piece = 16

    def mix(k, a, start):
        taps = [tap(k, a, b, start, piece).astype(F32) for b in range(3)]
        outer_taps, inner_tap = (taps[0] + taps[2]) * 0.5, taps[1] * 0.5
        mixed[k, 0, pl.ds(a * chans + start, piece)] = (outer_taps + inner_tap).astype(BF16)
        mixed[k, 1, pl.ds(a * chans + start, piece)] = (outer_taps - inner_tap).astype(BF16)

    for k in range(2):
        for a in range(3):
            for start in range(0, chans, piece):
                mix(k, a, start)
    for y in steps[len(steps) // 2 :]:
        lateral_two(y)
    smooth_copy[1].wait()

    def moved(value, by):
        length = value.shape[0]
        spot = lax.broadcasted_iota(jnp.int32, (8, value.shape[1]), 0)
        if by > 0:
            value = pltpu.roll(value, 1, 0)
            return jnp.concatenate([jnp.where(spot == 0, 0.0, value[:8]), value[8:]], 0)
        value = pltpu.roll(value, length - 1, 0)
        cut = length - 8
        return jnp.concatenate([value[:cut], jnp.where(spot == 7, 0.0, value[cut:])], 0)

    def put(k, r, i, value):
        big[k][r, i, :, 0:chans] = moved(value, 1).astype(BF16)
        big[k][r, i, :, chans : 2 * chans] = value.astype(BF16)
        big[k][r, i, :, 2 * chans :] = moved(value, -1).astype(BF16)

    def put_pairs(k, r, i, even, odd):
        vee[k][r, 0, i] = (moved(odd, 1) - odd).astype(BF16)
        vee[k][r, 1, i] = (even + odd).astype(BF16)
        vee[k][r, 2, i] = (odd - even).astype(BF16)
        vee[k][r, 3, i] = (even - moved(even, -1)).astype(BF16)

    def center(k, r, i):
        return big[k][r, i, :, chans : 2 * chans]

    def borders(k, i, above, below):
        edge[k][0, i] = jnp.where(first, center(k, 1, i), above.astype(BF16))
        edge[k][1, i] = jnp.where(last, center(k, rows[k], i), below.astype(BF16))
        put(k, 0, i, jnp.where(first, 0.0, above))
        put(k, top[k], i, jnp.where(last, 0.0, below))

    def pair(k, p, i):
        own = (lambda y: mid[y, i]) if k == 1 else (lambda y: center(k, y + 1, i))
        upper = edge[k][0, i] if p == 0 else own(p - 1)
        lower = edge[k][1, i] if p == rows[k] else own(p)
        return jnp.concatenate([upper, lower], 0)

    def folded(value):
        part = value.reshape(-1, 8, chans)
        return jnp.sum(part, 0), jnp.sum(part * part, 0)

    def conv_rows(k, apart):
        groups = [[i] for i in range(images)] if apart else [list(range(images))]
        sums = []
        for group in groups:
            bands = [
                jnp.concatenate([big[k][y + a, i] for i in group for y in range(rows[k])], 0)
                for a in range(3)
            ]
            total = mm(jnp.concatenate(bands, 1), smooth[k])
            total = total.reshape(len(group), rows[k], cols[k], chans)
            for j, i in enumerate(group):
                conv[k][i] = total[j]
                sums.append(folded(total[j]))
        return sums

    def conv_pairs(k, some, taps=(0, 1, 2), add=False, keep_sums=True):
        at = [slice(a * chans, (a + 1) * chans) for a in taps]
        weights = [
            jnp.concatenate([tap(k, a, 0) for a in taps], 0),
            jnp.concatenate([mixed[k, 0, here] for here in at], 0),
            jnp.concatenate([mixed[k, 1, here] for here in at], 0),
            jnp.concatenate([tap(k, a, 2) for a in taps], 0),
        ]
        parts = []
        for t in range(4):
            bands = [
                jnp.concatenate([vee[k][y + a, t, i] for y in some for i in range(images)], 0)
                for a in taps
            ]
            parts.append(mm(jnp.concatenate(bands, 1), weights[t]))
        even = (parts[1] + parts[2]) + parts[0]
        odd = (parts[1] - parts[2]) - parts[3]
        sums = [None] * images
        for j, (y, i) in enumerate((y, i) for y in some for i in range(images)):
            here = slice(j * half[k], (j + 1) * half[k])
            values = []
            for odd_ones, value in ((0, even[here]), (1, odd[here])):
                spots = [
                    conv[k].at[i, y, b, pl.ds(odd_ones, half[k], stride=2), :]
                    for b in range(blocks)
                ]
                if add:
                    value = value + jnp.concatenate([spot[...] for spot in spots], 1)
                for b, spot in enumerate(spots):
                    spot[...] = value[:, b * LANES : (b + 1) * LANES]
                values.append(value)
            if keep_sums:
                new = joined([[folded(value)] for value in values])[0]
                sums[i] = new if sums[i] is None else joined([[sums[i]], [new]])[0]
        return sums

    def joined(parts):
        total = parts[0]
        for part in parts[1:]:
            total = [(t[0] + u[0], t[1] + u[1]) for t, u in zip(total, part)]
        return total

    def stat_rows(sums):
        return [jnp.sum(part, 0, keepdims=True) for pair in sums for part in pair]

    def post(box, rows_of, send_sem, recv_sem):
        for j in range(box.shape[1]):
            some = rows_of[j * size : (j + 1) * size]
            some = some + [jnp.zeros_like(some[0])] * (size - len(some))
            box[0, j] = packed(some, size)
        for d in range(1, n):
            remote(box.at[0], box.at[d], send_sem.at[0], recv_sem.at[0], d).start()

    def all_of(box, sem):
        pltpu.make_async_copy(box.at[1:n], box.at[1:n], sem.at[0]).wait()

    def gathered(box):
        stats = []
        for j in range(box.shape[1]):
            total = box[0, j]
            for d in range(1, n):
                total = total + box[d, j]
            stats.append(unpacked(total, size))
        return jnp.concatenate(stats, 0)

    for i in range(images):
        for y in range(rows[3]):
            put(3, y + 1, i, five[i][y])
    halo_wait(3)
    for i in range(images):
        borders(3, i, recvs[3][0, i].astype(F32), recvs[3][1, i].astype(F32))

    outer = {}
    for p in range(rows[3] + 1):
        for i in range(images):
            both = mm(ups[2][...], pair(3, p, i))
            for y, value in ((2 * p - 1, both[: cols[2]]), (2 * p, both[cols[2] :])):
                if 0 <= y < rows[2]:
                    put(2, y + 1, i, lats[2][y, i] + value)
                else:
                    outer[y, i] = value
    def merge(k, p):
        for i in range(images):
            both = mm(ups[k][...], pair(k + 1, p, i))
            for y, value in ((2 * p - 1, both[: cols[k]]), (2 * p, both[cols[k] :])):
                if not 0 <= y < rows[k]:
                    if k == 0:
                        value = jnp.where(first if y < 0 else last, 0.0, value + bias[0:1, :])
                    hang[k][0 if y < 0 else 1, i] = value
                    continue
                even, odd = columns(k, y + 1 if k == 0 else y, i)
                even = even + value[: half[k]]
                odd = odd + value[half[k] :]
                if k:
                    mid[y, i, : half[k]] = even.astype(BF16)
                    mid[y, i, half[k] :] = odd.astype(BF16)
                put_pairs(k, y + 1, i, even, odd)

    sums_five = conv_rows(3, False)
    for p in range(1, rows[2]):
        merge(1, p)
    for p in range(2, rows[1] - 1):
        merge(0, p)

    halo_wait(2)
    for i in range(images):
        borders(
            2,
            i,
            recvs[2][0, i].astype(F32) + outer[-1, i],
            recvs[2][1, i].astype(F32) + outer[rows[2], i],
        )

    merge(1, 0)
    merge(1, rows[2])
    merge(0, 1)
    merge(0, rows[1] - 1)
    sums_four = conv_rows(2, True)
    sums_three = [conv_pairs(1, list(range(1, rows[1] - 1)))]
    sums_two = []

    def conv_two_row(y):
        sums_two.append(conv_pairs(0, [y]))

    inner = list(range(2, rows[0] - 2))
    for y in inner[: len(inner) // 2]:
        conv_two_row(y)

    carry_start(0)
    carry_start(1)
    halo_wait(1)
    for way in range(2):
        for i in range(images):
            value = recvs[1][way, i].astype(F32) + hang[1][way, i]
            none = last if way else first
            own = mid[way * (rows[1] - 1), i]
            edge[1][way, i] = jnp.where(none, own, value.astype(BF16))
            value = jnp.where(none, 0.0, value)
            put_pairs(1, way * top[1], i, value[: half[1]], value[half[1] :])
    merge(0, 0)
    merge(0, rows[1])
    for y in inner[len(inner) // 2 :]:
        conv_two_row(y)
    sums_three.append(conv_pairs(1, [0, rows[1] - 1]))
    conv_two_row(1)
    conv_two_row(rows[0] - 2)
    conv_pairs(0, [0], (1, 2), keep_sums=False)
    conv_pairs(0, [rows[0] - 1], (0, 1), keep_sums=False)
    rest_rows = stat_rows(joined(sums_three)) + stat_rows(sums_four) + stat_rows(sums_five)
    post(box_rest, rest_rows, rest_send, rest_recv)

    halo_wait(0)
    for way in range(2):
        value = mm(recvs[0][way].reshape(images * cols[0], -1), lat_w[0][...])
        for i in range(images):
            keep(0, way * top[0], i, value[i * cols[0] : (i + 1) * cols[0]])
    for way in range(2):
        for i in range(images):
            even, odd = columns(0, way * top[0], i)
            even = even + hang[0][way, i, : half[0]]
            odd = odd + hang[0][way, i, half[0] :]
            put_pairs(0, way * top[0], i, even, odd)
    sums_two.append(conv_pairs(0, [0], (0,), add=True))
    sums_two.append(conv_pairs(0, [rows[0] - 1], (2,), add=True))
    post(box_two, stat_rows(joined(sums_two)), two_send, two_recv)

    def scales(k, total, square):
        share = 1.0 / float(rows[k] * n * cols[k] * size)
        mean = total * share
        variance = square * share - mean * mean
        scale = lax.rsqrt(variance + EPSILON) * gain[k : k + 1, :]
        return scale, shift[k : k + 1, :] - mean * scale

    all_of(box_rest, rest_recv)
    rest = gathered(box_rest)
    for k in (1, 2, 3):
        for i in range(images):
            slot = ((k - 1) * images + i) * 2
            scale, offset = scales(k, rest[slot : slot + 1], rest[slot + 1 : slot + 2])
            if k == 1:
                for y in range(rows[k]):
                    value = jnp.concatenate([conv[k][i, y, b] for b in range(blocks)], 1)
                    done[k][i, y] = (value * scale + offset).astype(BF16)
            else:
                done[k][i] = (conv[k][i] * scale + offset).astype(BF16)
    on_ends(lambda way: [halo_copy(k, way).wait_send() for k in range(4)])
    carry(lambda way: pltpu.make_async_copy(hop, hop, hop_send.at[0]).wait())
    all_of(box_rest, rest_send)

    all_of(box_two, two_recv)
    two = gathered(box_two)
    for i in range(images):
        scale, offset = scales(0, two[2 * i : 2 * i + 1], two[2 * i + 1 : 2 * i + 2])
        affine[2 * i : 2 * i + 1, :] = scale
        affine[2 * i + 1 : 2 * i + 2, :] = offset
    all_of(box_two, two_send)


def finish_kernel(geom, *refs):
    images, rows = geom["images"], geom["rows"]
    conv_two, affine = refs[0:2]
    done = [None, *refs[2:5]]
    out_hbm, staged, rest_sem, two_sem = refs[5:9], refs[9], refs[10], refs[11]
    copies = []
    for k in (1, 2, 3):
        copies.append(pltpu.make_async_copy(done[k], out_hbm[k], rest_sem.at[k]))
        copies[-1].start()
    for i in range(images):
        scale = affine[2 * i : 2 * i + 1, :]
        offset = affine[2 * i + 1 : 2 * i + 2, :]
        for y in range(rows[0]):
            value = jnp.concatenate(
                [conv_two[i, y, b] for b in range(conv_two.shape[2])], 1
            )
            staged[i, y] = (value * scale + offset).astype(BF16)
            pltpu.make_async_copy(
                staged.at[i, y], out_hbm[0].at[i, y], two_sem.at[0]
            ).start()
    for copy in copies:
        copy.wait()
    pltpu.make_async_copy(staged, out_hbm[0], two_sem.at[0]).wait()


def per_device(n, *args):
    feats, lat_ws = args[0:4], args[4:8]
    bias, smooth, gain, shift = args[8:12]
    smooth = smooth.reshape(smooth.shape[0], -1, smooth.shape[3])
    images, chans = feats[0].shape[0], lat_ws[0].shape[1]
    rows = [f.shape[1] for f in feats]
    cols = [f.shape[2] for f in feats]
    geom = {"images": images, "chans": chans, "rows": rows, "cols": cols}
    any_spec = pl.BlockSpec(memory_space=pltpu.HBM)
    vmem_spec = pl.BlockSpec(memory_space=pltpu.VMEM)
    outs = [jax.ShapeDtypeStruct((images, r, c, chans), BF16) for r, c in zip(rows, cols)]
    dma = pltpu.SemaphoreType.DMA
    blocks = chans // LANES
    two_rows = -(-(images * 2) // 8) * 8
    strip = lambda k, count, width, kind: pltpu.VMEM((count, images, cols[k], width), kind)
    scratch = (
        [pltpu.VMEM(f.shape, BF16) for f in feats]
        + [pltpu.VMEM(w.shape, BF16) for w in lat_ws]
        + [pltpu.VMEM((3, *bias.shape), F32), pltpu.VMEM(smooth.shape, BF16)]
        + [pltpu.VMEM((2, 2, 3 * chans, chans), BF16)]
        + [pltpu.VMEM((rows[k] + 2, 4, images, cols[k] // 2, chans), BF16) for k in range(2)]
        + [strip(k, rows[k] + 2, 3 * chans, BF16) for k in (2, 3)]
        + [strip(k, min(rows[k], 2), chans, BF16) for k in range(1, 4)]
        + [strip(k, 2, chans, BF16) for k in range(4)]
        + [pltpu.VMEM((rows[0] + 2, images, blocks, cols[0], LANES), F32)]
        + [pltpu.VMEM((rows[1], images, blocks, cols[1], LANES), F32)]
        + [strip(2, rows[2], chans, F32)]
        + [pltpu.VMEM((images, rows[1], blocks, cols[1], LANES), F32)]
        + [pltpu.VMEM(o.shape, F32) for o in outs[2:]]
        + [pltpu.VMEM((2 * c, c), BF16) for c in cols[:3]]
        + [strip(k, 2, chans, BF16) for k in range(1, 4)]
        + [strip(k, 2, chans, F32) for k in range(2)]
        + [strip(1, rows[1], chans, BF16)]
        + [pltpu.VMEM((images, cols[0], chans), BF16)]
        + [
            pltpu.VMEM((n, -(-levels * images * 2 // (chans // GROUPS)), 1, chans), F32)
            for levels in (1, 3)
        ]
        + [dma((4,)), dma((4,)), dma((2,)), dma((1,))]
        + [dma((4, 2)), dma((4, 2)), dma((1,)), dma((2,))]
        + [dma((1,)) for _ in range(4)]
    )
    held = pl.pallas_call(
        functools.partial(kernel, n, geom),
        out_shape=[pltpu.VMEM((images, rows[0], blocks, cols[0], LANES), F32)]
        + [pltpu.VMEM(o.shape, BF16) for o in outs[1:]]
        + [pltpu.VMEM((two_rows, chans), F32)],
        in_specs=[any_spec] * 12,
        out_specs=[vmem_spec] * 5,
        scratch_shapes=scratch,
        compiler_params=pltpu.CompilerParams(
            collective_id=0, has_side_effects=True, vmem_limit_bytes=KERNEL_BYTES
        ),
    )(*args[:8], bias, gain, shift, smooth)
    held = [pltpu.with_memory_space_constraint(h, pltpu.VMEM) for h in held]
    return pl.pallas_call(
        functools.partial(finish_kernel, geom),
        out_shape=outs,
        in_specs=[vmem_spec] * 5,
        out_specs=[any_spec] * 4,
        scratch_shapes=[pltpu.VMEM(outs[0].shape, BF16), dma((4,)), dma((1,))],
        compiler_params=pltpu.CompilerParams(vmem_limit_bytes=16 * 1024 * 1024),
    )(held[0], held[4], *held[1:4])


def solution(mesh):
    strips = P("batch", "rows", None, None)
    run = functools.partial(per_device, mesh.shape["rows"])
    return jax.shard_map(
        lambda *args: tuple(run(*args)),
        mesh=mesh,
        in_specs=(strips,) * 4 + (P(),) * 8,
        out_specs=(strips,) * 4,
        check_vma=False,
    )
```

```python
import functools
import math

import jax
import jax.numpy as jnp
from jax import lax
from jax.experimental import pallas as pl
from jax.experimental.pallas import tpu as pltpu
from jax.sharding import PartitionSpec as P

GROUPS = 32
EPSILON = 1e-05
F32 = jnp.float32
BF16 = jnp.bfloat16
MESH = pl.DeviceIdType.MESH
KERNEL_BYTES = 52 * 1024 * 1024
LANES = 128


def halves_first(index, width, split):
    if not split:
        return index
    return 2 * (index % (width // 2)) + index // (width // 2)


def bilinear(cols, fine_split, coarse_split):
    half = cols // 2
    fine = halves_first(lax.broadcasted_iota(jnp.int32, (cols, cols), 0), cols, fine_split)
    place = lax.broadcasted_iota(jnp.int32, (cols, cols), 1)
    second = place >= half
    coarse = halves_first(jnp.where(second, place - half, place), half, coarse_split)
    near = fine // 2
    odd = fine % 2 == 1
    far = jnp.where(odd, jnp.minimum(near + 1, half - 1), jnp.maximum(near - 1, 0))
    value = jnp.where(coarse == near, 0.75, 0.0) + jnp.where(coarse == far, 0.25, 0.0)
    odd_rows = value * jnp.where(second, 0.25, 0.75)
    even_rows = value * jnp.where(second, 0.75, 0.25)
    return odd_rows.astype(BF16), even_rows.astype(BF16)


def mm(a, b):
    return jnp.dot(a, b, preferred_element_type=F32)


def group_totals(value, size):
    parts = []
    for start in range(0, value.shape[1], LANES):
        part = value[:, start : start + LANES]
        spot = lax.broadcasted_iota(jnp.int32, part.shape, 1) % size
        terms = [part]
        for step in range(1, size):
            terms.append(
                jnp.where(
                    spot >= step,
                    pltpu.roll(part, step, 1),
                    pltpu.roll(part, LANES + step - size, 1),
                )
            )
        while len(terms) > 1:
            terms = [sum(terms[j : j + 2]) for j in range(0, len(terms), 2)]
        parts.append(terms[0])
    return jnp.concatenate(parts, 1)


def own_slots(shape, size):
    row = lax.broadcasted_iota(jnp.int32, shape, 0)
    return lax.broadcasted_iota(jnp.int32, shape, 1) % size == row


def packed(stats, size):
    value = jnp.concatenate(stats, 0)
    value = jnp.where(own_slots(value.shape, size), group_totals(value, size), 0.0)
    return jnp.sum(value, 0, keepdims=True)


def unpacked(row, size):
    value = jnp.broadcast_to(row, (size, row.shape[1]))
    return group_totals(jnp.where(own_slots(value.shape, size), value, 0.0), size)


def kernel(n, geom, *refs):
    images, chans = geom["images"], geom["chans"]
    rows, cols = geom["rows"], geom["cols"]
    it = iter(refs)
    take = lambda count: [next(it) for _ in range(count)]
    feat_hbm, lat_hbm = take(4), take(4)
    consts_hbm, smooth_hbm = take(3), take(1)[0]
    (conv_two,) = take(1)
    done = [None] + take(3)
    (affine,) = take(1)
    feat, lat_w = take(4), take(4)
    consts, smooth, mixed = take(3)
    vee, big = take(2), [None, None] + take(2)
    sends, recvs, lats = [None] + take(3), take(4), take(3)
    conv = [conv_two] + take(3)
    ups, edge, hang = take(3), [None] + take(3), take(2)
    mid, hop = take(2)
    box_two, box_rest = take(2)
    in_sem, w_sem, s_sem, p_sem = take(4)
    halo_send, halo_recv, hop_send, hop_recv = take(4)
    two_send, two_recv, rest_send, rest_recv = take(4)
    bias, gain, shift = (consts.at[j] for j in range(3))

    me = lax.axis_index("rows")
    first, last = me == 0, me == n - 1
    size, blocks = chans // GROUPS, chans // LANES
    half = [c // 2 for c in cols]
    top = [r + 1 for r in rows]

    feat_copy = [pltpu.make_async_copy(feat_hbm[k], feat[k], in_sem.at[k]) for k in range(4)]
    lat_copy = [pltpu.make_async_copy(lat_hbm[k], lat_w[k], w_sem.at[k]) for k in range(4)]
    smooth_copy = [
        pltpu.make_async_copy(
            smooth_hbm.at[2 * j : 2 * j + 2], smooth.at[2 * j : 2 * j + 2], s_sem.at[j]
        )
        for j in range(2)
    ]
    feat_copy[3].start()
    lat_copy[3].start()
    for j in range(3):
        pltpu.make_async_copy(consts_hbm[j], consts.at[j], p_sem.at[0]).start()
    barrier = pltpu.get_barrier_semaphore()
    for d in range(1, n):
        pl.semaphore_signal(
            barrier, inc=1, device_id={"rows": lax.rem(me + d, n)}, device_id_type=MESH
        )
    for k in (2, 1, 0):
        lat_copy[k].start()
        feat_copy[k].start()
    for copy in smooth_copy:
        copy.start()

    @pl.when(first)
    def _():
        recvs[0][0] = jnp.zeros_like(recvs[0][0])

    @pl.when(last)
    def _():
        recvs[0][1] = jnp.zeros_like(recvs[0][1])

    for k in range(3):
        odd, even = bilinear(cols[k], k < 2, k == 0)
        ups[k][0 : cols[k]] = odd
        ups[k][cols[k] :] = even

    def remote(src, dst, send_sem, recv_sem, shift_by):
        return pltpu.make_async_remote_copy(
            src_ref=src,
            dst_ref=dst,
            send_sem=send_sem,
            recv_sem=recv_sem,
            device_id={"rows": lax.rem(me + (n + shift_by), n)},
            device_id_type=MESH,
        )

    def halo_source(k, way):
        if k == 0:
            return feat[0].at[:, way * (rows[0] - 1)]
        return sends[k].at[way * (sends[k].shape[0] - 1)]

    def halo_copy(k, way):
        return remote(
            halo_source(k, way),
            recvs[k].at[1 - way],
            halo_send.at[k, way],
            halo_recv.at[k, 1 - way],
            1 if way else -1,
        )

    def on_ends(act):
        @pl.when(jnp.logical_not(first))
        def _():
            act(0)

        @pl.when(jnp.logical_not(last))
        def _():
            act(1)

    def halo_start(k):
        on_ends(lambda way: halo_copy(k, way).start())

    def halo_wait(k):
        on_ends(lambda way: halo_copy(k, 1 - way).wait_recv())

    span = 2 * max(1, math.isqrt(n // 2))
    early = images // 2
    later = slice(early, images)
    pieces = (
        (slice(0, early), slice(0, cols[0])),
        (later, slice(0, half[0])),
        (later, slice(half[0], cols[0])),
    )
    place = lax.rem(me, span)
    crosses = (
        jnp.logical_and(place == 0, jnp.logical_not(first)),
        jnp.logical_and(place == span - 1, jnp.logical_not(last)),
    )
    carries = (
        jnp.logical_and(place == 0, me + span < n),
        jnp.logical_and(place == span - 1, me >= span),
    )
    relays = span < n
    hops = range(2) if early else range(1, 2)

    def fine_start():
        def begin(way):
            if not relays:
                halo_copy(0, way).start()
                return

            @pl.when(jnp.logical_not(crosses[way]))
            def _():
                halo_copy(0, way).start()

            @pl.when(crosses[way])
            def _():
                for j in (*hops, 2):
                    some, width = pieces[j]
                    last_hop = j == 2
                    remote(
                        feat[0].at[some, way * (rows[0] - 1), width],
                        recvs[0].at[1 - way, some, width] if last_hop else hop.at[some, width],
                        halo_send.at[0, way],
                        halo_recv.at[0, 1 - way] if last_hop else hop_recv.at[j],
                        (1 if last_hop else span) * (1 if way else -1),
                    ).start()

        on_ends(begin)

    def carry(act, ways=(0, 1)):
        if relays:
            for way in ways:
                pl.when(carries[way])(functools.partial(act, way))

    def carry_start(j, *ways):
        def act(way):
            some, width = pieces[j]
            here = hop.at[some, width]
            pltpu.make_async_copy(here, here, hop_recv.at[j]).wait()
            remote(
                here,
                recvs[0].at[1 - way, some, width],
                hop_send.at[j],
                halo_recv.at[0, 1 - way],
                1 - span if way else span - 1,
            ).start()

        if j in hops:
            carry(act, ways)

    pltpu.make_async_copy(consts, consts, p_sem.at[0]).wait()
    feat_copy[3].wait()
    lat_copy[3].wait()
    five = []
    for i in range(images):
        flat = feat[3][i].reshape(rows[3] * cols[3], -1)
        five.append((bias[3:4, :] + mm(flat, lat_w[3][...])).reshape(rows[3], cols[3], chans))
    for y in range(rows[3]):
        for i in range(images):
            sends[3][y, i] = five[i][y].astype(BF16)
    pl.semaphore_wait(barrier, n - 1)
    halo_start(3)

    lat_copy[2].wait()
    feat_copy[2].wait()
    for i in range(images):
        flat = feat[2][i].reshape(rows[2] * cols[2], -1)
        value = (bias[2:3, :] + mm(flat, lat_w[2][...])).reshape(rows[2], cols[2], chans)
        for y in range(rows[2]):
            lats[2][y, i] = value[y]
        sends[2][0, i] = value[0].astype(BF16)
        sends[2][1, i] = value[rows[2] - 1].astype(BF16)
    halo_start(2)

    def columns(k, r, i):
        return [
            jnp.concatenate(
                [lats[k][r, i, b, pl.ds(odd, half[k], stride=2), :] for b in range(blocks)], 1
            )
            for odd in range(2)
        ]

    def keep(k, r, i, value):
        for b in range(blocks):
            lats[k][r, i, b] = value[:, b * LANES : (b + 1) * LANES]

    lat_copy[1].wait()
    feat_copy[1].wait()

    def lateral_three(some):
        for i in range(images):
            flat = jnp.concatenate([feat[1][i, y] for y in some], 0)
            value = (bias[1:2, :] + mm(flat, lat_w[1][...])).reshape(len(some), cols[1], chans)
            for j, y in enumerate(some):
                keep(1, y, i, value[j])
        for y in some:
            if y in (0, rows[1] - 1):
                for i in range(images):
                    even, odd = columns(1, y, i)
                    sends[1][0 if y == 0 else 1, i, : half[1]] = even.astype(BF16)
                    sends[1][0 if y == 0 else 1, i, half[1] :] = odd.astype(BF16)

    lateral_three([0, rows[1] - 1])
    halo_start(1)
    lateral_three(list(range(1, rows[1] - 1)))

    def lateral_two(y):
        for i in range(images):
            flat = feat[0][i, y : y + 2].reshape(2 * cols[0], -1)
            value = bias[0:1, :] + mm(flat, lat_w[0][...])
            keep(0, y + 1, i, value[: cols[0]])
            keep(0, y + 2, i, value[cols[0] :])

    lat_copy[0].wait()
    feat_copy[0].wait()
    fine_start()
    steps = list(range(0, rows[0], 2))
    for y in steps[: len(steps) // 2]:
        lateral_two(y)

    def tap(k, a, b, start=0, count=chans):
        return smooth[k, pl.ds((3 * a + b) * chans + start, count)]

    smooth_copy[0].wait()
    piece = 16

    def mix(k, a, start):
        taps = [tap(k, a, b, start, piece).astype(F32) for b in range(3)]
        outer_taps, inner_tap = (taps[0] + taps[2]) * 0.5, taps[1] * 0.5
        mixed[k, 0, pl.ds(a * chans + start, piece)] = (outer_taps + inner_tap).astype(BF16)
        mixed[k, 1, pl.ds(a * chans + start, piece)] = (outer_taps - inner_tap).astype(BF16)

    for k in range(2):
        for a in range(3):
            for start in range(0, chans, piece):
                mix(k, a, start)
    for y in steps[len(steps) // 2 :]:
        lateral_two(y)
    smooth_copy[1].wait()

    def moved(value, by):
        length = value.shape[0]
        spot = lax.broadcasted_iota(jnp.int32, (8, value.shape[1]), 0)
        if by > 0:
            value = pltpu.roll(value, 1, 0)
            return jnp.concatenate([jnp.where(spot == 0, 0.0, value[:8]), value[8:]], 0)
        value = pltpu.roll(value, length - 1, 0)
        cut = length - 8
        return jnp.concatenate([value[:cut], jnp.where(spot == 7, 0.0, value[cut:])], 0)

    def put(k, r, i, value):
        big[k][r, i, :, 0:chans] = moved(value, 1).astype(BF16)
        big[k][r, i, :, chans : 2 * chans] = value.astype(BF16)
        big[k][r, i, :, 2 * chans :] = moved(value, -1).astype(BF16)

    def put_pairs(k, r, i, even, odd):
        vee[k][r, 0, i] = (moved(odd, 1) - odd).astype(BF16)
        vee[k][r, 1, i] = (even + odd).astype(BF16)
        vee[k][r, 2, i] = (odd - even).astype(BF16)
        vee[k][r, 3, i] = (even - moved(even, -1)).astype(BF16)

    def center(k, r, i):
        return big[k][r, i, :, chans : 2 * chans]

    def borders(k, i, above, below):
        edge[k][0, i] = jnp.where(first, center(k, 1, i), above.astype(BF16))
        edge[k][1, i] = jnp.where(last, center(k, rows[k], i), below.astype(BF16))
        put(k, 0, i, jnp.where(first, 0.0, above))
        put(k, top[k], i, jnp.where(last, 0.0, below))

    def pair(k, p, i):
        own = (lambda y: mid[y, i]) if k == 1 else (lambda y: center(k, y + 1, i))
        upper = edge[k][0, i] if p == 0 else own(p - 1)
        lower = edge[k][1, i] if p == rows[k] else own(p)
        return jnp.concatenate([upper, lower], 0)

    def folded(value):
        part = value.reshape(-1, 8, chans)
        return jnp.sum(part, 0), jnp.sum(part * part, 0)

    def conv_rows(k, apart):
        groups = [[i] for i in range(images)] if apart else [list(range(images))]
        sums = []
        for group in groups:
            bands = [
                jnp.concatenate([big[k][y + a, i] for i in group for y in range(rows[k])], 0)
                for a in range(3)
            ]
            total = mm(jnp.concatenate(bands, 1), smooth[k])
            total = total.reshape(len(group), rows[k], cols[k], chans)
            for j, i in enumerate(group):
                conv[k][i] = total[j]
                sums.append(folded(total[j]))
        return sums

    def conv_pairs(k, some, taps=(0, 1, 2), add=False, keep_sums=True):
        at = [slice(a * chans, (a + 1) * chans) for a in taps]
        weights = [
            jnp.concatenate([tap(k, a, 0) for a in taps], 0),
            jnp.concatenate([mixed[k, 0, here] for here in at], 0),
            jnp.concatenate([mixed[k, 1, here] for here in at], 0),
            jnp.concatenate([tap(k, a, 2) for a in taps], 0),
        ]
        parts = []
        for t in range(4):
            bands = [
                jnp.concatenate([vee[k][y + a, t, i] for y in some for i in range(images)], 0)
                for a in taps
            ]
            parts.append(mm(jnp.concatenate(bands, 1), weights[t]))
        even = (parts[1] + parts[2]) + parts[0]
        odd = (parts[1] - parts[2]) - parts[3]
        sums = [None] * images
        for j, (y, i) in enumerate((y, i) for y in some for i in range(images)):
            here = slice(j * half[k], (j + 1) * half[k])
            values = []
            for odd_ones, value in ((0, even[here]), (1, odd[here])):
                spots = [
                    conv[k].at[i, y, b, pl.ds(odd_ones, half[k], stride=2), :]
                    for b in range(blocks)
                ]
                if add:
                    value = value + jnp.concatenate([spot[...] for spot in spots], 1)
                for b, spot in enumerate(spots):
                    spot[...] = value[:, b * LANES : (b + 1) * LANES]
                values.append(value)
            if keep_sums:
                new = joined([[folded(value)] for value in values])[0]
                sums[i] = new if sums[i] is None else joined([[sums[i]], [new]])[0]
        return sums

    def joined(parts):
        total = parts[0]
        for part in parts[1:]:
            total = [(t[0] + u[0], t[1] + u[1]) for t, u in zip(total, part)]
        return total

    def stat_rows(sums):
        return [jnp.sum(part, 0, keepdims=True) for pair in sums for part in pair]

    def post(box, rows_of, send_sem, recv_sem):
        for j in range(box.shape[1]):
            some = rows_of[j * size : (j + 1) * size]
            some = some + [jnp.zeros_like(some[0])] * (size - len(some))
            box[0, j] = packed(some, size)
        for d in range(1, n):
            remote(box.at[0], box.at[d], send_sem.at[0], recv_sem.at[0], d).start()

    def all_of(box, sem):
        pltpu.make_async_copy(box.at[1:n], box.at[1:n], sem.at[0]).wait()

    def gathered(box):
        stats = []
        for j in range(box.shape[1]):
            total = box[0, j]
            for d in range(1, n):
                total = total + box[d, j]
            stats.append(unpacked(total, size))
        return jnp.concatenate(stats, 0)

    for i in range(images):
        for y in range(rows[3]):
            put(3, y + 1, i, five[i][y])
    halo_wait(3)
    for i in range(images):
        borders(3, i, recvs[3][0, i].astype(F32), recvs[3][1, i].astype(F32))

    outer = {}
    for p in range(rows[3] + 1):
        for i in range(images):
            both = mm(ups[2][...], pair(3, p, i))
            for y, value in ((2 * p - 1, both[: cols[2]]), (2 * p, both[cols[2] :])):
                if 0 <= y < rows[2]:
                    put(2, y + 1, i, lats[2][y, i] + value)
                else:
                    outer[y, i] = value
    def merge(k, p):
        for i in range(images):
            coarse = pair(k + 1, p, i)
            for y in (2 * p - 1, 2 * p):
                value = mm(ups[k][: cols[k]] if y < 2 * p else ups[k][cols[k] :], coarse)
                if not 0 <= y < rows[k]:
                    if k == 0:
                        value = jnp.where(first if y < 0 else last, 0.0, value + bias[0:1, :])
                    hang[k][0 if y < 0 else 1, i] = value
                    continue
                even, odd = columns(k, y + 1 if k == 0 else y, i)
                even = even + value[: half[k]]
                odd = odd + value[half[k] :]
                if k:
                    mid[y, i, : half[k]] = even.astype(BF16)
                    mid[y, i, half[k] :] = odd.astype(BF16)
                put_pairs(k, y + 1, i, even, odd)

    sums_five = conv_rows(3, False)
    for p in range(1, rows[2]):
        merge(1, p)
    for p in range(2, rows[1] - 1):
        merge(0, p)

    carry_start(0, 1)
    halo_wait(2)
    for i in range(images):
        borders(
            2,
            i,
            recvs[2][0, i].astype(F32) + outer[-1, i],
            recvs[2][1, i].astype(F32) + outer[rows[2], i],
        )

    merge(1, 0)
    merge(1, rows[2])
    merge(0, 1)
    merge(0, rows[1] - 1)
    sums_four = conv_rows(2, True)
    sums_three = [conv_pairs(1, list(range(1, rows[1] - 1)))]
    sums_two = []

    def conv_two_row(y):
        sums_two.append(conv_pairs(0, [y]))

    inner = list(range(2, rows[0] - 2))
    ahead = len(inner) * 3 // 4
    for y in inner[:ahead]:
        conv_two_row(y)

    carry_start(0, 0)
    carry_start(1, 0, 1)
    halo_wait(1)
    for way in range(2):
        for i in range(images):
            value = recvs[1][way, i].astype(F32) + hang[1][way, i]
            none = last if way else first
            own = mid[way * (rows[1] - 1), i]
            edge[1][way, i] = jnp.where(none, own, value.astype(BF16))
            value = jnp.where(none, 0.0, value)
            put_pairs(1, way * top[1], i, value[: half[1]], value[half[1] :])
    merge(0, 0)
    merge(0, rows[1])
    sums_three.append(conv_pairs(1, [0, rows[1] - 1]))
    for y in inner[ahead:]:
        conv_two_row(y)
    conv_two_row(1)
    conv_two_row(rows[0] - 2)
    conv_pairs(0, [0], (1, 2), keep_sums=False)
    conv_pairs(0, [rows[0] - 1], (0, 1), keep_sums=False)
    rest_rows = stat_rows(joined(sums_three)) + stat_rows(sums_four) + stat_rows(sums_five)
    post(box_rest, rest_rows, rest_send, rest_recv)

    halo_wait(0)
    for way in range(2):
        for i in range(images):
            keep(0, way * top[0], i, mm(recvs[0][way, i], lat_w[0][...]))
    for way in range(2):
        for i in range(images):
            even, odd = columns(0, way * top[0], i)
            even = even + hang[0][way, i, : half[0]]
            odd = odd + hang[0][way, i, half[0] :]
            put_pairs(0, way * top[0], i, even, odd)
    sums_two.append(conv_pairs(0, [0], (0,), add=True))
    sums_two.append(conv_pairs(0, [rows[0] - 1], (2,), add=True))
    post(box_two, stat_rows(joined(sums_two)), two_send, two_recv)

    def scales(k, total, square):
        share = 1.0 / float(rows[k] * n * cols[k] * size)
        mean = total * share
        variance = square * share - mean * mean
        scale = lax.rsqrt(variance + EPSILON) * gain[k : k + 1, :]
        return scale, shift[k : k + 1, :] - mean * scale

    all_of(box_rest, rest_recv)
    coarse = gathered(box_rest)
    for k in (1, 2, 3):
        for i in range(images):
            slot = ((k - 1) * images + i) * 2
            scale, offset = scales(k, coarse[slot : slot + 1], coarse[slot + 1 : slot + 2])
            if k == 1:
                for y in range(rows[k]):
                    value = jnp.concatenate([conv[k][i, y, b] for b in range(blocks)], 1)
                    done[k][i, y] = (value * scale + offset).astype(BF16)
            else:
                done[k][i] = (conv[k][i] * scale + offset).astype(BF16)
    on_ends(lambda way: [halo_copy(k, way).wait_send() for k in range(4)])
    for j in hops:
        here = hop.at[pieces[j]]
        carry(lambda way, h=here, j=j: pltpu.make_async_copy(h, h, hop_send.at[j]).wait())
    all_of(box_rest, rest_send)

    all_of(box_two, two_recv)
    two = gathered(box_two)
    for i in range(images):
        scale, offset = scales(0, two[2 * i : 2 * i + 1], two[2 * i + 1 : 2 * i + 2])
        affine[2 * i : 2 * i + 1, :] = scale
        affine[2 * i + 1 : 2 * i + 2, :] = offset
    all_of(box_two, two_send)


def finish_kernel(geom, *refs):
    images, rows = geom["images"], geom["rows"]
    conv_two, affine = refs[0:2]
    done = [None, *refs[2:5]]
    out_hbm, staged, rest_sem, two_sem = refs[5:9], refs[9], refs[10], refs[11]
    copies = []
    for k in (1, 2, 3):
        copies.append(pltpu.make_async_copy(done[k], out_hbm[k], rest_sem.at[k]))
        copies[-1].start()
    for i in range(images):
        scale = affine[2 * i : 2 * i + 1, :]
        offset = affine[2 * i + 1 : 2 * i + 2, :]
        for y in range(rows[0]):
            value = jnp.concatenate(
                [conv_two[i, y, b] for b in range(conv_two.shape[2])], 1
            )
            staged[i, y] = (value * scale + offset).astype(BF16)
            pltpu.make_async_copy(
                staged.at[i, y], out_hbm[0].at[i, y], two_sem.at[0]
            ).start()
    for copy in copies:
        copy.wait()
    pltpu.make_async_copy(staged, out_hbm[0], two_sem.at[0]).wait()


def per_device(n, *args):
    feats, lat_ws = args[0:4], args[4:8]
    bias, smooth, gain, shift = args[8:12]
    smooth = smooth.reshape(smooth.shape[0], -1, smooth.shape[3])
    images, chans = feats[0].shape[0], lat_ws[0].shape[1]
    rows = [f.shape[1] for f in feats]
    cols = [f.shape[2] for f in feats]
    geom = {"images": images, "chans": chans, "rows": rows, "cols": cols}
    any_spec = pl.BlockSpec(memory_space=pltpu.HBM)
    vmem_spec = pl.BlockSpec(memory_space=pltpu.VMEM)
    outs = [jax.ShapeDtypeStruct((images, r, c, chans), BF16) for r, c in zip(rows, cols)]
    dma = pltpu.SemaphoreType.DMA
    blocks = chans // LANES
    two_rows = -(-(images * 2) // 8) * 8
    strip = lambda k, count, width, kind: pltpu.VMEM((count, images, cols[k], width), kind)
    scratch = (
        [pltpu.VMEM(f.shape, BF16) for f in feats]
        + [pltpu.VMEM(w.shape, BF16) for w in lat_ws]
        + [pltpu.VMEM((3, *bias.shape), F32), pltpu.VMEM(smooth.shape, BF16)]
        + [pltpu.VMEM((2, 2, 3 * chans, chans), BF16)]
        + [pltpu.VMEM((rows[k] + 2, 4, images, cols[k] // 2, chans), BF16) for k in range(2)]
        + [strip(k, rows[k] + 2, 3 * chans, BF16) for k in (2, 3)]
        + [strip(k, min(rows[k], 2), chans, BF16) for k in range(1, 4)]
        + [strip(k, 2, chans, BF16) for k in range(4)]
        + [pltpu.VMEM((rows[0] + 2, images, blocks, cols[0], LANES), F32)]
        + [pltpu.VMEM((rows[1], images, blocks, cols[1], LANES), F32)]
        + [strip(2, rows[2], chans, F32)]
        + [pltpu.VMEM((images, rows[1], blocks, cols[1], LANES), F32)]
        + [pltpu.VMEM(o.shape, F32) for o in outs[2:]]
        + [pltpu.VMEM((2 * c, c), BF16) for c in cols[:3]]
        + [strip(k, 2, chans, BF16) for k in range(1, 4)]
        + [strip(k, 2, chans, F32) for k in range(2)]
        + [strip(1, rows[1], chans, BF16)]
        + [pltpu.VMEM((images, cols[0], chans), BF16)]
        + [
            pltpu.VMEM((n, -(-levels * images * 2 // (chans // GROUPS)), 1, chans), F32)
            for levels in (1, 3)
        ]
        + [dma((4,)), dma((4,)), dma((2,)), dma((1,))]
        + [dma((4, 2)), dma((4, 2)), dma((2,)), dma((2,))]
        + [dma((1,)) for _ in range(4)]
    )
    held = pl.pallas_call(
        functools.partial(kernel, n, geom),
        out_shape=[pltpu.VMEM((images, rows[0], blocks, cols[0], LANES), F32)]
        + [pltpu.VMEM(o.shape, BF16) for o in outs[1:]]
        + [pltpu.VMEM((two_rows, chans), F32)],
        in_specs=[any_spec] * 12,
        out_specs=[vmem_spec] * 5,
        scratch_shapes=scratch,
        compiler_params=pltpu.CompilerParams(
            collective_id=0, has_side_effects=True, vmem_limit_bytes=KERNEL_BYTES
        ),
    )(*args[:8], bias, gain, shift, smooth)
    held = [pltpu.with_memory_space_constraint(h, pltpu.VMEM) for h in held]
    return pl.pallas_call(
        functools.partial(finish_kernel, geom),
        out_shape=outs,
        in_specs=[vmem_spec] * 5,
        out_specs=[any_spec] * 4,
        scratch_shapes=[pltpu.VMEM(outs[0].shape, BF16), dma((4,)), dma((1,))],
        compiler_params=pltpu.CompilerParams(vmem_limit_bytes=16 * 1024 * 1024),
    )(held[0], held[4], *held[1:4])


def solution(mesh):
    strips = P("batch", "rows", None, None)
    run = functools.partial(per_device, mesh.shape["rows"])
    return jax.shard_map(
        lambda *args: tuple(run(*args)),
        mesh=mesh,
        in_specs=(strips,) * 4 + (P(),) * 8,
        out_specs=(strips,) * 4,
        check_vma=False,
    )
```

```python
import functools
import math

import jax
import jax.numpy as jnp
from jax import lax
from jax.experimental import pallas as pl
from jax.experimental.pallas import tpu as pltpu
from jax.sharding import PartitionSpec as P

GROUPS = 32
EPSILON = 1e-05
F32 = jnp.float32
BF16 = jnp.bfloat16
MESH = pl.DeviceIdType.MESH
KERNEL_BYTES = 52 * 1024 * 1024
LANES = 128


def halves_first(index, width, split):
    if not split:
        return index
    return 2 * (index % (width // 2)) + index // (width // 2)


def bilinear(cols, fine_split, coarse_split):
    half = cols // 2
    fine = halves_first(lax.broadcasted_iota(jnp.int32, (cols, cols), 0), cols, fine_split)
    place = lax.broadcasted_iota(jnp.int32, (cols, cols), 1)
    second = place >= half
    coarse = halves_first(jnp.where(second, place - half, place), half, coarse_split)
    near = fine // 2
    odd = fine % 2 == 1
    far = jnp.where(odd, jnp.minimum(near + 1, half - 1), jnp.maximum(near - 1, 0))
    value = jnp.where(coarse == near, 0.75, 0.0) + jnp.where(coarse == far, 0.25, 0.0)
    odd_rows = value * jnp.where(second, 0.25, 0.75)
    even_rows = value * jnp.where(second, 0.75, 0.25)
    return odd_rows.astype(BF16), even_rows.astype(BF16)


def mm(a, b):
    return jnp.dot(a, b, preferred_element_type=F32)


def group_totals(value, size):
    parts = []
    for start in range(0, value.shape[1], LANES):
        part = value[:, start : start + LANES]
        spot = lax.broadcasted_iota(jnp.int32, part.shape, 1) % size
        terms = [part]
        for step in range(1, size):
            terms.append(
                jnp.where(
                    spot >= step,
                    pltpu.roll(part, step, 1),
                    pltpu.roll(part, LANES + step - size, 1),
                )
            )
        while len(terms) > 1:
            terms = [sum(terms[j : j + 2]) for j in range(0, len(terms), 2)]
        parts.append(terms[0])
    return jnp.concatenate(parts, 1)


def own_slots(shape, size):
    row = lax.broadcasted_iota(jnp.int32, shape, 0)
    return lax.broadcasted_iota(jnp.int32, shape, 1) % size == row


def packed(stats, size):
    value = jnp.concatenate(stats, 0)
    value = jnp.where(own_slots(value.shape, size), group_totals(value, size), 0.0)
    return jnp.sum(value, 0, keepdims=True)


def unpacked(row, size):
    value = jnp.broadcast_to(row, (size, row.shape[1]))
    return group_totals(jnp.where(own_slots(value.shape, size), value, 0.0), size)


def kernel(n, geom, *refs):
    images, chans = geom["images"], geom["chans"]
    rows, cols = geom["rows"], geom["cols"]
    it = iter(refs)
    take = lambda count: [next(it) for _ in range(count)]
    feat_hbm, lat_hbm = take(4), take(4)
    consts_hbm, smooth_hbm = take(3), take(1)[0]
    (conv_two,) = take(1)
    done = [None] + take(3)
    (affine,) = take(1)
    feat, lat_w = take(4), take(4)
    consts, smooth, mixed = take(3)
    vee, big = take(2), [None, None] + take(2)
    sends, recvs, lats = [None] + take(3), take(4), take(3)
    conv = [conv_two] + take(3)
    ups, edge, hang = take(3), [None] + take(3), take(2)
    mid, hop = take(2)
    box_two, box_rest = take(2)
    in_sem, w_sem, s_sem, p_sem = take(4)
    halo_send, halo_recv, hop_send, hop_recv = take(4)
    two_send, two_recv, rest_send, rest_recv = take(4)
    bias, gain, shift = (consts.at[j] for j in range(3))

    me = lax.axis_index("rows")
    first, last = me == 0, me == n - 1
    size, blocks = chans // GROUPS, chans // LANES
    half = [c // 2 for c in cols]
    top = [r + 1 for r in rows]

    feat_copy = [pltpu.make_async_copy(feat_hbm[k], feat[k], in_sem.at[k]) for k in range(4)]
    lat_copy = [pltpu.make_async_copy(lat_hbm[k], lat_w[k], w_sem.at[k]) for k in range(4)]
    smooth_copy = [
        pltpu.make_async_copy(
            smooth_hbm.at[2 * j : 2 * j + 2], smooth.at[2 * j : 2 * j + 2], s_sem.at[j]
        )
        for j in range(2)
    ]
    feat_copy[3].start()
    lat_copy[3].start()
    for j in range(3):
        pltpu.make_async_copy(consts_hbm[j], consts.at[j], p_sem.at[0]).start()
    barrier = pltpu.get_barrier_semaphore()
    for d in range(1, n):
        pl.semaphore_signal(
            barrier, inc=1, device_id={"rows": lax.rem(me + d, n)}, device_id_type=MESH
        )
    for k in (2, 1, 0):
        lat_copy[k].start()
        feat_copy[k].start()
    for copy in smooth_copy:
        copy.start()

    @pl.when(first)
    def _():
        recvs[0][0] = jnp.zeros_like(recvs[0][0])

    @pl.when(last)
    def _():
        recvs[0][1] = jnp.zeros_like(recvs[0][1])

    for k in range(3):
        odd, even = bilinear(cols[k], k < 2, k == 0)
        ups[k][0 : cols[k]] = odd
        ups[k][cols[k] :] = even

    def remote(src, dst, send_sem, recv_sem, shift_by):
        return pltpu.make_async_remote_copy(
            src_ref=src,
            dst_ref=dst,
            send_sem=send_sem,
            recv_sem=recv_sem,
            device_id={"rows": lax.rem(me + (n + shift_by), n)},
            device_id_type=MESH,
        )

    def halo_source(k, way):
        if k == 0:
            return feat[0].at[:, way * (rows[0] - 1)]
        return sends[k].at[way * (sends[k].shape[0] - 1)]

    def halo_copy(k, way):
        return remote(
            halo_source(k, way),
            recvs[k].at[1 - way],
            halo_send.at[k, way],
            halo_recv.at[k, 1 - way],
            1 if way else -1,
        )

    def on_ends(act):
        @pl.when(jnp.logical_not(first))
        def _():
            act(0)

        @pl.when(jnp.logical_not(last))
        def _():
            act(1)

    def halo_start(k):
        on_ends(lambda way: halo_copy(k, way).start())

    def halo_wait(k):
        on_ends(lambda way: halo_copy(k, 1 - way).wait_recv())

    span = 2 * max(1, math.isqrt(n // 2))
    early = images // 2
    later = slice(early, images)
    pieces = (
        (slice(0, early), slice(0, cols[0])),
        (later, slice(0, half[0])),
        (later, slice(half[0], cols[0])),
    )
    place = lax.rem(me, span)
    crosses = (
        jnp.logical_and(place == 0, jnp.logical_not(first)),
        jnp.logical_and(place == span - 1, jnp.logical_not(last)),
    )
    carries = (
        jnp.logical_and(place == 0, me + span < n),
        jnp.logical_and(place == span - 1, me >= span),
    )
    relays = span < n
    hops = range(2) if early else range(1, 2)

    def fine_start():
        def begin(way):
            if not relays:
                halo_copy(0, way).start()
                return

            @pl.when(jnp.logical_not(crosses[way]))
            def _():
                halo_copy(0, way).start()

            @pl.when(crosses[way])
            def _():
                for j in (*hops, 2):
                    some, width = pieces[j]
                    last_hop = j == 2
                    remote(
                        feat[0].at[some, way * (rows[0] - 1), width],
                        recvs[0].at[1 - way, some, width] if last_hop else hop.at[some, width],
                        halo_send.at[0, way],
                        halo_recv.at[0, 1 - way] if last_hop else hop_recv.at[j],
                        (1 if last_hop else span) * (1 if way else -1),
                    ).start()

        on_ends(begin)

    def carry(act, ways=(0, 1)):
        if relays:
            for way in ways:
                pl.when(carries[way])(functools.partial(act, way))

    def carry_start(j, *ways):
        def act(way):
            some, width = pieces[j]
            here = hop.at[some, width]
            pltpu.make_async_copy(here, here, hop_recv.at[j]).wait()
            remote(
                here,
                recvs[0].at[1 - way, some, width],
                hop_send.at[j],
                halo_recv.at[0, 1 - way],
                1 - span if way else span - 1,
            ).start()

        if j in hops:
            carry(act, ways)

    pltpu.make_async_copy(consts, consts, p_sem.at[0]).wait()
    feat_copy[3].wait()
    lat_copy[3].wait()
    flat = feat[3][...].reshape(-1, feat[3].shape[-1])
    five = [
        mm(flat, lat_w[3][:, b * LANES : (b + 1) * LANES]) for b in range(blocks)
    ]
    five = bias[3:4, :] + jnp.concatenate(five, 1)
    five = five.reshape(images, rows[3], cols[3], chans)
    for y in range(rows[3]):
        for i in range(images):
            sends[3][y, i] = five[i, y].astype(BF16)
    pl.semaphore_wait(barrier, n - 1)
    halo_start(3)

    lat_copy[2].wait()
    feat_copy[2].wait()
    for i in range(images):
        flat = feat[2][i].reshape(rows[2] * cols[2], -1)
        value = (bias[2:3, :] + mm(flat, lat_w[2][...])).reshape(rows[2], cols[2], chans)
        for y in range(rows[2]):
            lats[2][y, i] = value[y]
        sends[2][0, i] = value[0].astype(BF16)
        sends[2][1, i] = value[rows[2] - 1].astype(BF16)
    halo_start(2)

    def columns(k, r, i):
        return [
            jnp.concatenate(
                [lats[k][r, i, b, pl.ds(odd, half[k], stride=2), :] for b in range(blocks)], 1
            )
            for odd in range(2)
        ]

    def keep(k, r, i, value):
        for b in range(blocks):
            lats[k][r, i, b] = value[:, b * LANES : (b + 1) * LANES]

    lat_copy[1].wait()
    feat_copy[1].wait()

    def lateral_three(some):
        for i in range(images):
            flat = jnp.concatenate([feat[1][i, y] for y in some], 0)
            value = (bias[1:2, :] + mm(flat, lat_w[1][...])).reshape(len(some), cols[1], chans)
            for j, y in enumerate(some):
                keep(1, y, i, value[j])
        for y in some:
            if y in (0, rows[1] - 1):
                for i in range(images):
                    even, odd = columns(1, y, i)
                    sends[1][0 if y == 0 else 1, i, : half[1]] = even.astype(BF16)
                    sends[1][0 if y == 0 else 1, i, half[1] :] = odd.astype(BF16)

    lateral_three([0, rows[1] - 1])
    halo_start(1)
    lateral_three(list(range(1, rows[1] - 1)))

    def lateral_two(y):
        for i in range(images):
            flat = feat[0][i, y : y + 2].reshape(2 * cols[0], -1)
            value = bias[0:1, :] + mm(flat, lat_w[0][...])
            keep(0, y + 1, i, value[: cols[0]])
            keep(0, y + 2, i, value[cols[0] :])

    lat_copy[0].wait()
    feat_copy[0].wait()
    fine_start()
    steps = list(range(0, rows[0], 2))
    for y in steps[: len(steps) // 2]:
        lateral_two(y)

    def tap(k, a, b, start=0, count=chans):
        return smooth[k, pl.ds((3 * a + b) * chans + start, count)]

    smooth_copy[0].wait()
    piece = 16

    def mix(k, a, start):
        taps = [tap(k, a, b, start, piece).astype(F32) for b in range(3)]
        outer_taps, inner_tap = (taps[0] + taps[2]) * 0.5, taps[1] * 0.5
        mixed[k, 0, pl.ds(a * chans + start, piece)] = (outer_taps + inner_tap).astype(BF16)
        mixed[k, 1, pl.ds(a * chans + start, piece)] = (outer_taps - inner_tap).astype(BF16)

    for k in range(2):
        for a in range(3):
            for start in range(0, chans, piece):
                mix(k, a, start)
    for y in steps[len(steps) // 2 :]:
        lateral_two(y)
    smooth_copy[1].wait()

    def moved(value, by):
        length = value.shape[0]
        spot = lax.broadcasted_iota(jnp.int32, (8, value.shape[1]), 0)
        if by > 0:
            value = pltpu.roll(value, 1, 0)
            return jnp.concatenate([jnp.where(spot == 0, 0.0, value[:8]), value[8:]], 0)
        value = pltpu.roll(value, length - 1, 0)
        cut = length - 8
        return jnp.concatenate([value[:cut], jnp.where(spot == 7, 0.0, value[cut:])], 0)

    def put(k, r, i, value):
        big[k][r, i, :, 0:chans] = moved(value, 1).astype(BF16)
        big[k][r, i, :, chans : 2 * chans] = value.astype(BF16)
        big[k][r, i, :, 2 * chans :] = moved(value, -1).astype(BF16)

    def put_pairs(k, r, i, even, odd):
        vee[k][r, 0, i] = (moved(odd, 1) - odd).astype(BF16)
        vee[k][r, 1, i] = (even + odd).astype(BF16)
        vee[k][r, 2, i] = (odd - even).astype(BF16)
        vee[k][r, 3, i] = (even - moved(even, -1)).astype(BF16)

    def center(k, r, i):
        return big[k][r, i, :, chans : 2 * chans]

    def borders(k, i, above, below):
        edge[k][0, i] = jnp.where(first, center(k, 1, i), above.astype(BF16))
        edge[k][1, i] = jnp.where(last, center(k, rows[k], i), below.astype(BF16))
        put(k, 0, i, jnp.where(first, 0.0, above))
        put(k, top[k], i, jnp.where(last, 0.0, below))

    def pair(k, p, i):
        own = (lambda y: mid[y, i]) if k == 1 else (lambda y: center(k, y + 1, i))
        upper = edge[k][0, i] if p == 0 else own(p - 1)
        lower = edge[k][1, i] if p == rows[k] else own(p)
        return jnp.concatenate([upper, lower], 0)

    def folded(value):
        part = value.reshape(-1, 8, chans)
        return jnp.sum(part, 0), jnp.sum(part * part, 0)

    def conv_rows(k, apart):
        groups = [[i] for i in range(images)] if apart else [list(range(images))]
        sums = []
        for group in groups:
            bands = [
                jnp.concatenate([big[k][y + a, i] for i in group for y in range(rows[k])], 0)
                for a in range(3)
            ]
            total = mm(jnp.concatenate(bands, 1), smooth[k])
            total = total.reshape(len(group), rows[k], cols[k], chans)
            for j, i in enumerate(group):
                conv[k][i] = total[j]
                sums.append(folded(total[j]))
        return sums

    def conv_pairs(k, some, taps=(0, 1, 2), add=False, keep_sums=True):
        at = [slice(a * chans, (a + 1) * chans) for a in taps]
        weights = [
            jnp.concatenate([tap(k, a, 0) for a in taps], 0),
            jnp.concatenate([mixed[k, 0, here] for here in at], 0),
            jnp.concatenate([mixed[k, 1, here] for here in at], 0),
            jnp.concatenate([tap(k, a, 2) for a in taps], 0),
        ]
        parts = []
        for t in range(4):
            bands = [
                jnp.concatenate([vee[k][y + a, t, i] for y in some for i in range(images)], 0)
                for a in taps
            ]
            parts.append(mm(jnp.concatenate(bands, 1), weights[t]))
        even = (parts[1] + parts[2]) + parts[0]
        odd = (parts[1] - parts[2]) - parts[3]
        sums = [None] * images
        for j, (y, i) in enumerate((y, i) for y in some for i in range(images)):
            here = slice(j * half[k], (j + 1) * half[k])
            values = []
            for odd_ones, value in ((0, even[here]), (1, odd[here])):
                spots = [
                    conv[k].at[i, y, b, pl.ds(odd_ones, half[k], stride=2), :]
                    for b in range(blocks)
                ]
                if add:
                    value = value + jnp.concatenate([spot[...] for spot in spots], 1)
                for b, spot in enumerate(spots):
                    spot[...] = value[:, b * LANES : (b + 1) * LANES]
                values.append(value)
            if keep_sums:
                new = joined([[folded(value)] for value in values])[0]
                sums[i] = new if sums[i] is None else joined([[sums[i]], [new]])[0]
        return sums

    def joined(parts):
        total = parts[0]
        for part in parts[1:]:
            total = [(t[0] + u[0], t[1] + u[1]) for t, u in zip(total, part)]
        return total

    def stat_rows(sums):
        return [jnp.sum(part, 0, keepdims=True) for pair in sums for part in pair]

    def post(box, rows_of, send_sem, recv_sem):
        for j in range(box.shape[1]):
            some = rows_of[j * size : (j + 1) * size]
            some = some + [jnp.zeros_like(some[0])] * (size - len(some))
            box[0, j] = packed(some, size)
        for d in range(1, n):
            remote(box.at[0], box.at[d], send_sem.at[0], recv_sem.at[0], d).start()

    def all_of(box, sem):
        pltpu.make_async_copy(box.at[1:n], box.at[1:n], sem.at[0]).wait()

    def gathered(box):
        stats = []
        for j in range(box.shape[1]):
            total = box[0, j]
            for d in range(1, n):
                total = total + box[d, j]
            stats.append(unpacked(total, size))
        return jnp.concatenate(stats, 0)

    for i in range(images):
        for y in range(rows[3]):
            put(3, y + 1, i, five[i, y])
    halo_wait(3)
    for i in range(images):
        borders(3, i, recvs[3][0, i].astype(F32), recvs[3][1, i].astype(F32))

    outer = {}
    for p in range(rows[3] + 1):
        for i in range(images):
            both = mm(ups[2][...], pair(3, p, i))
            for y, value in ((2 * p - 1, both[: cols[2]]), (2 * p, both[cols[2] :])):
                if 0 <= y < rows[2]:
                    put(2, y + 1, i, lats[2][y, i] + value)
                else:
                    outer[y, i] = value
    def merge(k, p):
        for i in range(images):
            coarse = pair(k + 1, p, i)
            for y in (2 * p - 1, 2 * p):
                value = mm(ups[k][: cols[k]] if y < 2 * p else ups[k][cols[k] :], coarse)
                if not 0 <= y < rows[k]:
                    if k == 0:
                        value = jnp.where(first if y < 0 else last, 0.0, value + bias[0:1, :])
                    hang[k][0 if y < 0 else 1, i] = value
                    continue
                even, odd = columns(k, y + 1 if k == 0 else y, i)
                even = even + value[: half[k]]
                odd = odd + value[half[k] :]
                if k:
                    mid[y, i, : half[k]] = even.astype(BF16)
                    mid[y, i, half[k] :] = odd.astype(BF16)
                put_pairs(k, y + 1, i, even, odd)

    sums_five = conv_rows(3, False)
    for p in range(1, rows[2]):
        merge(1, p)
    for p in range(2, rows[1] - 1):
        merge(0, p)

    carry_start(0, 1)
    halo_wait(2)
    for i in range(images):
        borders(
            2,
            i,
            recvs[2][0, i].astype(F32) + outer[-1, i],
            recvs[2][1, i].astype(F32) + outer[rows[2], i],
        )

    merge(1, 0)
    merge(1, rows[2])
    sums_four = conv_rows(2, True)
    merge(0, 1)
    sums_three = [conv_pairs(1, list(range(1, rows[1] - 1)))]
    sums_two = []

    def conv_two_row(y):
        sums_two.append(conv_pairs(0, [y]))

    inner = list(range(2, rows[0] - 2))
    ahead = len(inner) * 3 // 4
    for y in inner[:ahead]:
        if y == inner[min(2, ahead - 1)]:
            merge(0, rows[1] - 1)
        conv_two_row(y)

    carry_start(0, 0)
    carry_start(1, 0, 1)
    halo_wait(1)
    for way in range(2):
        for i in range(images):
            value = recvs[1][way, i].astype(F32) + hang[1][way, i]
            none = last if way else first
            own = mid[way * (rows[1] - 1), i]
            edge[1][way, i] = jnp.where(none, own, value.astype(BF16))
            value = jnp.where(none, 0.0, value)
            put_pairs(1, way * top[1], i, value[: half[1]], value[half[1] :])
    merge(0, 0)
    merge(0, rows[1])
    sums_three.append(conv_pairs(1, [0, rows[1] - 1]))
    for y in inner[ahead:]:
        conv_two_row(y)
    conv_two_row(1)
    conv_two_row(rows[0] - 2)
    conv_pairs(0, [0], (1, 2), keep_sums=False)
    conv_pairs(0, [rows[0] - 1], (0, 1), keep_sums=False)
    rest_rows = stat_rows(joined(sums_three)) + stat_rows(sums_four) + stat_rows(sums_five)
    post(box_rest, rest_rows, rest_send, rest_recv)

    halo_wait(0)
    for way in range(2):
        for i in range(images):
            keep(0, way * top[0], i, mm(recvs[0][way, i], lat_w[0][...]))
    for way in range(2):
        for i in range(images):
            even, odd = columns(0, way * top[0], i)
            even = even + hang[0][way, i, : half[0]]
            odd = odd + hang[0][way, i, half[0] :]
            put_pairs(0, way * top[0], i, even, odd)
    sums_two.append(conv_pairs(0, [0], (0,), add=True))
    sums_two.append(conv_pairs(0, [rows[0] - 1], (2,), add=True))
    post(box_two, stat_rows(joined(sums_two)), two_send, two_recv)

    def scales(k, total, square):
        share = 1.0 / float(rows[k] * n * cols[k] * size)
        mean = total * share
        variance = square * share - mean * mean
        scale = lax.rsqrt(variance + EPSILON) * gain[k : k + 1, :]
        return scale, shift[k : k + 1, :] - mean * scale

    all_of(box_rest, rest_recv)
    coarse = gathered(box_rest)
    for k in (1, 2, 3):
        for i in range(images):
            slot = ((k - 1) * images + i) * 2
            scale, offset = scales(k, coarse[slot : slot + 1], coarse[slot + 1 : slot + 2])
            if k == 1:
                for y in range(rows[k]):
                    value = jnp.concatenate([conv[k][i, y, b] for b in range(blocks)], 1)
                    done[k][i, y] = (value * scale + offset).astype(BF16)
            else:
                done[k][i] = (conv[k][i] * scale + offset).astype(BF16)
    on_ends(lambda way: [halo_copy(k, way).wait_send() for k in range(4)])
    for j in hops:
        here = hop.at[pieces[j]]
        carry(lambda way, h=here, j=j: pltpu.make_async_copy(h, h, hop_send.at[j]).wait())
    all_of(box_rest, rest_send)

    all_of(box_two, two_recv)
    two = gathered(box_two)
    for i in range(images):
        scale, offset = scales(0, two[2 * i : 2 * i + 1], two[2 * i + 1 : 2 * i + 2])
        affine[2 * i : 2 * i + 1, :] = scale
        affine[2 * i + 1 : 2 * i + 2, :] = offset
    all_of(box_two, two_send)


def finish_kernel(geom, *refs):
    images, rows = geom["images"], geom["rows"]
    conv_two, affine = refs[0:2]
    done = [None, *refs[2:5]]
    out_hbm, staged, rest_sem, two_sem = refs[5:9], refs[9], refs[10], refs[11]
    copies = []
    for k in (1, 2, 3):
        copies.append(pltpu.make_async_copy(done[k], out_hbm[k], rest_sem.at[k]))
        copies[-1].start()
    for i in range(images):
        scale = affine[2 * i : 2 * i + 1, :]
        offset = affine[2 * i + 1 : 2 * i + 2, :]
        for y in range(rows[0]):
            value = jnp.concatenate(
                [conv_two[i, y, b] for b in range(conv_two.shape[2])], 1
            )
            staged[i, y] = (value * scale + offset).astype(BF16)
            pltpu.make_async_copy(
                staged.at[i, y], out_hbm[0].at[i, y], two_sem.at[0]
            ).start()
    for copy in copies:
        copy.wait()
    pltpu.make_async_copy(staged, out_hbm[0], two_sem.at[0]).wait()


def per_device(n, *args):
    feats, lat_ws = args[0:4], args[4:8]
    bias, smooth, gain, shift = args[8:12]
    smooth = smooth.reshape(smooth.shape[0], -1, smooth.shape[3])
    images, chans = feats[0].shape[0], lat_ws[0].shape[1]
    rows = [f.shape[1] for f in feats]
    cols = [f.shape[2] for f in feats]
    geom = {"images": images, "chans": chans, "rows": rows, "cols": cols}
    any_spec = pl.BlockSpec(memory_space=pltpu.HBM)
    vmem_spec = pl.BlockSpec(memory_space=pltpu.VMEM)
    outs = [jax.ShapeDtypeStruct((images, r, c, chans), BF16) for r, c in zip(rows, cols)]
    dma = pltpu.SemaphoreType.DMA
    blocks = chans // LANES
    two_rows = -(-(images * 2) // 8) * 8
    strip = lambda k, count, width, kind: pltpu.VMEM((count, images, cols[k], width), kind)
    scratch = (
        [pltpu.VMEM(f.shape, BF16) for f in feats]
        + [pltpu.VMEM(w.shape, BF16) for w in lat_ws]
        + [pltpu.VMEM((3, *bias.shape), F32), pltpu.VMEM(smooth.shape, BF16)]
        + [pltpu.VMEM((2, 2, 3 * chans, chans), BF16)]
        + [pltpu.VMEM((rows[k] + 2, 4, images, cols[k] // 2, chans), BF16) for k in range(2)]
        + [strip(k, rows[k] + 2, 3 * chans, BF16) for k in (2, 3)]
        + [strip(k, min(rows[k], 2), chans, BF16) for k in range(1, 4)]
        + [strip(k, 2, chans, BF16) for k in range(4)]
        + [pltpu.VMEM((rows[0] + 2, images, blocks, cols[0], LANES), F32)]
        + [pltpu.VMEM((rows[1], images, blocks, cols[1], LANES), F32)]
        + [strip(2, rows[2], chans, F32)]
        + [pltpu.VMEM((images, rows[1], blocks, cols[1], LANES), F32)]
        + [pltpu.VMEM(o.shape, F32) for o in outs[2:]]
        + [pltpu.VMEM((2 * c, c), BF16) for c in cols[:3]]
        + [strip(k, 2, chans, BF16) for k in range(1, 4)]
        + [strip(k, 2, chans, F32) for k in range(2)]
        + [strip(1, rows[1], chans, BF16)]
        + [pltpu.VMEM((images, cols[0], chans), BF16)]
        + [
            pltpu.VMEM((n, -(-levels * images * 2 // (chans // GROUPS)), 1, chans), F32)
            for levels in (1, 3)
        ]
        + [dma((4,)), dma((4,)), dma((2,)), dma((1,))]
        + [dma((4, 2)), dma((4, 2)), dma((2,)), dma((2,))]
        + [dma((1,)) for _ in range(4)]
    )
    held = pl.pallas_call(
        functools.partial(kernel, n, geom),
        out_shape=[pltpu.VMEM((images, rows[0], blocks, cols[0], LANES), F32)]
        + [pltpu.VMEM(o.shape, BF16) for o in outs[1:]]
        + [pltpu.VMEM((two_rows, chans), F32)],
        in_specs=[any_spec] * 12,
        out_specs=[vmem_spec] * 5,
        scratch_shapes=scratch,
        compiler_params=pltpu.CompilerParams(
            collective_id=0, has_side_effects=True, vmem_limit_bytes=KERNEL_BYTES
        ),
    )(*args[:8], bias, gain, shift, smooth)
    held = [pltpu.with_memory_space_constraint(h, pltpu.VMEM) for h in held]
    return pl.pallas_call(
        functools.partial(finish_kernel, geom),
        out_shape=outs,
        in_specs=[vmem_spec] * 5,
        out_specs=[any_spec] * 4,
        scratch_shapes=[pltpu.VMEM(outs[0].shape, BF16), dma((4,)), dma((1,))],
        compiler_params=pltpu.CompilerParams(vmem_limit_bytes=16 * 1024 * 1024),
    )(held[0], held[4], *held[1:4])


def solution(mesh):
    strips = P("batch", "rows", None, None)
    run = functools.partial(per_device, mesh.shape["rows"])
    return jax.shard_map(
        lambda *args: tuple(run(*args)),
        mesh=mesh,
        in_specs=(strips,) * 4 + (P(),) * 8,
        out_specs=(strips,) * 4,
        check_vma=False,
    )
```

```python
import functools
import math

import jax
import jax.numpy as jnp
from jax import lax
from jax.experimental import pallas as pl
from jax.experimental.pallas import tpu as pltpu
from jax.sharding import PartitionSpec as P

GROUPS = 32
EPSILON = 1e-05
F32 = jnp.float32
BF16 = jnp.bfloat16
MESH = pl.DeviceIdType.MESH
KERNEL_BYTES = 52 * 1024 * 1024
LANES = 128


def halves_first(index, width, split):
    if not split:
        return index
    return 2 * (index % (width // 2)) + index // (width // 2)


def bilinear(cols, fine_split, coarse_split):
    half = cols // 2
    fine = halves_first(lax.broadcasted_iota(jnp.int32, (cols, cols), 0), cols, fine_split)
    place = lax.broadcasted_iota(jnp.int32, (cols, cols), 1)
    second = place >= half
    coarse = halves_first(jnp.where(second, place - half, place), half, coarse_split)
    near = fine // 2
    odd = fine % 2 == 1
    far = jnp.where(odd, jnp.minimum(near + 1, half - 1), jnp.maximum(near - 1, 0))
    value = jnp.where(coarse == near, 0.75, 0.0) + jnp.where(coarse == far, 0.25, 0.0)
    odd_rows = value * jnp.where(second, 0.25, 0.75)
    even_rows = value * jnp.where(second, 0.75, 0.25)
    return odd_rows.astype(BF16), even_rows.astype(BF16)


def mm(a, b):
    return jnp.dot(a, b, preferred_element_type=F32)


def group_totals(value, size):
    parts = []
    for start in range(0, value.shape[1], LANES):
        part = value[:, start : start + LANES]
        spot = lax.broadcasted_iota(jnp.int32, part.shape, 1) % size
        terms = [part]
        for step in range(1, size):
            terms.append(
                jnp.where(
                    spot >= step,
                    pltpu.roll(part, step, 1),
                    pltpu.roll(part, LANES + step - size, 1),
                )
            )
        while len(terms) > 1:
            terms = [sum(terms[j : j + 2]) for j in range(0, len(terms), 2)]
        parts.append(terms[0])
    return jnp.concatenate(parts, 1)


def own_slots(shape, size):
    row = lax.broadcasted_iota(jnp.int32, shape, 0)
    return lax.broadcasted_iota(jnp.int32, shape, 1) % size == row


def packed(stats, size):
    value = jnp.concatenate(stats, 0)
    value = jnp.where(own_slots(value.shape, size), group_totals(value, size), 0.0)
    return jnp.sum(value, 0, keepdims=True)


def unpacked(row, size):
    value = jnp.broadcast_to(row, (size, row.shape[1]))
    return group_totals(jnp.where(own_slots(value.shape, size), value, 0.0), size)


def kernel(n, geom, *refs):
    images, chans = geom["images"], geom["chans"]
    rows, cols = geom["rows"], geom["cols"]
    it = iter(refs)
    take = lambda count: [next(it) for _ in range(count)]
    feat_hbm, lat_hbm = take(4), take(4)
    consts_hbm, smooth_hbm = take(3), take(1)[0]
    (conv_two,) = take(1)
    conv = [conv_two] + take(3)
    (affine,) = take(1)
    feat, lat_w = take(4), take(4)
    consts, smooth, mixed = take(3)
    vee, big = take(2), [None, None] + take(2)
    sends, recvs, lats = [None] + take(3), take(4), take(3)
    ups, edge, hang = take(3), [None] + take(3), take(2)
    mid, hop = take(2)
    (box,) = take(1)
    in_sem, w_sem, s_sem, p_sem = take(4)
    halo_send, halo_recv, hop_send, hop_recv = take(4)
    sum_send, sum_recv = take(2)
    bias, gain, shift = (consts.at[j] for j in range(3))

    me = lax.axis_index("rows")
    first, last = me == 0, me == n - 1
    size, blocks = chans // GROUPS, chans // LANES
    half = [c // 2 for c in cols]
    top = [r + 1 for r in rows]

    feat_copy = [pltpu.make_async_copy(feat_hbm[k], feat[k], in_sem.at[k]) for k in range(4)]
    lat_copy = [pltpu.make_async_copy(lat_hbm[k], lat_w[k], w_sem.at[k]) for k in range(4)]
    smooth_copy = [
        pltpu.make_async_copy(
            smooth_hbm.at[2 * j : 2 * j + 2], smooth.at[2 * j : 2 * j + 2], s_sem.at[j]
        )
        for j in range(2)
    ]
    feat_copy[3].start()
    lat_copy[3].start()
    for j in range(3):
        pltpu.make_async_copy(consts_hbm[j], consts.at[j], p_sem.at[0]).start()
    barrier = pltpu.get_barrier_semaphore()
    for d in range(1, n):
        pl.semaphore_signal(
            barrier, inc=1, device_id={"rows": lax.rem(me + d, n)}, device_id_type=MESH
        )
    for k in (2, 1, 0):
        lat_copy[k].start()
        feat_copy[k].start()
    for copy in smooth_copy:
        copy.start()

    @pl.when(first)
    def _():
        recvs[0][0] = jnp.zeros_like(recvs[0][0])

    @pl.when(last)
    def _():
        recvs[0][1] = jnp.zeros_like(recvs[0][1])

    for k in range(3):
        odd, even = bilinear(cols[k], k < 2, k == 0)
        ups[k][0 : cols[k]] = odd
        ups[k][cols[k] :] = even

    def remote(src, dst, send_sem, recv_sem, shift_by):
        return pltpu.make_async_remote_copy(
            src_ref=src,
            dst_ref=dst,
            send_sem=send_sem,
            recv_sem=recv_sem,
            device_id={"rows": lax.rem(me + (n + shift_by), n)},
            device_id_type=MESH,
        )

    def halo_source(k, way):
        if k == 0:
            return feat[0].at[:, way * (rows[0] - 1)]
        return sends[k].at[way * (sends[k].shape[0] - 1)]

    def halo_copy(k, way):
        return remote(
            halo_source(k, way),
            recvs[k].at[1 - way],
            halo_send.at[k, way],
            halo_recv.at[k, 1 - way],
            1 if way else -1,
        )

    def on_ends(act):
        @pl.when(jnp.logical_not(first))
        def _():
            act(0)

        @pl.when(jnp.logical_not(last))
        def _():
            act(1)

    def halo_start(k):
        on_ends(lambda way: halo_copy(k, way).start())

    def halo_wait(k):
        on_ends(lambda way: halo_copy(k, 1 - way).wait_recv())

    span = 2 * max(1, math.isqrt(n // 2))
    early = images // 2
    later = slice(early, images)
    pieces = (
        (slice(0, early), slice(0, cols[0])),
        (later, slice(0, half[0])),
        (later, slice(half[0], cols[0])),
    )
    place = lax.rem(me, span)
    crosses = (
        jnp.logical_and(place == 0, jnp.logical_not(first)),
        jnp.logical_and(place == span - 1, jnp.logical_not(last)),
    )
    carries = (
        jnp.logical_and(place == 0, me + span < n),
        jnp.logical_and(place == span - 1, me >= span),
    )
    relays = span < n
    hops = range(2) if early else range(1, 2)

    def fine_start():
        def begin(way):
            if not relays:
                halo_copy(0, way).start()
                return

            @pl.when(jnp.logical_not(crosses[way]))
            def _():
                halo_copy(0, way).start()

            @pl.when(crosses[way])
            def _():
                for j in (*hops, 2):
                    some, width = pieces[j]
                    last_hop = j == 2
                    remote(
                        feat[0].at[some, way * (rows[0] - 1), width],
                        recvs[0].at[1 - way, some, width] if last_hop else hop.at[some, width],
                        halo_send.at[0, way],
                        halo_recv.at[0, 1 - way] if last_hop else hop_recv.at[j],
                        (1 if last_hop else span) * (1 if way else -1),
                    ).start()

        on_ends(begin)

    def carry(act, ways=(0, 1)):
        if relays:
            for way in ways:
                pl.when(carries[way])(functools.partial(act, way))

    def carry_start(j, *ways):
        def act(way):
            some, width = pieces[j]
            here = hop.at[some, width]
            pltpu.make_async_copy(here, here, hop_recv.at[j]).wait()
            remote(
                here,
                recvs[0].at[1 - way, some, width],
                hop_send.at[j],
                halo_recv.at[0, 1 - way],
                1 - span if way else span - 1,
            ).start()

        if j in hops:
            carry(act, ways)

    pltpu.make_async_copy(consts, consts, p_sem.at[0]).wait()
    feat_copy[3].wait()
    lat_copy[3].wait()
    flat = feat[3][...].reshape(-1, feat[3].shape[-1])
    five = [
        mm(flat, lat_w[3][:, b * LANES : (b + 1) * LANES]) for b in range(blocks)
    ]
    five = bias[3:4, :] + jnp.concatenate(five, 1)
    five = five.reshape(images, rows[3], cols[3], chans)
    for y in range(rows[3]):
        for i in range(images):
            sends[3][y, i] = five[i, y].astype(BF16)
    pl.semaphore_wait(barrier, n - 1)
    halo_start(3)

    lat_copy[2].wait()
    feat_copy[2].wait()
    for i in range(images):
        flat = feat[2][i].reshape(rows[2] * cols[2], -1)
        value = (bias[2:3, :] + mm(flat, lat_w[2][...])).reshape(rows[2], cols[2], chans)
        for y in range(rows[2]):
            lats[2][y, i] = value[y]
        sends[2][0, i] = value[0].astype(BF16)
        sends[2][1, i] = value[rows[2] - 1].astype(BF16)
    halo_start(2)

    def columns(k, r, i):
        return [
            jnp.concatenate(
                [lats[k][r, i, b, pl.ds(odd, half[k], stride=2), :] for b in range(blocks)], 1
            )
            for odd in range(2)
        ]

    def keep(k, r, i, value):
        for b in range(blocks):
            lats[k][r, i, b] = value[:, b * LANES : (b + 1) * LANES]

    lat_copy[1].wait()
    feat_copy[1].wait()

    def lateral_three(some):
        for i in range(images):
            flat = jnp.concatenate([feat[1][i, y] for y in some], 0)
            value = (bias[1:2, :] + mm(flat, lat_w[1][...])).reshape(len(some), cols[1], chans)
            for j, y in enumerate(some):
                keep(1, y, i, value[j])
        for y in some:
            if y in (0, rows[1] - 1):
                for i in range(images):
                    even, odd = columns(1, y, i)
                    sends[1][0 if y == 0 else 1, i, : half[1]] = even.astype(BF16)
                    sends[1][0 if y == 0 else 1, i, half[1] :] = odd.astype(BF16)

    lateral_three([0, rows[1] - 1])
    halo_start(1)
    lateral_three(list(range(1, rows[1] - 1)))

    def lateral_two(y):
        for i in range(images):
            flat = feat[0][i, y : y + 2].reshape(2 * cols[0], -1)
            value = bias[0:1, :] + mm(flat, lat_w[0][...])
            keep(0, y + 1, i, value[: cols[0]])
            keep(0, y + 2, i, value[cols[0] :])

    lat_copy[0].wait()
    feat_copy[0].wait()
    fine_start()
    steps = list(range(0, rows[0], 2))
    for y in steps[: len(steps) // 2]:
        lateral_two(y)

    def tap(k, a, b, start=0, count=chans):
        return smooth[k, pl.ds((3 * a + b) * chans + start, count)]

    smooth_copy[0].wait()
    piece = 16

    def mix(k, a, start):
        taps = [tap(k, a, b, start, piece).astype(F32) for b in range(3)]
        outer_taps, inner_tap = (taps[0] + taps[2]) * 0.5, taps[1] * 0.5
        mixed[k, 0, pl.ds(a * chans + start, piece)] = (outer_taps + inner_tap).astype(BF16)
        mixed[k, 1, pl.ds(a * chans + start, piece)] = (outer_taps - inner_tap).astype(BF16)

    for k in range(2):
        for a in range(3):
            for start in range(0, chans, piece):
                mix(k, a, start)
    for y in steps[len(steps) // 2 :]:
        lateral_two(y)
    smooth_copy[1].wait()

    def moved(value, by):
        length = value.shape[0]
        spot = lax.broadcasted_iota(jnp.int32, (8, value.shape[1]), 0)
        if by > 0:
            value = pltpu.roll(value, 1, 0)
            return jnp.concatenate([jnp.where(spot == 0, 0.0, value[:8]), value[8:]], 0)
        value = pltpu.roll(value, length - 1, 0)
        cut = length - 8
        return jnp.concatenate([value[:cut], jnp.where(spot == 7, 0.0, value[cut:])], 0)

    def put(k, r, i, value):
        big[k][r, i, :, 0:chans] = moved(value, 1).astype(BF16)
        big[k][r, i, :, chans : 2 * chans] = value.astype(BF16)
        big[k][r, i, :, 2 * chans :] = moved(value, -1).astype(BF16)

    def put_pairs(k, r, i, even, odd):
        vee[k][r, 0, i] = (moved(odd, 1) - odd).astype(BF16)
        vee[k][r, 1, i] = (even + odd).astype(BF16)
        vee[k][r, 2, i] = (odd - even).astype(BF16)
        vee[k][r, 3, i] = (even - moved(even, -1)).astype(BF16)

    def center(k, r, i):
        return big[k][r, i, :, chans : 2 * chans]

    def borders(k, i, above, below):
        edge[k][0, i] = jnp.where(first, center(k, 1, i), above.astype(BF16))
        edge[k][1, i] = jnp.where(last, center(k, rows[k], i), below.astype(BF16))
        put(k, 0, i, jnp.where(first, 0.0, above))
        put(k, top[k], i, jnp.where(last, 0.0, below))

    def pair(k, p, i):
        own = (lambda y: mid[y, i]) if k == 1 else (lambda y: center(k, y + 1, i))
        upper = edge[k][0, i] if p == 0 else own(p - 1)
        lower = edge[k][1, i] if p == rows[k] else own(p)
        return jnp.concatenate([upper, lower], 0)

    def folded(value):
        part = value.reshape(-1, 8, chans)
        return jnp.sum(part, 0), jnp.sum(part * part, 0)

    def conv_rows(k, apart):
        groups = [[i] for i in range(images)] if apart else [list(range(images))]
        sums = []
        for group in groups:
            bands = [
                jnp.concatenate([big[k][y + a, i] for i in group for y in range(rows[k])], 0)
                for a in range(3)
            ]
            total = mm(jnp.concatenate(bands, 1), smooth[k])
            total = total.reshape(len(group), rows[k], cols[k], chans)
            for j, i in enumerate(group):
                conv[k][i] = total[j]
                sums.append(folded(total[j]))
        return sums

    def conv_pairs(k, some, taps=(0, 1, 2), add=False, keep_sums=True):
        at = [slice(a * chans, (a + 1) * chans) for a in taps]
        weights = [
            jnp.concatenate([tap(k, a, 0) for a in taps], 0),
            jnp.concatenate([mixed[k, 0, here] for here in at], 0),
            jnp.concatenate([mixed[k, 1, here] for here in at], 0),
            jnp.concatenate([tap(k, a, 2) for a in taps], 0),
        ]
        parts = []
        for t in range(4):
            bands = [
                jnp.concatenate([vee[k][y + a, t, i] for y in some for i in range(images)], 0)
                for a in taps
            ]
            parts.append(mm(jnp.concatenate(bands, 1), weights[t]))
        even = (parts[1] + parts[2]) + parts[0]
        odd = (parts[1] - parts[2]) - parts[3]
        sums = [None] * images
        for j, (y, i) in enumerate((y, i) for y in some for i in range(images)):
            here = slice(j * half[k], (j + 1) * half[k])
            values = []
            for odd_ones, value in ((0, even[here]), (1, odd[here])):
                spots = [
                    conv[k].at[i, y, b, pl.ds(odd_ones, half[k], stride=2), :]
                    for b in range(blocks)
                ]
                if add:
                    value = value + jnp.concatenate([spot[...] for spot in spots], 1)
                for b, spot in enumerate(spots):
                    spot[...] = value[:, b * LANES : (b + 1) * LANES]
                values.append(value)
            if keep_sums:
                new = joined([[folded(value)] for value in values])[0]
                sums[i] = new if sums[i] is None else joined([[sums[i]], [new]])[0]
        return sums

    def joined(parts):
        total = parts[0]
        for part in parts[1:]:
            total = [(t[0] + u[0], t[1] + u[1]) for t, u in zip(total, part)]
        return total

    def stat_rows(sums):
        return [jnp.sum(part, 0, keepdims=True) for pair in sums for part in pair]

    def post(box, rows_of, send_sem, recv_sem):
        for j in range(box.shape[1]):
            some = rows_of[j * size : (j + 1) * size]
            some = some + [jnp.zeros_like(some[0])] * (size - len(some))
            box[0, j] = packed(some, size)
        for d in range(1, n):
            remote(box.at[0], box.at[d], send_sem.at[0], recv_sem.at[0], d).start()

    def all_of(box, sem):
        pltpu.make_async_copy(box.at[1:n], box.at[1:n], sem.at[0]).wait()

    def gathered(box):
        stats = []
        for j in range(box.shape[1]):
            total = box[0, j]
            for d in range(1, n):
                total = total + box[d, j]
            stats.append(unpacked(total, size))
        return jnp.concatenate(stats, 0)

    for i in range(images):
        for y in range(rows[3]):
            put(3, y + 1, i, five[i, y])
    halo_wait(3)
    for i in range(images):
        borders(3, i, recvs[3][0, i].astype(F32), recvs[3][1, i].astype(F32))

    outer = {}
    for p in range(rows[3] + 1):
        for i in range(images):
            both = mm(ups[2][...], pair(3, p, i))
            for y, value in ((2 * p - 1, both[: cols[2]]), (2 * p, both[cols[2] :])):
                if 0 <= y < rows[2]:
                    put(2, y + 1, i, lats[2][y, i] + value)
                else:
                    outer[y, i] = value
    def merge(k, p):
        for i in range(images):
            coarse = pair(k + 1, p, i)
            for y in (2 * p - 1, 2 * p):
                value = mm(ups[k][: cols[k]] if y < 2 * p else ups[k][cols[k] :], coarse)
                if not 0 <= y < rows[k]:
                    if k == 0:
                        value = jnp.where(first if y < 0 else last, 0.0, value + bias[0:1, :])
                    hang[k][0 if y < 0 else 1, i] = value
                    continue
                even, odd = columns(k, y + 1 if k == 0 else y, i)
                even = even + value[: half[k]]
                odd = odd + value[half[k] :]
                if k:
                    mid[y, i, : half[k]] = even.astype(BF16)
                    mid[y, i, half[k] :] = odd.astype(BF16)
                put_pairs(k, y + 1, i, even, odd)

    sums_five = conv_rows(3, False)
    for p in range(1, rows[2]):
        merge(1, p)
    for p in range(2, rows[1] - 1):
        merge(0, p)

    carry_start(0, 1)
    halo_wait(2)
    for i in range(images):
        borders(
            2,
            i,
            recvs[2][0, i].astype(F32) + outer[-1, i],
            recvs[2][1, i].astype(F32) + outer[rows[2], i],
        )

    merge(1, 0)
    merge(1, rows[2])
    sums_four = conv_rows(2, True)
    merge(0, 1)
    sums_three = [conv_pairs(1, list(range(1, rows[1] - 1)))]
    sums_two = []

    def conv_two_row(y):
        sums_two.append(conv_pairs(0, [y]))

    inner = list(range(2, rows[0] - 2))
    ahead = len(inner) * 3 // 4
    for y in inner[:ahead]:
        if y == inner[min(2, ahead - 1)]:
            merge(0, rows[1] - 1)
        conv_two_row(y)

    carry_start(0, 0)
    carry_start(1, 0, 1)
    halo_wait(1)
    for way in range(2):
        for i in range(images):
            value = recvs[1][way, i].astype(F32) + hang[1][way, i]
            none = last if way else first
            own = mid[way * (rows[1] - 1), i]
            edge[1][way, i] = jnp.where(none, own, value.astype(BF16))
            value = jnp.where(none, 0.0, value)
            put_pairs(1, way * top[1], i, value[: half[1]], value[half[1] :])
    merge(0, 0)
    merge(0, rows[1])
    sums_three.append(conv_pairs(1, [0, rows[1] - 1]))
    for y in inner[ahead:]:
        conv_two_row(y)
    conv_two_row(1)
    conv_two_row(rows[0] - 2)
    conv_pairs(0, [0], (1, 2), keep_sums=False)
    conv_pairs(0, [rows[0] - 1], (0, 1), keep_sums=False)
    coarse_rows = stat_rows(joined(sums_three)) + stat_rows(sums_four) + stat_rows(sums_five)

    halo_wait(0)
    for way in range(2):
        for i in range(images):
            keep(0, way * top[0], i, mm(recvs[0][way, i], lat_w[0][...]))
    for way in range(2):
        for i in range(images):
            even, odd = columns(0, way * top[0], i)
            even = even + hang[0][way, i, : half[0]]
            odd = odd + hang[0][way, i, half[0] :]
            put_pairs(0, way * top[0], i, even, odd)
    sums_two.append(conv_pairs(0, [0], (0,), add=True))
    sums_two.append(conv_pairs(0, [rows[0] - 1], (2,), add=True))
    post(box, stat_rows(joined(sums_two)) + coarse_rows, sum_send, sum_recv)

    def scales(k, total, square):
        share = 1.0 / float(rows[k] * n * cols[k] * size)
        mean = total * share
        variance = square * share - mean * mean
        scale = lax.rsqrt(variance + EPSILON) * gain[k : k + 1, :]
        return scale, shift[k : k + 1, :] - mean * scale

    on_ends(lambda way: [halo_copy(k, way).wait_send() for k in range(4)])
    for j in hops:
        here = hop.at[pieces[j]]
        carry(lambda way, h=here, j=j: pltpu.make_async_copy(h, h, hop_send.at[j]).wait())
    all_of(box, sum_recv)
    stats = gathered(box)
    for k in range(4):
        for i in range(images):
            slot = (k * images + i) * 2
            scale, offset = scales(k, stats[slot : slot + 1], stats[slot + 1 : slot + 2])
            affine[slot : slot + 1, :] = scale
            affine[slot + 1 : slot + 2, :] = offset
    all_of(box, sum_send)


def finish_kernel(geom, *refs):
    images, rows = geom["images"], geom["rows"]
    conv, affine = refs[0:4], refs[4]
    out_hbm, staged, out_sem = refs[5:9], refs[9:13], refs[13]

    def finish(k, i, y):
        if k < 2:
            value = jnp.concatenate([conv[k][i, y, b] for b in range(conv[k].shape[2])], 1)
        else:
            value = conv[k][i, y]
        slot = (k * images + i) * 2
        value = value * affine[slot : slot + 1, :] + affine[slot + 1 : slot + 2, :]
        staged[k][i, y] = value.astype(BF16)

    for i in range(images):
        for y in range(rows[0]):
            finish(0, i, y)
            pltpu.make_async_copy(staged[0].at[i, y], out_hbm[0].at[i, y], out_sem.at[0]).start()
    for k in (1, 2, 3):
        for i in range(images):
            for y in range(rows[k]):
                finish(k, i, y)
        pltpu.make_async_copy(staged[k], out_hbm[k], out_sem.at[k]).start()
    for k in range(4):
        pltpu.make_async_copy(staged[k], out_hbm[k], out_sem.at[k]).wait()


def per_device(n, *args):
    feats, lat_ws = args[0:4], args[4:8]
    bias, smooth, gain, shift = args[8:12]
    smooth = smooth.reshape(smooth.shape[0], -1, smooth.shape[3])
    images, chans = feats[0].shape[0], lat_ws[0].shape[1]
    rows = [f.shape[1] for f in feats]
    cols = [f.shape[2] for f in feats]
    geom = {"images": images, "chans": chans, "rows": rows, "cols": cols}
    any_spec = pl.BlockSpec(memory_space=pltpu.HBM)
    vmem_spec = pl.BlockSpec(memory_space=pltpu.VMEM)
    outs = [jax.ShapeDtypeStruct((images, r, c, chans), BF16) for r, c in zip(rows, cols)]
    dma = pltpu.SemaphoreType.DMA
    blocks = chans // LANES
    stat_rows = -(-(4 * images * 2) // 8) * 8
    strip = lambda k, count, width, kind: pltpu.VMEM((count, images, cols[k], width), kind)
    scratch = (
        [pltpu.VMEM(f.shape, BF16) for f in feats]
        + [pltpu.VMEM(w.shape, BF16) for w in lat_ws]
        + [pltpu.VMEM((3, *bias.shape), F32), pltpu.VMEM(smooth.shape, BF16)]
        + [pltpu.VMEM((2, 2, 3 * chans, chans), BF16)]
        + [pltpu.VMEM((rows[k] + 2, 4, images, cols[k] // 2, chans), BF16) for k in range(2)]
        + [strip(k, rows[k] + 2, 3 * chans, BF16) for k in (2, 3)]
        + [strip(k, min(rows[k], 2), chans, BF16) for k in range(1, 4)]
        + [strip(k, 2, chans, BF16) for k in range(4)]
        + [pltpu.VMEM((rows[0] + 2, images, blocks, cols[0], LANES), F32)]
        + [pltpu.VMEM((rows[1], images, blocks, cols[1], LANES), F32)]
        + [strip(2, rows[2], chans, F32)]
        + [pltpu.VMEM((2 * c, c), BF16) for c in cols[:3]]
        + [strip(k, 2, chans, BF16) for k in range(1, 4)]
        + [strip(k, 2, chans, F32) for k in range(2)]
        + [strip(1, rows[1], chans, BF16)]
        + [pltpu.VMEM((images, cols[0], chans), BF16)]
        + [
            pltpu.VMEM((n, -(-4 * images * 2 // (chans // GROUPS)), 1, chans), F32)
        ]
        + [dma((4,)), dma((4,)), dma((2,)), dma((1,))]
        + [dma((4, 2)), dma((4, 2)), dma((2,)), dma((2,))]
        + [dma((1,)) for _ in range(2)]
    )
    held = pl.pallas_call(
        functools.partial(kernel, n, geom),
        out_shape=[
            pltpu.VMEM((images, rows[k], blocks, cols[k], LANES), F32) for k in range(2)
        ]
        + [pltpu.VMEM(o.shape, F32) for o in outs[2:]]
        + [pltpu.VMEM((stat_rows, chans), F32)],
        in_specs=[any_spec] * 12,
        out_specs=[vmem_spec] * 5,
        scratch_shapes=scratch,
        compiler_params=pltpu.CompilerParams(
            collective_id=0, has_side_effects=True, vmem_limit_bytes=KERNEL_BYTES
        ),
    )(*args[:8], bias, gain, shift, smooth)
    held = [pltpu.with_memory_space_constraint(h, pltpu.VMEM) for h in held]
    return pl.pallas_call(
        functools.partial(finish_kernel, geom),
        out_shape=outs,
        in_specs=[vmem_spec] * 5,
        out_specs=[any_spec] * 4,
        scratch_shapes=[pltpu.VMEM(o.shape, BF16) for o in outs] + [dma((4,))],
        compiler_params=pltpu.CompilerParams(vmem_limit_bytes=16 * 1024 * 1024),
    )(*held)


def solution(mesh):
    strips = P("batch", "rows", None, None)
    run = functools.partial(per_device, mesh.shape["rows"])
    return jax.shard_map(
        lambda *args: tuple(run(*args)),
        mesh=mesh,
        in_specs=(strips,) * 4 + (P(),) * 8,
        out_specs=(strips,) * 4,
        check_vma=False,
    )
```

```python
import functools
import math

import jax
import jax.numpy as jnp
from jax import lax
from jax.experimental import pallas as pl
from jax.experimental.pallas import tpu as pltpu
from jax.sharding import PartitionSpec as P

GROUPS = 32
EPSILON = 1e-05
F32 = jnp.float32
BF16 = jnp.bfloat16
MESH = pl.DeviceIdType.MESH
KERNEL_BYTES = 52 * 1024 * 1024
LANES = 128


def halves_first(index, width, split):
    if not split:
        return index
    return 2 * (index % (width // 2)) + index // (width // 2)


def bilinear(cols, fine_split, coarse_split):
    half = cols // 2
    fine = halves_first(lax.broadcasted_iota(jnp.int32, (cols, cols), 0), cols, fine_split)
    place = lax.broadcasted_iota(jnp.int32, (cols, cols), 1)
    second = place >= half
    coarse = halves_first(jnp.where(second, place - half, place), half, coarse_split)
    near = fine // 2
    odd = fine % 2 == 1
    far = jnp.where(odd, jnp.minimum(near + 1, half - 1), jnp.maximum(near - 1, 0))
    value = jnp.where(coarse == near, 0.75, 0.0) + jnp.where(coarse == far, 0.25, 0.0)
    odd_rows = value * jnp.where(second, 0.25, 0.75)
    even_rows = value * jnp.where(second, 0.75, 0.25)
    return odd_rows.astype(BF16), even_rows.astype(BF16)


def mm(a, b):
    return jnp.dot(a, b, preferred_element_type=F32)


def group_totals(value, size):
    parts = []
    for start in range(0, value.shape[1], LANES):
        part = value[:, start : start + LANES]
        spot = lax.broadcasted_iota(jnp.int32, part.shape, 1) % size
        terms = [part]
        for step in range(1, size):
            terms.append(
                jnp.where(
                    spot >= step,
                    pltpu.roll(part, step, 1),
                    pltpu.roll(part, LANES + step - size, 1),
                )
            )
        while len(terms) > 1:
            terms = [sum(terms[j : j + 2]) for j in range(0, len(terms), 2)]
        parts.append(terms[0])
    return jnp.concatenate(parts, 1)


def own_slots(shape, size):
    row = lax.broadcasted_iota(jnp.int32, shape, 0)
    return lax.broadcasted_iota(jnp.int32, shape, 1) % size == row


def packed(stats, size):
    value = jnp.concatenate(stats, 0)
    value = jnp.where(own_slots(value.shape, size), group_totals(value, size), 0.0)
    return jnp.sum(value, 0, keepdims=True)


def unpacked(row, size):
    value = jnp.broadcast_to(row, (size, row.shape[1]))
    return group_totals(jnp.where(own_slots(value.shape, size), value, 0.0), size)


def kernel(n, geom, *refs):
    images, chans = geom["images"], geom["chans"]
    rows, cols = geom["rows"], geom["cols"]
    it = iter(refs)
    take = lambda count: [next(it) for _ in range(count)]
    feat_hbm, lat_hbm = take(4), take(4)
    consts_hbm, smooth_hbm = take(3), take(1)[0]
    (conv_two,) = take(1)
    done = [None] + take(3)
    (affine,) = take(1)
    feat, lat_w = take(4), take(4)
    consts, smooth, mixed = take(3)
    vee, big = take(2), [None, None] + take(2)
    sends, recvs, lats = [None] + take(3), take(4), take(3)
    conv = [conv_two] + take(3)
    ups, edge, hang = take(3), [None] + take(3), take(2)
    mid, hop = take(2)
    box_two, box_rest = take(2)
    in_sem, w_sem, s_sem, p_sem = take(4)
    halo_recv, hop_recv = take(2)
    two_send, two_recv, rest_recv = take(3)
    halo_send, hop_send, rest_send = (in_sem, w_sem), s_sem, p_sem
    bias, gain, shift = (consts.at[j] for j in range(3))

    me = lax.axis_index("rows")
    first, last = me == 0, me == n - 1
    size, blocks = chans // GROUPS, chans // LANES
    half = [c // 2 for c in cols]
    top = [r + 1 for r in rows]

    feat_copy = [pltpu.make_async_copy(feat_hbm[k], feat[k], in_sem.at[k]) for k in range(4)]
    lat_copy = [pltpu.make_async_copy(lat_hbm[k], lat_w[k], w_sem.at[k]) for k in range(4)]
    smooth_copy = [
        pltpu.make_async_copy(
            smooth_hbm.at[2 * j : 2 * j + 2], smooth.at[2 * j : 2 * j + 2], s_sem.at[j]
        )
        for j in range(2)
    ]
    feat_copy[3].start()
    lat_copy[3].start()
    for j in range(3):
        pltpu.make_async_copy(consts_hbm[j], consts.at[j], p_sem.at[0]).start()
    barrier = pltpu.get_barrier_semaphore()
    for d in range(1, n):
        pl.semaphore_signal(
            barrier, inc=1, device_id={"rows": lax.rem(me + d, n)}, device_id_type=MESH
        )
    for k in (2, 1, 0):
        lat_copy[k].start()
        feat_copy[k].start()
    for copy in smooth_copy:
        copy.start()

    @pl.when(first)
    def _():
        recvs[0][0] = jnp.zeros_like(recvs[0][0])

    @pl.when(last)
    def _():
        recvs[0][1] = jnp.zeros_like(recvs[0][1])

    for k in range(3):
        odd, even = bilinear(cols[k], k < 2, k == 0)
        ups[k][0 : cols[k]] = odd
        ups[k][cols[k] :] = even

    def remote(src, dst, send_sem, recv_sem, shift_by):
        return pltpu.make_async_remote_copy(
            src_ref=src,
            dst_ref=dst,
            send_sem=send_sem,
            recv_sem=recv_sem,
            device_id={"rows": lax.rem(me + (n + shift_by), n)},
            device_id_type=MESH,
        )

    def halo_source(k, way):
        if k == 0:
            return feat[0].at[:, way * (rows[0] - 1)]
        return sends[k].at[way * (sends[k].shape[0] - 1)]

    def halo_copy(k, way):
        return remote(
            halo_source(k, way),
            recvs[k].at[1 - way],
            halo_send[way].at[k],
            halo_recv.at[k, 1 - way],
            1 if way else -1,
        )

    def on_ends(act):
        @pl.when(jnp.logical_not(first))
        def _():
            act(0)

        @pl.when(jnp.logical_not(last))
        def _():
            act(1)

    def halo_start(k):
        on_ends(lambda way: halo_copy(k, way).start())

    def halo_wait(k):
        on_ends(lambda way: halo_copy(k, 1 - way).wait_recv())

    span = 2 * max(1, math.isqrt(n // 2))
    early = images // 2
    later = slice(early, images)
    pieces = (
        (slice(0, early), slice(0, cols[0])),
        (later, slice(0, half[0])),
        (later, slice(half[0], cols[0])),
    )
    place = lax.rem(me, span)
    crosses = (
        jnp.logical_and(place == 0, jnp.logical_not(first)),
        jnp.logical_and(place == span - 1, jnp.logical_not(last)),
    )
    carries = (
        jnp.logical_and(place == 0, me + span < n),
        jnp.logical_and(place == span - 1, me >= span),
    )
    relays = span < n
    hops = range(2) if early else range(1, 2)

    def fine_start():
        def begin(way):
            if not relays:
                halo_copy(0, way).start()
                return

            @pl.when(jnp.logical_not(crosses[way]))
            def _():
                halo_copy(0, way).start()

            @pl.when(crosses[way])
            def _():
                for j in (*hops, 2):
                    some, width = pieces[j]
                    last_hop = j == 2
                    remote(
                        feat[0].at[some, way * (rows[0] - 1), width],
                        recvs[0].at[1 - way, some, width] if last_hop else hop.at[some, width],
                        halo_send[way].at[0],
                        halo_recv.at[0, 1 - way] if last_hop else hop_recv.at[j],
                        (1 if last_hop else span) * (1 if way else -1),
                    ).start()

        on_ends(begin)

    def carry(act, ways=(0, 1)):
        if relays:
            for way in ways:
                pl.when(carries[way])(functools.partial(act, way))

    def carry_start(j, *ways):
        def act(way):
            some, width = pieces[j]
            here = hop.at[some, width]
            pltpu.make_async_copy(here, here, hop_recv.at[j]).wait()
            remote(
                here,
                recvs[0].at[1 - way, some, width],
                hop_send.at[j],
                halo_recv.at[0, 1 - way],
                1 - span if way else span - 1,
            ).start()

        if j in hops:
            carry(act, ways)

    pltpu.make_async_copy(consts, consts, p_sem.at[0]).wait()
    feat_copy[3].wait()
    lat_copy[3].wait()
    flat = feat[3][...].reshape(-1, feat[3].shape[-1])
    five = [
        mm(flat, lat_w[3][:, b * LANES : (b + 1) * LANES]) for b in range(blocks)
    ]
    five = bias[3:4, :] + jnp.concatenate(five, 1)
    five = five.reshape(images, rows[3], cols[3], chans)
    for y in range(rows[3]):
        for i in range(images):
            sends[3][y, i] = five[i, y].astype(BF16)
    pl.semaphore_wait(barrier, n - 1)
    halo_start(3)

    lat_copy[2].wait()
    feat_copy[2].wait()
    for i in range(images):
        flat = feat[2][i].reshape(rows[2] * cols[2], -1)
        value = (bias[2:3, :] + mm(flat, lat_w[2][...])).reshape(rows[2], cols[2], chans)
        for y in range(rows[2]):
            lats[2][y, i] = value[y]
        sends[2][0, i] = value[0].astype(BF16)
        sends[2][1, i] = value[rows[2] - 1].astype(BF16)
    halo_start(2)

    def columns(k, r, i):
        return [
            jnp.concatenate(
                [lats[k][r, i, b, pl.ds(odd, half[k], stride=2), :] for b in range(blocks)], 1
            )
            for odd in range(2)
        ]

    def keep(k, r, i, value):
        for b in range(blocks):
            lats[k][r, i, b] = value[:, b * LANES : (b + 1) * LANES]

    lat_copy[1].wait()
    feat_copy[1].wait()

    def lateral_three(some):
        for i in range(images):
            flat = jnp.concatenate([feat[1][i, y] for y in some], 0)
            value = (bias[1:2, :] + mm(flat, lat_w[1][...])).reshape(len(some), cols[1], chans)
            for j, y in enumerate(some):
                keep(1, y, i, value[j])
        for y in some:
            if y in (0, rows[1] - 1):
                for i in range(images):
                    even, odd = columns(1, y, i)
                    sends[1][0 if y == 0 else 1, i, : half[1]] = even.astype(BF16)
                    sends[1][0 if y == 0 else 1, i, half[1] :] = odd.astype(BF16)

    lateral_three([0, rows[1] - 1])
    halo_start(1)
    lateral_three(list(range(1, rows[1] - 1)))

    def lateral_two(y):
        for i in range(images):
            flat = feat[0][i, y : y + 2].reshape(2 * cols[0], -1)
            value = bias[0:1, :] + mm(flat, lat_w[0][...])
            keep(0, y + 1, i, value[: cols[0]])
            keep(0, y + 2, i, value[cols[0] :])

    lat_copy[0].wait()
    feat_copy[0].wait()
    fine_start()
    steps = list(range(0, rows[0], 2))
    for y in steps[: len(steps) // 2]:
        lateral_two(y)

    def tap(k, a, b, start=0, count=chans):
        return smooth[k, pl.ds((3 * a + b) * chans + start, count)]

    smooth_copy[0].wait()
    piece = 16

    def mix(k, a, start):
        taps = [tap(k, a, b, start, piece).astype(F32) for b in range(3)]
        outer_taps, inner_tap = (taps[0] + taps[2]) * 0.5, taps[1] * 0.5
        mixed[k, 0, pl.ds(a * chans + start, piece)] = (outer_taps + inner_tap).astype(BF16)
        mixed[k, 1, pl.ds(a * chans + start, piece)] = (outer_taps - inner_tap).astype(BF16)

    for k in range(2):
        for a in range(3):
            for start in range(0, chans, piece):
                mix(k, a, start)
    for y in steps[len(steps) // 2 :]:
        lateral_two(y)
    smooth_copy[1].wait()

    def moved(value, by):
        length = value.shape[0]
        spot = lax.broadcasted_iota(jnp.int32, (8, value.shape[1]), 0)
        if by > 0:
            value = pltpu.roll(value, 1, 0)
            return jnp.concatenate([jnp.where(spot == 0, 0.0, value[:8]), value[8:]], 0)
        value = pltpu.roll(value, length - 1, 0)
        cut = length - 8
        return jnp.concatenate([value[:cut], jnp.where(spot == 7, 0.0, value[cut:])], 0)

    def put(k, r, i, value):
        big[k][r, i, :, 0:chans] = moved(value, 1).astype(BF16)
        big[k][r, i, :, chans : 2 * chans] = value.astype(BF16)
        big[k][r, i, :, 2 * chans :] = moved(value, -1).astype(BF16)

    def put_pairs(k, r, i, even, odd):
        vee[k][r, 0, i] = (moved(odd, 1) - odd).astype(BF16)
        vee[k][r, 1, i] = (even + odd).astype(BF16)
        vee[k][r, 2, i] = (odd - even).astype(BF16)
        vee[k][r, 3, i] = (even - moved(even, -1)).astype(BF16)

    def center(k, r, i):
        return big[k][r, i, :, chans : 2 * chans]

    def borders(k, i, above, below):
        edge[k][0, i] = jnp.where(first, center(k, 1, i), above.astype(BF16))
        edge[k][1, i] = jnp.where(last, center(k, rows[k], i), below.astype(BF16))
        put(k, 0, i, jnp.where(first, 0.0, above))
        put(k, top[k], i, jnp.where(last, 0.0, below))

    def pair(k, p, i):
        own = (lambda y: mid[y, i]) if k == 1 else (lambda y: center(k, y + 1, i))
        upper = edge[k][0, i] if p == 0 else own(p - 1)
        lower = edge[k][1, i] if p == rows[k] else own(p)
        return jnp.concatenate([upper, lower], 0)

    def folded(value):
        part = value.reshape(-1, 8, chans)
        return jnp.sum(part, 0), jnp.sum(part * part, 0)

    def conv_rows(k, apart):
        groups = [[i] for i in range(images)] if apart else [list(range(images))]
        sums = []
        for group in groups:
            bands = [
                jnp.concatenate([big[k][y + a, i] for i in group for y in range(rows[k])], 0)
                for a in range(3)
            ]
            total = mm(jnp.concatenate(bands, 1), smooth[k])
            total = total.reshape(len(group), rows[k], cols[k], chans)
            for j, i in enumerate(group):
                conv[k][i] = total[j]
                sums.append(folded(total[j]))
        return sums

    def conv_pairs(k, some, taps=(0, 1, 2), add=False, keep_sums=True):
        at = [slice(a * chans, (a + 1) * chans) for a in taps]
        weights = [
            jnp.concatenate([tap(k, a, 0) for a in taps], 0),
            jnp.concatenate([mixed[k, 0, here] for here in at], 0),
            jnp.concatenate([mixed[k, 1, here] for here in at], 0),
            jnp.concatenate([tap(k, a, 2) for a in taps], 0),
        ]
        parts = []
        for t in range(4):
            bands = [
                jnp.concatenate([vee[k][y + a, t, i] for y in some for i in range(images)], 0)
                for a in taps
            ]
            parts.append(mm(jnp.concatenate(bands, 1), weights[t]))
        even = (parts[1] + parts[2]) + parts[0]
        odd = (parts[1] - parts[2]) - parts[3]
        sums = [None] * images
        for j, (y, i) in enumerate((y, i) for y in some for i in range(images)):
            here = slice(j * half[k], (j + 1) * half[k])
            values = []
            for odd_ones, value in ((0, even[here]), (1, odd[here])):
                spots = [
                    conv[k].at[i, y, b, pl.ds(odd_ones, half[k], stride=2), :]
                    for b in range(blocks)
                ]
                if add:
                    value = value + jnp.concatenate([spot[...] for spot in spots], 1)
                for b, spot in enumerate(spots):
                    spot[...] = value[:, b * LANES : (b + 1) * LANES]
                values.append(value)
            if keep_sums:
                new = joined([[folded(value)] for value in values])[0]
                sums[i] = new if sums[i] is None else joined([[sums[i]], [new]])[0]
        return sums

    def joined(parts):
        total = parts[0]
        for part in parts[1:]:
            total = [(t[0] + u[0], t[1] + u[1]) for t, u in zip(total, part)]
        return total

    def stat_rows(sums):
        return [jnp.sum(part, 0, keepdims=True) for pair in sums for part in pair]

    def post(box, rows_of, send_sem, recv_sem):
        for j in range(box.shape[1]):
            some = rows_of[j * size : (j + 1) * size]
            some = some + [jnp.zeros_like(some[0])] * (size - len(some))
            box[0, j] = packed(some, size)
        for d in range(1, n):
            remote(box.at[0], box.at[d], send_sem.at[0], recv_sem.at[0], d).start()

    def all_of(box, sem):
        pltpu.make_async_copy(box.at[1:n], box.at[1:n], sem.at[0]).wait()

    def gathered(box):
        stats = []
        for j in range(box.shape[1]):
            total = box[0, j]
            for d in range(1, n):
                total = total + box[d, j]
            stats.append(unpacked(total, size))
        return jnp.concatenate(stats, 0)

    for i in range(images):
        for y in range(rows[3]):
            put(3, y + 1, i, five[i, y])
    halo_wait(3)
    for i in range(images):
        borders(3, i, recvs[3][0, i].astype(F32), recvs[3][1, i].astype(F32))

    outer = {}
    for p in range(rows[3] + 1):
        for i in range(images):
            both = mm(ups[2][...], pair(3, p, i))
            for y, value in ((2 * p - 1, both[: cols[2]]), (2 * p, both[cols[2] :])):
                if 0 <= y < rows[2]:
                    put(2, y + 1, i, lats[2][y, i] + value)
                else:
                    outer[y, i] = value
    def merge(k, p):
        for i in range(images):
            coarse = pair(k + 1, p, i)
            for y in (2 * p - 1, 2 * p):
                value = mm(ups[k][: cols[k]] if y < 2 * p else ups[k][cols[k] :], coarse)
                if not 0 <= y < rows[k]:
                    if k == 0:
                        value = jnp.where(first if y < 0 else last, 0.0, value + bias[0:1, :])
                    hang[k][0 if y < 0 else 1, i] = value
                    continue
                even, odd = columns(k, y + 1 if k == 0 else y, i)
                even = even + value[: half[k]]
                odd = odd + value[half[k] :]
                if k:
                    mid[y, i, : half[k]] = even.astype(BF16)
                    mid[y, i, half[k] :] = odd.astype(BF16)
                put_pairs(k, y + 1, i, even, odd)

    sums_five = conv_rows(3, False)
    for p in range(1, rows[2]):
        merge(1, p)
    for p in range(2, rows[1] - 1):
        merge(0, p)

    carry_start(0, 1)
    halo_wait(2)
    for i in range(images):
        borders(
            2,
            i,
            recvs[2][0, i].astype(F32) + outer[-1, i],
            recvs[2][1, i].astype(F32) + outer[rows[2], i],
        )

    merge(1, 0)
    merge(1, rows[2])
    sums_four = conv_rows(2, True)
    merge(0, 1)
    sums_three = [conv_pairs(1, list(range(1, rows[1] - 1)))]
    sums_two = []

    def conv_two_row(y):
        sums_two.append(conv_pairs(0, [y]))

    inner = list(range(2, rows[0] - 2))
    ahead = len(inner) * 3 // 4
    for y in inner[:ahead]:
        if y == inner[min(2, ahead - 1)]:
            merge(0, rows[1] - 1)
        conv_two_row(y)

    carry_start(0, 0)
    carry_start(1, 0, 1)
    halo_wait(1)
    for way in range(2):
        for i in range(images):
            value = recvs[1][way, i].astype(F32) + hang[1][way, i]
            none = last if way else first
            own = mid[way * (rows[1] - 1), i]
            edge[1][way, i] = jnp.where(none, own, value.astype(BF16))
            value = jnp.where(none, 0.0, value)
            put_pairs(1, way * top[1], i, value[: half[1]], value[half[1] :])
    merge(0, 0)
    merge(0, rows[1])
    sums_three.append(conv_pairs(1, [0, rows[1] - 1]))
    for y in inner[ahead:]:
        conv_two_row(y)
    conv_two_row(1)
    conv_two_row(rows[0] - 2)
    conv_pairs(0, [0], (1, 2), keep_sums=False)
    conv_pairs(0, [rows[0] - 1], (0, 1), keep_sums=False)
    rest_rows = stat_rows(joined(sums_three)) + stat_rows(sums_four) + stat_rows(sums_five)
    post(box_rest, rest_rows, rest_send, rest_recv)

    halo_wait(0)
    for way in range(2):
        for i in range(images):
            keep(0, way * top[0], i, mm(recvs[0][way, i], lat_w[0][...]))
    for way in range(2):
        for i in range(images):
            even, odd = columns(0, way * top[0], i)
            even = even + hang[0][way, i, : half[0]]
            odd = odd + hang[0][way, i, half[0] :]
            put_pairs(0, way * top[0], i, even, odd)
    sums_two.append(conv_pairs(0, [0], (0,), add=True))
    sums_two.append(conv_pairs(0, [rows[0] - 1], (2,), add=True))
    post(box_two, stat_rows(joined(sums_two)), two_send, two_recv)

    def scales(k, total, square):
        share = 1.0 / float(rows[k] * n * cols[k] * size)
        mean = total * share
        variance = square * share - mean * mean
        scale = lax.rsqrt(variance + EPSILON) * gain[k : k + 1, :]
        return scale, shift[k : k + 1, :] - mean * scale

    all_of(box_rest, rest_recv)
    coarse = gathered(box_rest)
    for k in (1, 2, 3):
        for i in range(images):
            slot = ((k - 1) * images + i) * 2
            scale, offset = scales(k, coarse[slot : slot + 1], coarse[slot + 1 : slot + 2])
            if k == 1:
                for y in range(rows[k]):
                    value = jnp.concatenate([conv[k][i, y, b] for b in range(blocks)], 1)
                    done[k][i, y] = (value * scale + offset).astype(BF16)
            else:
                done[k][i] = (conv[k][i] * scale + offset).astype(BF16)
    on_ends(lambda way: [halo_copy(k, way).wait_send() for k in range(4)])
    for j in hops:
        here = hop.at[pieces[j]]
        carry(lambda way, h=here, j=j: pltpu.make_async_copy(h, h, hop_send.at[j]).wait())
    all_of(box_rest, rest_send)

    all_of(box_two, two_recv)
    two = gathered(box_two)
    for i in range(images):
        scale, offset = scales(0, two[2 * i : 2 * i + 1], two[2 * i + 1 : 2 * i + 2])
        affine[2 * i : 2 * i + 1, :] = scale
        affine[2 * i + 1 : 2 * i + 2, :] = offset
    all_of(box_two, two_send)


def finish_kernel(geom, *refs):
    images, rows = geom["images"], geom["rows"]
    conv_two, affine = refs[0:2]
    done = [None, *refs[2:5]]
    out_hbm, staged, rest_sem, two_sem = refs[5:9], refs[9], refs[10], refs[11]
    copies = []
    for k in (1, 2, 3):
        copies.append(pltpu.make_async_copy(done[k], out_hbm[k], rest_sem.at[k]))
        copies[-1].start()
    for i in range(images):
        scale = affine[2 * i : 2 * i + 1, :]
        offset = affine[2 * i + 1 : 2 * i + 2, :]
        for y in range(rows[0]):
            value = jnp.concatenate(
                [conv_two[i, y, b] for b in range(conv_two.shape[2])], 1
            )
            staged[i, y] = (value * scale + offset).astype(BF16)
            pltpu.make_async_copy(
                staged.at[i, y], out_hbm[0].at[i, y], two_sem.at[0]
            ).start()
    for copy in copies:
        copy.wait()
    pltpu.make_async_copy(staged, out_hbm[0], two_sem.at[0]).wait()


def per_device(n, *args):
    feats, lat_ws = args[0:4], args[4:8]
    bias, smooth, gain, shift = args[8:12]
    smooth = smooth.reshape(smooth.shape[0], -1, smooth.shape[3])
    images, chans = feats[0].shape[0], lat_ws[0].shape[1]
    rows = [f.shape[1] for f in feats]
    cols = [f.shape[2] for f in feats]
    geom = {"images": images, "chans": chans, "rows": rows, "cols": cols}
    any_spec = pl.BlockSpec(memory_space=pltpu.HBM)
    vmem_spec = pl.BlockSpec(memory_space=pltpu.VMEM)
    outs = [jax.ShapeDtypeStruct((images, r, c, chans), BF16) for r, c in zip(rows, cols)]
    dma = pltpu.SemaphoreType.DMA
    blocks = chans // LANES
    two_rows = -(-(images * 2) // 8) * 8
    strip = lambda k, count, width, kind: pltpu.VMEM((count, images, cols[k], width), kind)
    scratch = (
        [pltpu.VMEM(f.shape, BF16) for f in feats]
        + [pltpu.VMEM(w.shape, BF16) for w in lat_ws]
        + [pltpu.VMEM((3, *bias.shape), F32), pltpu.VMEM(smooth.shape, BF16)]
        + [pltpu.VMEM((2, 2, 3 * chans, chans), BF16)]
        + [pltpu.VMEM((rows[k] + 2, 4, images, cols[k] // 2, chans), BF16) for k in range(2)]
        + [strip(k, rows[k] + 2, 3 * chans, BF16) for k in (2, 3)]
        + [strip(k, min(rows[k], 2), chans, BF16) for k in range(1, 4)]
        + [strip(k, 2, chans, BF16) for k in range(4)]
        + [pltpu.VMEM((rows[0] + 2, images, blocks, cols[0], LANES), F32)]
        + [pltpu.VMEM((rows[1], images, blocks, cols[1], LANES), F32)]
        + [strip(2, rows[2], chans, F32)]
        + [pltpu.VMEM((images, rows[1], blocks, cols[1], LANES), F32)]
        + [pltpu.VMEM(o.shape, F32) for o in outs[2:]]
        + [pltpu.VMEM((2 * c, c), BF16) for c in cols[:3]]
        + [strip(k, 2, chans, BF16) for k in range(1, 4)]
        + [strip(k, 2, chans, F32) for k in range(2)]
        + [strip(1, rows[1], chans, BF16)]
        + [pltpu.VMEM((images, cols[0], chans), BF16)]
        + [
            pltpu.VMEM((n, -(-levels * images * 2 // (chans // GROUPS)), 1, chans), F32)
            for levels in (1, 3)
        ]
        + [dma((4,)), dma((4,)), dma((2,)), dma((1,))]
        + [dma((4, 2)), dma((2,))]
        + [dma((1,)) for _ in range(3)]
    )
    held = pl.pallas_call(
        functools.partial(kernel, n, geom),
        out_shape=[pltpu.VMEM((images, rows[0], blocks, cols[0], LANES), F32)]
        + [pltpu.VMEM(o.shape, BF16) for o in outs[1:]]
        + [pltpu.VMEM((two_rows, chans), F32)],
        in_specs=[any_spec] * 12,
        out_specs=[vmem_spec] * 5,
        scratch_shapes=scratch,
        compiler_params=pltpu.CompilerParams(
            collective_id=0, has_side_effects=True, vmem_limit_bytes=KERNEL_BYTES
        ),
    )(*args[:8], bias, gain, shift, smooth)
    held = [pltpu.with_memory_space_constraint(h, pltpu.VMEM) for h in held]
    return pl.pallas_call(
        functools.partial(finish_kernel, geom),
        out_shape=outs,
        in_specs=[vmem_spec] * 5,
        out_specs=[any_spec] * 4,
        scratch_shapes=[pltpu.VMEM(outs[0].shape, BF16), dma((4,)), dma((1,))],
        compiler_params=pltpu.CompilerParams(vmem_limit_bytes=16 * 1024 * 1024),
    )(held[0], held[4], *held[1:4])


def solution(mesh):
    strips = P("batch", "rows", None, None)
    run = functools.partial(per_device, mesh.shape["rows"])
    return jax.shard_map(
        lambda *args: tuple(run(*args)),
        mesh=mesh,
        in_specs=(strips,) * 4 + (P(),) * 8,
        out_specs=(strips,) * 4,
        check_vma=False,
    )
```
